8 devices in a mesh: outer: 2 (over z, y), middle: 2 (over x), inner: 2 (over core).
Axes of the slice: x: 2, y: 2, z: 1, core: 2. Of those that a mesh axis runs over, the one named last changes fastest.
Arguments:
- g_embed: float32 [8, 32768, 128], P(('outer', 'middle', 'inner'))
- g_attn: float32 [8, 16, 128, 512], P(('outer', 'middle', 'inner'))
- g_ffn_in: float32 [8, 16, 128, 512], P(('outer', 'middle', 'inner'))
- g_ffn_out: float32 [8, 16, 512, 128], P(('outer', 'middle', 'inner'))
- g_vec: float32 [8, 16, 1664], P(('outer', 'middle', 'inner'))
- m_flat: float32 [7366656], P(('outer', 'middle', 'inner'))
- v_flat: float32 [7366656], P(('outer', 'middle', 'inner'))
- w_flat: float32 [7366656], P(('outer', 'middle', 'inner'))
Outputs:
- output 1: float32 [7366656], P(('outer', 'middle', 'inner'))
- output 2: float32 [7366656], P(('outer', 'middle', 'inner'))
- output 3: float32 [7366656], P(('outer', 'middle', 'inner'))
- output 4: bfloat16 [32768, 128], replicated
- output 5: bfloat16 [16, 128, 512], replicated
- output 6: bfloat16 [16, 128, 512], replicated
- output 7: bfloat16 [16, 512, 128], replicated
- output 8: bfloat16 [16, 1664], replicated
- output 9: bfloat16 [8, 1841664], P(('outer', 'middle', 'inner'))
All inputs are finite; a program needn't handle non-finite values.
Results may differ from the reference program's by a relative error of at most 0.001.
Values are sent between devices in bfloat16 or wider.
A program may use at most 1 GiB of HBM per device.

```python
import math
import jax
import jax.numpy as jnp

DEVICES = 8
VOCAB_ROWS = 32768
D = 128
FF = 512
LAYERS = 16
ADAM_STEP = 3

ADAM_BETA1 = 0.9
ADAM_BETA2 = 0.98
ADAM_EPS = 1e-9
LEARN_RATE = 0.05
NUM_CHIPS = DEVICES // 2
VEC_WIDTH = 9 * D + FF
TENSOR_SHAPES = ((VOCAB_ROWS, D), (LAYERS, D, 4 * D), (LAYERS, D, FF), (LAYERS, FF, D), (LAYERS, VEC_WIDTH))
PARAM_COUNT = sum(math.prod(shape) for shape in TENSOR_SHAPES)


def draw_gradient(gen_key, shape):
    common_key, chip_key, core_key = jax.random.split(gen_key, 3)
    common = jax.random.normal(common_key, shape, jnp.float32)
    per_chip = jax.random.normal(chip_key, (NUM_CHIPS,) + shape, jnp.float32)
    per_core = jax.random.normal(core_key, (DEVICES,) + shape, jnp.float32)
    return common[None] + jnp.repeat(per_chip, 2, axis=0) + 0.25 * per_core


def setup_inputs(seed: int = 0) -> dict:
    key_list = jax.random.split(jax.random.key(seed), 8)
    return {
        'g_embed': draw_gradient(key_list[0], TENSOR_SHAPES[0]),
        'g_attn': draw_gradient(key_list[1], TENSOR_SHAPES[1]),
        'g_ffn_in': draw_gradient(key_list[2], TENSOR_SHAPES[2]),
        'g_ffn_out': draw_gradient(key_list[3], TENSOR_SHAPES[3]),
        'g_vec': draw_gradient(key_list[4], TENSOR_SHAPES[4]),
        'm_flat': 0.3 * jax.random.normal(key_list[5], (PARAM_COUNT,), jnp.float32),
        'v_flat': 0.1 * (0.5 + jax.random.uniform(key_list[6], (PARAM_COUNT,), jnp.float32)),
        'w_flat': jax.random.normal(key_list[7], (PARAM_COUNT,), jnp.float32),
    }


def adam_update(grad_mean, m_old, v_old, w_old):
    m_new = ADAM_BETA1 * m_old + (1.0 - ADAM_BETA1) * grad_mean
    v_new = ADAM_BETA2 * v_old + (1.0 - ADAM_BETA2) * (grad_mean * grad_mean)
    m_hat = m_new / (1.0 - ADAM_BETA1 ** ADAM_STEP)
    v_hat = v_new / (1.0 - ADAM_BETA2 ** ADAM_STEP)
    w_new = w_old - LEARN_RATE * m_hat / (jnp.sqrt(v_hat) + ADAM_EPS)
    return m_new, v_new, w_new


def split_tensors(flat_values, shape_list):
    pieces = []
    offset = 0
    for shape in shape_list:
        count = math.prod(shape)
        pieces.append(flat_values[offset:offset + count].reshape(shape))
        offset += count
    return pieces


def chip_blocks(w_tensors, num_chips):
    blocks = [w_tensors[0].reshape(num_chips, -1)]
    for tensor in w_tensors[1:]:
        layer_count = tensor.shape[0]
        blocks.append(jnp.swapaxes(tensor.reshape(layer_count, num_chips, -1), 0, 1).reshape(num_chips, -1))
    return jnp.concatenate(blocks, axis=1)


def reference(g_embed, g_attn, g_ffn_in, g_ffn_out, g_vec, m_flat, v_flat, w_flat):
    grad_list = (g_embed, g_attn, g_ffn_in, g_ffn_out, g_vec)
    grad_mean = jnp.concatenate([jnp.sum(gradient, axis=0).reshape(-1) for gradient in grad_list]) / DEVICES
    m_new, v_new, w_new = adam_update(grad_mean, m_flat, v_flat, w_flat)
    w_tensors = split_tensors(w_new.astype(jnp.bfloat16), TENSOR_SHAPES)
    w_chip = jnp.repeat(chip_blocks(w_tensors, NUM_CHIPS), 2, axis=0)
    return (m_new, v_new, w_new, w_tensors[0], w_tensors[1], w_tensors[2], w_tensors[3], w_tensors[4], w_chip)
```

```python
import functools
import math
import jax
import jax.numpy as jnp
from jax import lax
from jax.experimental import pallas as pl
from jax.experimental.pallas import tpu as pltpu
from jax.sharding import PartitionSpec as P

MESH_AXES = ('outer', 'middle', 'inner')
ADAM_BETA1 = 0.9
ADAM_BETA2 = 0.98
ADAM_EPS = 1e-9
LEARN_RATE = 0.05
ADAM_STEP = 3

MESH = pl.DeviceIdType.MESH
F32 = jnp.float32
BF16 = jnp.bfloat16

LANES = 128
GROUP = 32
ROWS = 7366656 // LANES
SLICE_ROWS = ROWS // 8
CHUNKS = 19
CHUNK_GROUPS = 12
CHUNK = CHUNK_GROUPS * GROUP
HALF = CHUNK // 2
WINDOW = CHUNKS * CHUNK
LAST_ROWS = SLICE_ROWS - (CHUNKS - 1) * CHUNK
FRONT = 96
BOUNDS = (0, 1024, 1280, 1536, 1792, 1799)
PERMUTED = (1024, 1536)
START_MAX = BOUNDS[-1] - WINDOW // GROUP


def window_start(device):
    return min(SLICE_ROWS * device // GROUP, START_MAX)


def window_start_traced(device):
    return jnp.minimum(lax.div(device * SLICE_ROWS, GROUP), START_MAX)


def split_chunks():
    found = []
    for device in range(8):
        for chunk in range(CHUNKS):
            first = window_start(device) + chunk * CHUNK_GROUPS
            for tensor in range(4):
                edge = BOUNDS[tensor + 1]
                if first < edge < first + CHUNK_GROUPS:
                    found.append((first, tensor, edge - first))
    return tuple(found)


SPLITS = split_chunks()


def step_kernel(e_ref, a_ref, f1_ref, f2_ref, b_ref, m_ref, v_ref, w_ref,
                m_out, v_out, w_out, wg_ref,
                acc, local, p1x, p1y, p2x, p2y, gflat, wflat, wbf, m_in, m_new,
                local_sem, d2d_send, d2d_recv, p1_send, p1x_recv, p1y_recv, p2_send, p2x_recv, p2y_recv,
                in_sem, out_sem, ag_send, agx_recv, agy_recv, relay_send, relx_recv, rely_recv, fwd_send, fwd_recv):
    o, m, i = lax.axis_index('outer'), lax.axis_index('middle'), lax.axis_index('inner')
    x_dev, y_dev, p_dev = (o, 1 - m, i), (1 - o, m, i), (o, m, 1 - i)
    places = ((o, m), (o, 1 - m), (1 - o, m), (1 - o, 1 - m))
    mine = [(po * 2 + pm) * 2 + i for po, pm in places]
    theirs = [(po * 2 + pm) * 2 + (1 - i) for po, pm in places]
    start = window_start_traced(mine[0])
    shift = mine[0] * SLICE_ROWS - start * GROUP
    tensors = (e_ref, a_ref, f1_ref, f2_ref, b_ref)

    barrier = pltpu.get_barrier_semaphore()
    for device in (x_dev, y_dev, p_dev):
        pl.semaphore_signal(barrier, inc=1, device_id=device, device_id_type=MESH)
    pl.semaphore_wait(barrier, 3)

    def remote(src, dst, send, recv, device):
        pltpu.make_async_remote_copy(src_ref=src, dst_ref=dst, send_sem=send, recv_sem=recv, device_id=device, device_id_type=MESH).start()

    def drain(ref, sem):
        pltpu.make_async_copy(ref, ref, sem).wait()

    def load_chunk(device, chunk, copy):
        first = window_start_traced(device) + chunk * CHUNK_GROUPS
        for tensor in range(4):
            @pl.when((first >= BOUNDS[tensor]) & (first + CHUNK_GROUPS <= BOUNDS[tensor + 1]))
            def _():
                row = pl.multiple_of((first - BOUNDS[tensor]) * GROUP, GROUP)
                copy(tensors[tensor].at[pl.ds(row, CHUNK)], 0, CHUNK)
        for known, tensor, count in SPLITS:
            @pl.when(first == known)
            def _():
                head = count * GROUP
                copy(tensors[tensor].at[pl.ds((known - BOUNDS[tensor]) * GROUP, head)], 0, head)
                copy(tensors[tensor + 1].at[pl.ds(0, CHUNK - head)], head, CHUNK - head)

    def issue_gradients(chunk):
        slot = lax.rem(chunk, 3)
        base = pl.multiple_of(chunk * CHUNK, CHUNK)
        for j in (3, 1, 2, 0):
            load_chunk(theirs[j], chunk, lambda src, off, size: remote(
                src, acc.at[j, pl.ds(pl.multiple_of(base + off, GROUP), size)], d2d_send, d2d_recv.at[chunk], p_dev))
            load_chunk(mine[j], chunk, lambda src, off, size: pltpu.make_async_copy(
                src, local.at[slot, j, pl.ds(off, size)], local_sem.at[slot]).start())

    def add_rows(j, base, count, term):
        @pl.loop(0, count // GROUP)
        def _(r):
            off = pl.multiple_of(r * GROUP, GROUP)
            at = pl.ds(pl.multiple_of(base + off, GROUP), GROUP)
            acc[j, at] = acc[j, at] + term(off)

    def first_phase(chunk):
        slot = lax.rem(chunk, 3)
        base = pl.multiple_of(chunk * CHUNK, CHUNK)
        second = pl.multiple_of(base + HALF, HALF)
        drain(local.at[slot], local_sem.at[slot])
        drain(local.at[0], d2d_recv.at[chunk])
        add_rows(1, base, HALF, lambda off: local[slot, 1, pl.ds(off, GROUP)])
        add_rows(2, second, HALF, lambda off: local[slot, 2, pl.ds(HALF + off, GROUP)])
        add_rows(3, base, CHUNK, lambda off: local[slot, 3, pl.ds(off, GROUP)])
        remote(acc.at[1, pl.ds(base, HALF)], p1x.at[chunk, 0], p1_send.at[0], p1x_recv.at[chunk], x_dev)
        remote(acc.at[2, pl.ds(second, HALF)], p1y.at[chunk, 0], p1_send.at[1], p1y_recv.at[chunk], y_dev)
        remote(acc.at[3, pl.ds(base, HALF)], p1x.at[chunk, 1], p1_send.at[0], p1x_recv.at[chunk], x_dev)
        remote(acc.at[3, pl.ds(second, HALF)], p1y.at[chunk, 1], p1_send.at[1], p1y_recv.at[chunk], y_dev)
        add_rows(2, base, HALF, lambda off: local[slot, 2, pl.ds(off, GROUP)])
        add_rows(1, second, HALF, lambda off: local[slot, 1, pl.ds(HALF + off, GROUP)])
        add_rows(0, base, CHUNK, lambda off: local[slot, 0, pl.ds(off, GROUP)])

    def second_phase(chunk):
        base = pl.multiple_of(chunk * CHUNK, CHUNK)
        second = pl.multiple_of(base + HALF, HALF)
        drain(p1x.at[chunk], p1x_recv.at[chunk])
        add_rows(2, base, HALF, lambda off: p1x[chunk, 1, pl.ds(off, GROUP)])
        drain(p1y.at[chunk], p1y_recv.at[chunk])
        add_rows(1, second, HALF, lambda off: p1y[chunk, 1, pl.ds(off, GROUP)])
        remote(acc.at[2, pl.ds(base, HALF)], p2y.at[chunk], p2_send.at[0], p2y_recv.at[chunk], y_dev)
        remote(acc.at[1, pl.ds(second, HALF)], p2x.at[chunk], p2_send.at[1], p2x_recv.at[chunk], x_dev)
        add_rows(0, base, HALF, lambda off: p1x[chunk, 0, pl.ds(off, GROUP)])
        add_rows(0, second, HALF, lambda off: p1y[chunk, 0, pl.ds(off, GROUP)])

    def is_permuted(group):
        return (group >= PERMUTED[0]) & (group < PERMUTED[1])

    def last_phase(chunk):
        base = pl.multiple_of(chunk * CHUNK, CHUNK)
        first = start + chunk * CHUNK_GROUPS
        for part, (arrived, sem) in enumerate(((p2y, p2y_recv), (p2x, p2x_recv))):
            drain(arrived.at[chunk], sem.at[chunk])

            @pl.loop(0, HALF // GROUP)
            def _(r):
                off = pl.multiple_of(r * GROUP, GROUP)
                row = pl.multiple_of(base + part * HALF + off, GROUP)
                total = acc[0, pl.ds(row, GROUP)] + arrived[chunk, pl.ds(off, GROUP)]
                permuted = is_permuted(first + part * (HALF // GROUP) + r)

                @pl.when(permuted)
                def _():
                    for tile in range(4):
                        gflat[pl.ds(row + tile, 8, stride=4)] = total[8 * tile:8 * tile + 8]

                @pl.when(jnp.logical_not(permuted))
                def _():
                    gflat[pl.ds(row, GROUP)] = total

    def state_copies(block, size):
        slot = lax.rem(block, 2)
        at = pl.ds(pl.multiple_of(block * CHUNK, CHUNK), size)
        loads = [pltpu.make_async_copy(ref.at[at], m_in.at[slot, q, pl.ds(0, size)], in_sem.at[slot, q])
                 for q, ref in enumerate((m_ref, v_ref, w_ref))]
        stores = [pltpu.make_async_copy(m_new.at[slot, q, pl.ds(0, size)], ref.at[at], out_sem.at[slot, q])
                  for q, ref in enumerate((m_out, v_out, w_out))]
        return loads, stores

    def for_block(block, action):
        @pl.when(block < CHUNKS - 1)
        def _():
            action(*state_copies(block, CHUNK))

        @pl.when(block == CHUNKS - 1)
        def _():
            action(*state_copies(block, LAST_ROWS))

    def start_loads(loads, stores):
        for copy in loads:
            copy.start()

    def wait_loads(loads, stores):
        for copy in loads:
            copy.wait()

    def start_stores(loads, stores):
        for copy in stores:
            copy.start()

    def wait_stores(loads, stores):
        for copy in stores:
            copy.wait()

    def adam(block):
        slot = lax.rem(block, 2)
        base = pl.multiple_of(block * CHUNK, CHUNK)
        for_block(block, wait_loads)

        @pl.when(block >= 2)
        def _():
            for_block(block - 2, wait_stores)

        @pl.loop(0, CHUNK_GROUPS)
        def _(r):
            off = pl.multiple_of(r * GROUP, GROUP)
            at = pl.ds(off, GROUP)
            grad = gflat[pl.ds(base + off + shift, GROUP)] / 8
            m_val = ADAM_BETA1 * m_in[slot, 0, at] + (1.0 - ADAM_BETA1) * grad
            v_val = ADAM_BETA2 * m_in[slot, 1, at] + (1.0 - ADAM_BETA2) * (grad * grad)
            m_hat = m_val / (1.0 - ADAM_BETA1 ** ADAM_STEP)
            v_hat = v_val / (1.0 - ADAM_BETA2 ** ADAM_STEP)
            w_val = m_in[slot, 2, at] - LEARN_RATE * m_hat / (jnp.sqrt(v_hat) + ADAM_EPS)
            m_new[slot, 0, at] = m_val
            m_new[slot, 1, at] = v_val
            m_new[slot, 2, at] = w_val
            wflat[pl.ds(pl.multiple_of(FRONT + base + off, GROUP), GROUP)] = w_val

        for_block(block, start_stores)

        @pl.loop(0, CHUNK_GROUPS)
        def _(r):
            row = pl.multiple_of(base + r * GROUP, GROUP)
            source = FRONT + row - shift
            permuted = is_permuted(start + block * CHUNK_GROUPS + r)

            @pl.when(permuted)
            def _():
                tiles = [wflat[pl.ds(source + tile, 8, stride=4)] for tile in range(4)]
                wbf[pl.ds(row, GROUP)] = jnp.concatenate(tiles, axis=0).astype(BF16)

            @pl.when(jnp.logical_not(permuted))
            def _():
                wbf[pl.ds(row, GROUP)] = wflat[pl.ds(source, GROUP)].astype(BF16)

        at = pl.ds(base, CHUNK)
        remote(wbf.at[at], wg_ref.at[mine[0], at], ag_send.at[0], agx_recv.at[block], x_dev)
        remote(wbf.at[at], wg_ref.at[mine[0], at], ag_send.at[1], agy_recv.at[block], y_dev)
        remote(wbf.at[at], wg_ref.at[mine[0], at], fwd_send.at[0], fwd_recv.at[0], p_dev)
        pltpu.make_async_copy(wbf.at[at], wg_ref.at[mine[0], at], ag_send.at[2]).start()

    def relay(chunk):
        base = pl.multiple_of(chunk * CHUNK, CHUNK)
        at, head, tail = pl.ds(base, CHUNK), pl.ds(base, HALF), pl.ds(pl.multiple_of(base + HALF, HALF), HALF)
        drain(wbf.at[pl.ds(0, CHUNK)], agx_recv.at[chunk])
        remote(wg_ref.at[mine[1], head], wg_ref.at[mine[1], head], relay_send.at[0], rely_recv.at[chunk], y_dev)
        remote(wg_ref.at[mine[1], at], wg_ref.at[mine[1], at], fwd_send.at[1], fwd_recv.at[1], p_dev)
        drain(wbf.at[pl.ds(0, CHUNK)], agy_recv.at[chunk])
        remote(wg_ref.at[mine[2], tail], wg_ref.at[mine[2], tail], relay_send.at[1], relx_recv.at[chunk], x_dev)
        remote(wg_ref.at[mine[2], at], wg_ref.at[mine[2], at], fwd_send.at[2], fwd_recv.at[2], p_dev)

    def forward(chunk):
        base = pl.multiple_of(chunk * CHUNK, CHUNK)
        at = pl.ds(base, CHUNK)
        drain(wbf.at[pl.ds(0, HALF)], rely_recv.at[chunk])
        drain(wbf.at[pl.ds(0, HALF)], relx_recv.at[chunk])
        remote(wg_ref.at[mine[3], at], wg_ref.at[mine[3], at], fwd_send.at[3], fwd_recv.at[3], p_dev)

    issue_gradients(0)
    issue_gradients(1)

    stages = ((0, first_phase), (1, second_phase), (2, last_phase), (3, adam), (5, relay), (6, forward))

    @pl.loop(0, CHUNKS + stages[-1][0])
    def _(t):
        @pl.when(t + 2 < CHUNKS)
        def _():
            issue_gradients(t + 2)

        @pl.when((t >= 2) & (t - 2 < CHUNKS))
        def _():
            for_block(t - 2, start_loads)

        for lag, stage in stages:
            @pl.when((t >= lag) & (t - lag < CHUNKS))
            def _():
                stage(t - lag)

    for block in (CHUNKS - 2, CHUNKS - 1):
        for_block(block, wait_stores)
    drain(acc, d2d_send)
    for q in range(2):
        drain(acc.at[0], p1_send.at[q])
        drain(acc.at[0, pl.ds(0, WINDOW // 2)], p2_send.at[q])
        drain(wbf.at[pl.ds(0, WINDOW // 2)], relay_send.at[q])
    for q in range(3):
        drain(wbf, ag_send.at[q])
    for q in range(4):
        drain(wbf, fwd_send.at[q])
        drain(wbf, fwd_recv.at[q])


def step_call(tensors, state):
    hbm = pl.BlockSpec(memory_space=pl.ANY)
    dma = pltpu.SemaphoreType.DMA
    flat = jax.ShapeDtypeStruct((SLICE_ROWS, LANES), F32)
    return pl.pallas_call(
        step_kernel,
        name='adam_step',
        out_shape=(flat, flat, flat, jax.ShapeDtypeStruct((8, WINDOW, LANES), BF16)),
        in_specs=[hbm] * 8,
        out_specs=[hbm] * 4,
        scratch_shapes=[
            pltpu.VMEM((4, WINDOW, LANES), F32),
            pltpu.VMEM((3, 4, CHUNK, LANES), F32),
            pltpu.VMEM((CHUNKS, 2, HALF, LANES), F32),
            pltpu.VMEM((CHUNKS, 2, HALF, LANES), F32),
            pltpu.VMEM((CHUNKS, HALF, LANES), F32),
            pltpu.VMEM((CHUNKS, HALF, LANES), F32),
            pltpu.VMEM((WINDOW + 128, LANES), F32),
            pltpu.VMEM((WINDOW + FRONT, LANES), F32),
            pltpu.VMEM((WINDOW, LANES), BF16),
            pltpu.VMEM((2, 3, CHUNK, LANES), F32),
            pltpu.VMEM((2, 3, CHUNK, LANES), F32),
            dma((3,)), dma, dma((CHUNKS,)), dma((2,)), dma((CHUNKS,)), dma((CHUNKS,)), dma((2,)), dma((CHUNKS,)), dma((CHUNKS,)),
            dma((2, 3)), dma((2, 3)), dma((3,)), dma((CHUNKS,)), dma((CHUNKS,)), dma((2,)), dma((CHUNKS,)), dma((CHUNKS,)),
            dma((4,)), dma((4,)),
        ],
        compiler_params=pltpu.CompilerParams(collective_id=0, has_side_effects=True, vmem_limit_bytes=56 * 1024 * 1024),
    )(*tensors, *state)


LAYERS = 16
CHIP_ROWS = 8192 + 3 * 2048


def place_kernel(wg_ref, e_ref, a_ref, f1_ref, f2_ref, b_ref, chip_ref, full, edge, wide, block, in_sem, edge_sem, out_sem, chip_sem):
    chip = lax.axis_index('outer') * 2 + lax.axis_index('middle')
    firsts = [SLICE_ROWS * d // GROUP for d in range(8)] + [BOUNDS[-1]]
    loads = []
    for d in range(8):
        first, last = firsts[d], firsts[d + 1]
        src = wg_ref.at[d, pl.ds((first - window_start(d)) * GROUP, (last - first) * GROUP)]
        loads.append(pltpu.make_async_copy(src, full.at[pl.ds(first * GROUP, (last - first) * GROUP)], in_sem.at[d]))
        loads[-1].start()
    edges = []
    for d in range(1, 8):
        src = wg_ref.at[d - 1, pl.ds((firsts[d] - window_start(d - 1)) * GROUP, GROUP)]
        edges.append(pltpu.make_async_copy(src, edge.at[d - 1], edge_sem.at[d - 1]))
        edges[-1].start()
    for d in range(8):
        loads[d].wait()
        if d:
            edges[d - 1].wait()
            keep = SLICE_ROWS * d - firsts[d] * GROUP
            row = lax.broadcasted_iota(jnp.int32, (GROUP, LANES), 0)
            if PERMUTED[0] <= firsts[d] < PERMUTED[1]:
                row = 4 * (row % 8) + row // 8
            at = pl.ds(firsts[d] * GROUP, GROUP)
            full[at] = jnp.where(row < keep, edge[d - 1].astype(F32), full[at].astype(F32)).astype(BF16)
    outs = []
    for q, ref in enumerate((e_ref, a_ref, f1_ref, f2_ref, b_ref)):
        size = ref.shape[0]
        outs.append(pltpu.make_async_copy(full.at[pl.ds(BOUNDS[q] * GROUP, size)], ref, out_sem.at[q]))
        outs[-1].start()
    embed = pltpu.make_async_copy(full.at[pl.ds(pl.multiple_of(chip * 8192, GROUP), 8192)], chip_ref.at[pl.ds(0, 8192)], chip_sem.at[0])
    embed.start()

    @pl.loop(0, LAYERS)
    def _(layer):
        row = pl.multiple_of(BOUNDS[3] * GROUP + layer * 512 + chip * 128, GROUP)
        pltpu.make_async_copy(full.at[pl.ds(row, 128)], chip_ref.at[pl.ds(pl.multiple_of(8192 + 4096 + layer * 128, 128), 128)], chip_sem.at[1]).start()

    for q in range(2):
        @pl.loop(0, LAYERS * 4)
        def _(r):
            row = pl.multiple_of(BOUNDS[1 + q] * GROUP + (r // 4) * 512 + chip * 128 + (r % 4) * GROUP, GROUP)
            group = full[pl.ds(row, GROUP)].astype(F32)
            for tile in range(4):
                wide[r % 4, pl.ds(tile, 8, stride=4)] = group[8 * tile:8 * tile + 8]
            block[q, pl.ds(pl.multiple_of(r * GROUP, GROUP), GROUP)] = wide[r % 4].astype(BF16)
        outs.append(pltpu.make_async_copy(block.at[q], chip_ref.at[pl.ds(8192 + q * 2048, 2048)], chip_sem.at[2 + q]))
        outs[-1].start()
    for copy in outs:
        copy.wait()
    embed.wait()
    pltpu.make_async_copy(block.at[0], chip_ref.at[pl.ds(8192 + 4096, 2048)], chip_sem.at[1]).wait()


def place_call(gathered):
    hbm = pl.BlockSpec(memory_space=pl.ANY)
    dma = pltpu.SemaphoreType.DMA
    sizes = (32768, 8192, 8192, 8192, 208, CHIP_ROWS)
    return pl.pallas_call(
        place_kernel,
        name='place_weights',
        out_shape=tuple(jax.ShapeDtypeStruct((size, LANES), BF16) for size in sizes),
        in_specs=[hbm],
        out_specs=[hbm] * 6,
        scratch_shapes=[
            pltpu.VMEM((BOUNDS[-1] * GROUP, LANES), BF16),
            pltpu.VMEM((7, GROUP, LANES), BF16),
            pltpu.VMEM((4, GROUP, LANES), F32),
            pltpu.VMEM((2, 2048, LANES), BF16),
            dma((8,)), dma((7,)), dma((5,)), dma((4,)),
        ],
        compiler_params=pltpu.CompilerParams(vmem_limit_bytes=24 * 1024 * 1024),
    )(gathered)


def to_tiles(tensor):
    return tensor.reshape(256, 8, 4, LANES).transpose(0, 2, 1, 3).reshape(8192, LANES)


def from_tiles(rows):
    return rows.reshape(256, 4, 8, LANES).transpose(0, 2, 1, 3).reshape(16, 128, 512)


def solution(mesh):
    def local_step(g_embed, g_attn, g_ffn_in, g_ffn_out, g_vec, m_shard, v_shard, w_shard):
        vec_rows = jnp.pad(g_vec.reshape(208, LANES), ((0, 16), (0, 0)))
        tensors = (g_embed.reshape(32768, LANES), to_tiles(g_attn), to_tiles(g_ffn_in), g_ffn_out.reshape(8192, LANES), vec_rows)
        state = [shard.reshape(SLICE_ROWS, LANES) for shard in (m_shard, v_shard, w_shard)]
        m_new, v_new, w_new, gathered = step_call(tensors, state)
        embed, attn, ffn_in, ffn_out, vec, chip_rows = place_call(gathered)
        wb_vec = vec.reshape(16, 1664)
        chip = lax.axis_index('outer') * 2 + lax.axis_index('middle')
        vec_block = lax.dynamic_slice_in_dim(wb_vec, chip * 416, 416, axis=1).reshape(-1)
        w_chip = jnp.concatenate([chip_rows.reshape(-1), vec_block])[None, :]
        return (m_new.reshape(-1), v_new.reshape(-1), w_new.reshape(-1), embed, from_tiles(attn), from_tiles(ffn_in),
                ffn_out.reshape(16, 512, 128), wb_vec, w_chip)

    return jax.shard_map(local_step, mesh=mesh, in_specs=(P(MESH_AXES),) * 8, out_specs=(P(MESH_AXES),) * 3 + (P(),) * 5 + (P(MESH_AXES),), check_vma=False)
```

```python
import functools
import math
import jax
import jax.numpy as jnp
from jax import lax
from jax.experimental import pallas as pl
from jax.experimental.pallas import tpu as pltpu
from jax.sharding import PartitionSpec as P

MESH_AXES = ('outer', 'middle', 'inner')
ADAM_BETA1 = 0.9
ADAM_BETA2 = 0.98
ADAM_EPS = 1e-9
LEARN_RATE = 0.05
ADAM_STEP = 3

MESH = pl.DeviceIdType.MESH
F32 = jnp.float32
BF16 = jnp.bfloat16

LANES = 128
GROUP = 32
ROWS = 7366656 // LANES
SLICE_ROWS = ROWS // 8
CHUNKS = 19
CHUNK_GROUPS = 12
CHUNK = CHUNK_GROUPS * GROUP
HALF = CHUNK // 2
RING = 4
WINDOW = CHUNKS * CHUNK
LAST_ROWS = SLICE_ROWS - (CHUNKS - 1) * CHUNK
FRONT = 96
BOUNDS = (0, 1024, 1280, 1536, 1792, 1799)
PERMUTED = (1024, 1536)
START_MAX = BOUNDS[-1] - WINDOW // GROUP


def window_start(device):
    return min(SLICE_ROWS * device // GROUP, START_MAX)


def window_start_traced(device):
    return jnp.minimum(lax.div(device * SLICE_ROWS, GROUP), START_MAX)


def split_chunks():
    found = []
    for device in range(8):
        for chunk in range(CHUNKS):
            first = window_start(device) + chunk * CHUNK_GROUPS
            for tensor in range(4):
                edge = BOUNDS[tensor + 1]
                if first < edge < first + CHUNK_GROUPS:
                    found.append((first, tensor, edge - first))
    return tuple(found)


SPLITS = split_chunks()
FIRSTS = tuple(SLICE_ROWS * d // GROUP for d in range(8)) + (BOUNDS[-1] - 1,)


def step_kernel(e_ref, a_ref, f1_ref, f2_ref, b_ref, m_ref, v_ref, w_ref,
                m_out, v_out, w_out, wg_ref,
                acc, local, p1x, p1y, p2x, p2y, gflat, wflat, m_in,
                local_sem, d2d_send, d2d_recv, p1_send, p1x_recv, p1y_recv, p2_send, p2x_recv, p2y_recv,
                in_sem, ag_send, agx_recv, agy_recv, relay_send, relx_recv, rely_recv, fwd_send, fwd_recv):
    o, m, i = lax.axis_index('outer'), lax.axis_index('middle'), lax.axis_index('inner')
    x_dev, y_dev, p_dev = (o, 1 - m, i), (1 - o, m, i), (o, m, 1 - i)
    places = ((o, m), (o, 1 - m), (1 - o, m), (1 - o, 1 - m))
    mine = [(po * 2 + pm) * 2 + i for po, pm in places]
    theirs = [(po * 2 + pm) * 2 + (1 - i) for po, pm in places]
    start = window_start_traced(mine[0])
    shift = mine[0] * SLICE_ROWS - start * GROUP
    tensors = (e_ref, a_ref, f1_ref, f2_ref, b_ref)

    barrier = pltpu.get_barrier_semaphore()
    for device in (x_dev, y_dev, p_dev):
        pl.semaphore_signal(barrier, inc=1, device_id=device, device_id_type=MESH)
    pl.semaphore_wait(barrier, 3)

    def remote(src, dst, send, recv, device):
        pltpu.make_async_remote_copy(src_ref=src, dst_ref=dst, send_sem=send, recv_sem=recv, device_id=device, device_id_type=MESH).start()

    def drain(ref, sem):
        pltpu.make_async_copy(ref, ref, sem).wait()

    def load_chunk(device, chunk, copy):
        first = window_start_traced(device) + chunk * CHUNK_GROUPS
        for tensor in range(4):
            @pl.when((first >= BOUNDS[tensor]) & (first + CHUNK_GROUPS <= BOUNDS[tensor + 1]))
            def _():
                row = pl.multiple_of((first - BOUNDS[tensor]) * GROUP, GROUP)
                copy(tensors[tensor].at[pl.ds(row, CHUNK)], 0, CHUNK)
        for known, tensor, count in SPLITS:
            @pl.when(first == known)
            def _():
                head = count * GROUP
                copy(tensors[tensor].at[pl.ds((known - BOUNDS[tensor]) * GROUP, head)], 0, head)
                copy(tensors[tensor + 1].at[pl.ds(0, CHUNK - head)], head, CHUNK - head)

    def issue_gradients(chunk):
        slot = lax.rem(chunk, 3)
        base = pl.multiple_of(chunk * CHUNK, CHUNK)
        for j in (3, 1, 2, 0):
            load_chunk(theirs[j], chunk, lambda src, off, size: remote(
                src, acc.at[j, pl.ds(pl.multiple_of(base + off, GROUP), size)], d2d_send, d2d_recv.at[chunk], p_dev))
            load_chunk(mine[j], chunk, lambda src, off, size: pltpu.make_async_copy(
                src, local.at[slot, j, pl.ds(off, size)], local_sem.at[slot]).start())

    def add_rows(j, base, count, term):
        @pl.loop(0, count // GROUP)
        def _(r):
            off = pl.multiple_of(r * GROUP, GROUP)
            at = pl.ds(pl.multiple_of(base + off, GROUP), GROUP)
            acc[j, at] = acc[j, at] + term(off)

    def first_phase(chunk):
        slot = lax.rem(chunk, 3)
        ring = lax.rem(chunk, RING)
        base = pl.multiple_of(chunk * CHUNK, CHUNK)
        second = pl.multiple_of(base + HALF, HALF)
        drain(local.at[slot], local_sem.at[slot])
        drain(local.at[0], d2d_recv.at[chunk])
        add_rows(1, base, HALF, lambda off: local[slot, 1, pl.ds(off, GROUP)])
        add_rows(2, second, HALF, lambda off: local[slot, 2, pl.ds(HALF + off, GROUP)])
        add_rows(3, base, CHUNK, lambda off: local[slot, 3, pl.ds(off, GROUP)])
        remote(acc.at[1, pl.ds(base, HALF)], p1x.at[ring, 0], p1_send.at[0], p1x_recv.at[chunk], x_dev)
        remote(acc.at[2, pl.ds(second, HALF)], p1y.at[ring, 0], p1_send.at[1], p1y_recv.at[chunk], y_dev)
        remote(acc.at[3, pl.ds(base, HALF)], p1x.at[ring, 1], p1_send.at[0], p1x_recv.at[chunk], x_dev)
        remote(acc.at[3, pl.ds(second, HALF)], p1y.at[ring, 1], p1_send.at[1], p1y_recv.at[chunk], y_dev)
        add_rows(2, base, HALF, lambda off: local[slot, 2, pl.ds(off, GROUP)])
        add_rows(1, second, HALF, lambda off: local[slot, 1, pl.ds(HALF + off, GROUP)])
        add_rows(0, base, CHUNK, lambda off: local[slot, 0, pl.ds(off, GROUP)])

    def second_phase(chunk):
        ring = lax.rem(chunk, RING)
        base = pl.multiple_of(chunk * CHUNK, CHUNK)
        second = pl.multiple_of(base + HALF, HALF)
        drain(p1x.at[ring], p1x_recv.at[chunk])
        add_rows(2, base, HALF, lambda off: p1x[ring, 1, pl.ds(off, GROUP)])
        drain(p1y.at[ring], p1y_recv.at[chunk])
        add_rows(1, second, HALF, lambda off: p1y[ring, 1, pl.ds(off, GROUP)])
        remote(acc.at[2, pl.ds(base, HALF)], p2y.at[ring], p2_send.at[0], p2y_recv.at[chunk], y_dev)
        remote(acc.at[1, pl.ds(second, HALF)], p2x.at[ring], p2_send.at[1], p2x_recv.at[chunk], x_dev)
        add_rows(0, base, HALF, lambda off: p1x[ring, 0, pl.ds(off, GROUP)])
        add_rows(0, second, HALF, lambda off: p1y[ring, 0, pl.ds(off, GROUP)])

    def is_permuted(group):
        return (group >= PERMUTED[0]) & (group < PERMUTED[1])

    def last_phase(chunk):
        ring = lax.rem(chunk, RING)
        base = pl.multiple_of(chunk * CHUNK, CHUNK)
        first = start + chunk * CHUNK_GROUPS
        for part, (arrived, sem) in enumerate(((p2y, p2y_recv), (p2x, p2x_recv))):
            drain(arrived.at[ring], sem.at[chunk])

            @pl.loop(0, HALF // GROUP)
            def _(r):
                off = pl.multiple_of(r * GROUP, GROUP)
                row = pl.multiple_of(base + part * HALF + off, GROUP)
                total = acc[0, pl.ds(row, GROUP)] + arrived[ring, pl.ds(off, GROUP)]
                permuted = is_permuted(first + part * (HALF // GROUP) + r)

                @pl.when(permuted)
                def _():
                    for tile in range(4):
                        gflat[pl.ds(row + tile, 8, stride=4)] = total[8 * tile:8 * tile + 8]

                @pl.when(jnp.logical_not(permuted))
                def _():
                    gflat[pl.ds(row, GROUP)] = total

    def state_loads(block, size):
        slot = lax.rem(block, 2)
        at = pl.ds(pl.multiple_of(block * CHUNK, CHUNK), size)
        return [pltpu.make_async_copy(ref.at[at], m_in.at[slot, q, pl.ds(0, size)], in_sem.at[slot, q])
                for q, ref in enumerate((m_ref, v_ref, w_ref))]

    def start_loads(block):
        for last, size in ((False, CHUNK), (True, LAST_ROWS)):
            @pl.when((block == CHUNKS - 1) == last)
            def _():
                for copy in state_loads(block, size):
                    copy.start()

    def wait_loads(block):
        for last, size in ((False, CHUNK), (True, LAST_ROWS)):
            @pl.when((block == CHUNKS - 1) == last)
            def _():
                for copy in state_loads(block, size):
                    copy.wait()

    def adam_rows(slot, base, off, count):
        at = pl.ds(off, count)
        grad = gflat[pl.ds(base + off + shift, count)] / 8
        m_val = ADAM_BETA1 * m_in[slot, 0, at] + (1.0 - ADAM_BETA1) * grad
        v_val = ADAM_BETA2 * m_in[slot, 1, at] + (1.0 - ADAM_BETA2) * (grad * grad)
        m_hat = m_val / (1.0 - ADAM_BETA1 ** ADAM_STEP)
        v_hat = v_val / (1.0 - ADAM_BETA2 ** ADAM_STEP)
        w_val = m_in[slot, 2, at] - LEARN_RATE * m_hat / (jnp.sqrt(v_hat) + ADAM_EPS)
        out = pl.ds(pl.multiple_of(base + off, GROUP), count)
        m_out[out] = m_val
        v_out[out] = v_val
        w_out[out] = w_val
        wflat[pl.ds(pl.multiple_of(FRONT + base + off, GROUP), count)] = w_val

    def adam(block):
        slot = lax.rem(block, 2)
        base = pl.multiple_of(block * CHUNK, CHUNK)
        wait_loads(block)

        @pl.loop(0, jnp.where(block == CHUNKS - 1, LAST_ROWS // GROUP, CHUNK_GROUPS))
        def _(r):
            adam_rows(slot, base, pl.multiple_of(r * GROUP, GROUP), GROUP)

        @pl.when(block == CHUNKS - 1)
        def _():
            adam_rows((CHUNKS - 1) % 2, (CHUNKS - 1) * CHUNK, LAST_ROWS // GROUP * GROUP, LAST_ROWS % GROUP)

        @pl.loop(0, CHUNK_GROUPS)
        def _(r):
            row = pl.multiple_of(base + r * GROUP, GROUP)
            source = FRONT + row - shift
            permuted = is_permuted(start + block * CHUNK_GROUPS + r)

            @pl.when(permuted)
            def _():
                tiles = [wflat[pl.ds(source + tile, 8, stride=4)] for tile in range(4)]
                wg_ref[mine[0], pl.ds(row, GROUP)] = jnp.concatenate(tiles, axis=0).astype(BF16)

            @pl.when(jnp.logical_not(permuted))
            def _():
                wg_ref[mine[0], pl.ds(row, GROUP)] = wflat[pl.ds(source, GROUP)].astype(BF16)

        ours = wg_ref.at[mine[0], pl.ds(base, CHUNK)]
        remote(ours, ours, ag_send.at[0], agx_recv.at[block], x_dev)
        remote(ours, ours, ag_send.at[1], agy_recv.at[block], y_dev)
        remote(ours, ours, fwd_send.at[0], fwd_recv.at[0], p_dev)

    def relay(chunk):
        base = pl.multiple_of(chunk * CHUNK, CHUNK)
        at, head, tail = pl.ds(base, CHUNK), pl.ds(base, HALF), pl.ds(pl.multiple_of(base + HALF, HALF), HALF)
        drain(wg_ref.at[0, pl.ds(0, CHUNK)], agx_recv.at[chunk])
        remote(wg_ref.at[mine[1], head], wg_ref.at[mine[1], head], relay_send.at[0], rely_recv.at[chunk], y_dev)
        remote(wg_ref.at[mine[1], at], wg_ref.at[mine[1], at], fwd_send.at[1], fwd_recv.at[1], p_dev)
        drain(wg_ref.at[0, pl.ds(0, CHUNK)], agy_recv.at[chunk])
        remote(wg_ref.at[mine[2], tail], wg_ref.at[mine[2], tail], relay_send.at[1], relx_recv.at[chunk], x_dev)
        remote(wg_ref.at[mine[2], at], wg_ref.at[mine[2], at], fwd_send.at[2], fwd_recv.at[2], p_dev)

    def forward(chunk):
        base = pl.multiple_of(chunk * CHUNK, CHUNK)
        at = pl.ds(base, CHUNK)
        drain(wg_ref.at[0, pl.ds(0, HALF)], rely_recv.at[chunk])
        drain(wg_ref.at[0, pl.ds(0, HALF)], relx_recv.at[chunk])
        remote(wg_ref.at[mine[3], at], wg_ref.at[mine[3], at], fwd_send.at[3], fwd_recv.at[3], p_dev)

    issue_gradients(0)
    issue_gradients(1)

    stages = ((0, first_phase), (1, second_phase), (2, last_phase), (3, adam), (5, relay), (6, forward))

    @pl.loop(0, CHUNKS + stages[-1][0])
    def _(t):
        @pl.when(t + 2 < CHUNKS)
        def _():
            issue_gradients(t + 2)

        @pl.when((t >= 2) & (t - 2 < CHUNKS))
        def _():
            start_loads(t - 2)

        for lag, stage in stages:
            @pl.when((t >= lag) & (t - lag < CHUNKS))
            def _():
                stage(t - lag)

    drain(acc, d2d_send)
    for q in range(2):
        drain(acc.at[0], p1_send.at[q])
        drain(acc.at[0, pl.ds(0, WINDOW // 2)], p2_send.at[q])
        drain(wg_ref.at[0, pl.ds(0, WINDOW // 2)], relay_send.at[q])
        drain(wg_ref.at[0], ag_send.at[q])
    for q in range(4):
        drain(wg_ref.at[0], fwd_send.at[q])
        drain(wg_ref.at[0], fwd_recv.at[q])

    for d in range(1, 8):
        keep = SLICE_ROWS * d - FIRSTS[d] * GROUP
        row = lax.broadcasted_iota(jnp.int32, (GROUP, LANES), 0)
        if PERMUTED[0] <= FIRSTS[d] < PERMUTED[1]:
            row = 4 * (row % 8) + row // 8
        before = pl.ds((FIRSTS[d] - window_start(d - 1)) * GROUP, GROUP)
        after = pl.ds((FIRSTS[d] - window_start(d)) * GROUP, GROUP)
        wg_ref[d - 1, before] = jnp.where(row < keep, wg_ref[d - 1, before].astype(F32), wg_ref[d, after].astype(F32)).astype(BF16)


def step_call(tensors, state):
    hbm = pl.BlockSpec(memory_space=pl.ANY)
    dma = pltpu.SemaphoreType.DMA
    flat = pltpu.VMEM((SLICE_ROWS, LANES), F32)
    return pl.pallas_call(
        step_kernel,
        name='adam_step',
        out_shape=(flat, flat, flat, pltpu.VMEM((8, WINDOW, LANES), BF16)),
        in_specs=[hbm] * 8,
        out_specs=[pl.BlockSpec(memory_space=pltpu.VMEM)] * 4,
        scratch_shapes=[
            pltpu.VMEM((4, WINDOW, LANES), F32),
            pltpu.VMEM((3, 4, CHUNK, LANES), F32),
            pltpu.VMEM((RING, 2, HALF, LANES), F32),
            pltpu.VMEM((RING, 2, HALF, LANES), F32),
            pltpu.VMEM((RING, HALF, LANES), F32),
            pltpu.VMEM((RING, HALF, LANES), F32),
            pltpu.VMEM((WINDOW + 128, LANES), F32),
            pltpu.VMEM((WINDOW + FRONT, LANES), F32),
            pltpu.VMEM((2, 3, CHUNK, LANES), F32),
            dma((3,)), dma, dma((CHUNKS,)), dma((2,)), dma((CHUNKS,)), dma((CHUNKS,)), dma((2,)), dma((CHUNKS,)), dma((CHUNKS,)),
            dma((2, 3)), dma((2,)), dma((CHUNKS,)), dma((CHUNKS,)), dma((2,)), dma((CHUNKS,)), dma((CHUNKS,)),
            dma((4,)), dma((4,)),
        ],
        compiler_params=pltpu.CompilerParams(collective_id=0, has_side_effects=True, vmem_limit_bytes=32 * 1024 * 1024),
    )(*tensors, *state)


LAYERS = 16
PAIR_ROWS = 8192 + 3 * 2048 + 52
PAIR_SIZE = PAIR_ROWS * LANES
PARTS = 4


def place_kernel(mv_ref, vv_ref, wv_ref, wg_ref, m_out, v_out, w_out, e_ref, a_ref, f1_ref, f2_ref, b_ref, pair_ref, flat, wide, state_sem, out_sem, pair_sem):
    pair = lax.axis_index('outer') * 2 + lax.axis_index('middle')
    copies = []

    def put(src, dst, sem):
        copies.append(pltpu.make_async_copy(src, dst, sem))
        copies[-1].start()

    for q, (src, dst) in enumerate(((mv_ref, m_out), (vv_ref, v_out), (wv_ref, w_out))):
        put(src, dst, state_sem.at[q])
    count = 0
    for d in range(8):
        low, high = (FIRSTS[d] + 1 if d else 0), FIRSTS[d + 1] + 1
        for q, ref in enumerate((e_ref, a_ref, f1_ref, f2_ref, b_ref)):
            begin, end = max(low, BOUNDS[q]), min(high, BOUNDS[q + 1])
            if begin < end:
                offset = (begin - BOUNDS[q]) * GROUP
                size = min((end - begin) * GROUP, ref.shape[0] - offset)
                put(wg_ref.at[d, pl.ds((begin - window_start(d)) * GROUP, size)], ref.at[pl.ds(offset, size)], out_sem.at[count])
                count += 1

    def finish(begin, size, sem):
        put(flat.at[:, pl.ds(begin * LANES, size * LANES)], pair_ref.at[:, pl.ds(begin * LANES, size * LANES)], sem)

    def source(group, low, last, starts):
        late = group > last
        row = (group - jnp.where(late, starts[1], starts[0])) * GROUP
        return low + jnp.where(late, 1, 0), pl.multiple_of(row, GROUP)

    embed_starts = (window_start_traced(pair), window_start_traced(pair + 1))
    for part in range(PARTS):
        @pl.loop(part * 256 // PARTS, (part + 1) * 256 // PARTS)
        def _(g):
            d, row = source(pair * 256 + g, pair, embed_starts[1], embed_starts)
            for tile in range(4):
                flat[0:1, pl.ds(pl.multiple_of(g * 4096 + tile * 1024, 1024), 1024)] = wg_ref[d, pl.ds(row + 8 * tile, 8)].reshape(1, 1024)

        finish(part * 8192 // PARTS, 8192 // PARTS, pair_sem.at[part])

    for q in range(3):
        low = 4 + q
        base = 8192 + 2048 * q

        @pl.loop(0, LAYERS * 4)
        def _(g):
            d, row = source(BOUNDS[1 + q] + (g // 4) * 16 + pair * 4 + g % 4, low, FIRSTS[low + 1], (window_start(low), window_start(low + 1)))
            at = base * LANES + g * 4096
            if q < 2:
                group = wg_ref[d, pl.ds(row, GROUP)].astype(F32)
                for tile in range(4):
                    wide[g % 4, pl.ds(tile, 8, stride=4)] = group[8 * tile:8 * tile + 8]
            for tile in range(4):
                if q < 2:
                    rows = wide[g % 4, pl.ds(8 * tile, 8)].reshape(1, 1024).astype(BF16)
                else:
                    rows = wg_ref[d, pl.ds(row + 8 * tile, 8)].reshape(1, 1024)
                flat[0:1, pl.ds(pl.multiple_of(at + tile * 1024, 1024), 1024)] = rows

        finish(base, 2048, pair_sem.at[PARTS + q])
    for copy in copies:
        copy.wait()


def place_call(m_new, v_new, w_new, gathered):
    hbm = pl.BlockSpec(memory_space=pl.ANY)
    dma = pltpu.SemaphoreType.DMA
    flat = jax.ShapeDtypeStruct((SLICE_ROWS, LANES), F32)
    return pl.pallas_call(
        place_kernel,
        name='place_weights',
        out_shape=(flat, flat, flat) + tuple(jax.ShapeDtypeStruct((size, LANES), BF16) for size in (32768, 8192, 8192, 8192, 208))
        + (jax.ShapeDtypeStruct((1, PAIR_SIZE), BF16),),
        in_specs=[pl.BlockSpec(memory_space=pltpu.VMEM)] * 4,
        out_specs=[hbm] * 9,
        scratch_shapes=[
            pltpu.VMEM((1, PAIR_SIZE), BF16),
            pltpu.VMEM((4, GROUP, LANES), F32),
            dma((3,)), dma((12,)), dma((PARTS + 3,)),
        ],
        compiler_params=pltpu.CompilerParams(vmem_limit_bytes=12 * 1024 * 1024),
    )(*(pltpu.with_memory_space_constraint(x, pltpu.VMEM) for x in (m_new, v_new, w_new, gathered)))


def to_tiles(tensor):
    return tensor.reshape(256, 8, 4, LANES).transpose(0, 2, 1, 3).reshape(8192, LANES)


def from_tiles(rows):
    return rows.reshape(256, 4, 8, LANES).transpose(0, 2, 1, 3).reshape(16, 128, 512)


def solution(mesh):
    def local_step(g_embed, g_attn, g_ffn_in, g_ffn_out, g_vec, m_shard, v_shard, w_shard):
        vec_rows = jnp.pad(g_vec.reshape(208, LANES), ((0, 16), (0, 0)))
        tensors = (g_embed.reshape(32768, LANES), to_tiles(g_attn), to_tiles(g_ffn_in), g_ffn_out.reshape(8192, LANES), vec_rows)
        state = [shard.reshape(SLICE_ROWS, LANES) for shard in (m_shard, v_shard, w_shard)]
        m_new, v_new, w_new, gathered = step_call(tensors, state)
        m_new, v_new, w_new, embed, attn, ffn_in, ffn_out, vec, w_pair = place_call(m_new, v_new, w_new, gathered)
        wb_vec = vec.reshape(16, 1664)
        pair = lax.axis_index('outer') * 2 + lax.axis_index('middle')
        vec_block = lax.dynamic_slice_in_dim(wb_vec, pair * 416, 416, axis=1).reshape(1, -1)
        w_pair = lax.dynamic_update_slice(w_pair, vec_block, (0, PAIR_SIZE - 6656))
        return (m_new.reshape(-1), v_new.reshape(-1), w_new.reshape(-1), embed, from_tiles(attn), from_tiles(ffn_in),
                ffn_out.reshape(16, 512, 128), wb_vec, w_pair)

    return jax.shard_map(local_step, mesh=mesh, in_specs=(P(MESH_AXES),) * 8, out_specs=(P(MESH_AXES),) * 3 + (P(),) * 5 + (P(MESH_AXES),), check_vma=False)
```

```python
import functools
import math
import jax
import jax.numpy as jnp
from jax import lax
from jax.experimental import pallas as pl
from jax.experimental.pallas import tpu as pltpu
from jax.sharding import PartitionSpec as P

MESH_AXES = ('outer', 'middle', 'inner')
ADAM_BETA1 = 0.9
ADAM_BETA2 = 0.98
ADAM_EPS = 1e-9
LEARN_RATE = 0.05
ADAM_STEP = 3

MESH = pl.DeviceIdType.MESH
F32 = jnp.float32
BF16 = jnp.bfloat16

LANES = 128
GROUP = 32
ROWS = 7366656 // LANES
SLICE_ROWS = ROWS // 8
CHUNKS = 19
CHUNK_GROUPS = 12
CHUNK = CHUNK_GROUPS * GROUP
HALF = CHUNK // 2
RING = 4
WINDOW = CHUNKS * CHUNK
LAST_ROWS = SLICE_ROWS - (CHUNKS - 1) * CHUNK
FRONT = 96
BOUNDS = (0, 1024, 1280, 1536, 1792, 1799)
PERMUTED = (1024, 1536)
START_MAX = BOUNDS[-1] - WINDOW // GROUP


def window_start(device):
    return min(SLICE_ROWS * device // GROUP, START_MAX)


def window_start_traced(device):
    return jnp.minimum(lax.div(device * SLICE_ROWS, GROUP), START_MAX)


def split_chunks():
    found = []
    for device in range(8):
        for chunk in range(CHUNKS):
            first = window_start(device) + chunk * CHUNK_GROUPS
            for tensor in range(4):
                edge = BOUNDS[tensor + 1]
                if first < edge < first + CHUNK_GROUPS:
                    found.append((first, tensor, edge - first))
    return tuple(found)


SPLITS = split_chunks()
FIRSTS = tuple(SLICE_ROWS * d // GROUP for d in range(8)) + (BOUNDS[-1] - 1,)


def step_kernel(e_ref, a_ref, f1_ref, f2_ref, b_ref, m_ref, v_ref, w_ref,
                m_out, v_out, w_out, wg_ref,
                acc, local, p1x, p1y, p2x, p2y, gflat, wflat, m_in,
                local_sem, d2d_send, d2d_recv, p1_send, p1x_recv, p1y_recv, p2_send, p2x_recv, p2y_recv,
                in_sem, ag_send, agx_recv, agy_recv, relay_send, relx_recv, rely_recv, fwd_send, fwd_recv):
    o, m, i = lax.axis_index('outer'), lax.axis_index('middle'), lax.axis_index('inner')
    x_dev, y_dev, p_dev = (o, 1 - m, i), (1 - o, m, i), (o, m, 1 - i)
    places = ((o, m), (o, 1 - m), (1 - o, m), (1 - o, 1 - m))
    mine = [(po * 2 + pm) * 2 + i for po, pm in places]
    theirs = [(po * 2 + pm) * 2 + (1 - i) for po, pm in places]
    start = window_start_traced(mine[0])
    shift = mine[0] * SLICE_ROWS - start * GROUP
    tensors = (e_ref, a_ref, f1_ref, f2_ref, b_ref)

    barrier = pltpu.get_barrier_semaphore()
    for device in (x_dev, y_dev, p_dev):
        pl.semaphore_signal(barrier, inc=1, device_id=device, device_id_type=MESH)
    pl.semaphore_wait(barrier, 3)

    def remote(src, dst, send, recv, device):
        pltpu.make_async_remote_copy(src_ref=src, dst_ref=dst, send_sem=send, recv_sem=recv, device_id=device, device_id_type=MESH).start()

    def drain(ref, sem):
        pltpu.make_async_copy(ref, ref, sem).wait()

    def load_chunk(device, chunk, copy):
        first = window_start_traced(device) + chunk * CHUNK_GROUPS
        for tensor in range(4):
            @pl.when((first >= BOUNDS[tensor]) & (first + CHUNK_GROUPS <= BOUNDS[tensor + 1]))
            def _():
                row = pl.multiple_of((first - BOUNDS[tensor]) * GROUP, GROUP)
                copy(tensors[tensor].at[pl.ds(row, CHUNK)], 0, CHUNK)
        for known, tensor, count in SPLITS:
            @pl.when(first == known)
            def _():
                head = count * GROUP
                copy(tensors[tensor].at[pl.ds((known - BOUNDS[tensor]) * GROUP, head)], 0, head)
                copy(tensors[tensor + 1].at[pl.ds(0, CHUNK - head)], head, CHUNK - head)

    def issue_gradients(chunk):
        slot = lax.rem(chunk, 3)
        base = pl.multiple_of(chunk * CHUNK, CHUNK)
        for j in (3, 1, 2, 0):
            load_chunk(theirs[j], chunk, lambda src, off, size: remote(
                src, acc.at[j, pl.ds(pl.multiple_of(base + off, GROUP), size)], d2d_send, d2d_recv.at[chunk], p_dev))
            load_chunk(mine[j], chunk, lambda src, off, size: pltpu.make_async_copy(
                src, local.at[slot, j, pl.ds(off, size)], local_sem.at[slot]).start())

    def add_rows(j, base, count, term):
        @pl.loop(0, count // GROUP)
        def _(r):
            off = pl.multiple_of(r * GROUP, GROUP)
            at = pl.ds(pl.multiple_of(base + off, GROUP), GROUP)
            acc[j, at] = acc[j, at] + term(off)

    def first_phase(chunk):
        slot = lax.rem(chunk, 3)
        ring = lax.rem(chunk, RING)
        base = pl.multiple_of(chunk * CHUNK, CHUNK)
        second = pl.multiple_of(base + HALF, HALF)
        drain(local.at[slot], local_sem.at[slot])
        drain(local.at[0], d2d_recv.at[chunk])
        add_rows(1, base, HALF, lambda off: local[slot, 1, pl.ds(off, GROUP)])
        add_rows(2, second, HALF, lambda off: local[slot, 2, pl.ds(HALF + off, GROUP)])
        add_rows(3, base, CHUNK, lambda off: local[slot, 3, pl.ds(off, GROUP)])
        remote(acc.at[1, pl.ds(base, HALF)], p1x.at[ring, 0], p1_send.at[0], p1x_recv.at[chunk], x_dev)
        remote(acc.at[2, pl.ds(second, HALF)], p1y.at[ring, 0], p1_send.at[1], p1y_recv.at[chunk], y_dev)
        remote(acc.at[3, pl.ds(base, HALF)], p1x.at[ring, 1], p1_send.at[0], p1x_recv.at[chunk], x_dev)
        remote(acc.at[3, pl.ds(second, HALF)], p1y.at[ring, 1], p1_send.at[1], p1y_recv.at[chunk], y_dev)
        add_rows(2, base, HALF, lambda off: local[slot, 2, pl.ds(off, GROUP)])
        add_rows(1, second, HALF, lambda off: local[slot, 1, pl.ds(HALF + off, GROUP)])
        add_rows(0, base, CHUNK, lambda off: local[slot, 0, pl.ds(off, GROUP)])

    def second_phase(chunk):
        ring = lax.rem(chunk, RING)
        base = pl.multiple_of(chunk * CHUNK, CHUNK)
        second = pl.multiple_of(base + HALF, HALF)
        drain(p1x.at[ring], p1x_recv.at[chunk])
        add_rows(2, base, HALF, lambda off: p1x[ring, 1, pl.ds(off, GROUP)])
        drain(p1y.at[ring], p1y_recv.at[chunk])
        add_rows(1, second, HALF, lambda off: p1y[ring, 1, pl.ds(off, GROUP)])
        remote(acc.at[2, pl.ds(base, HALF)], p2y.at[ring], p2_send.at[0], p2y_recv.at[chunk], y_dev)
        remote(acc.at[1, pl.ds(second, HALF)], p2x.at[ring], p2_send.at[1], p2x_recv.at[chunk], x_dev)
        add_rows(0, base, HALF, lambda off: p1x[ring, 0, pl.ds(off, GROUP)])
        add_rows(0, second, HALF, lambda off: p1y[ring, 0, pl.ds(off, GROUP)])

    def is_permuted(group):
        return (group >= PERMUTED[0]) & (group < PERMUTED[1])

    def last_phase(chunk):
        ring = lax.rem(chunk, RING)
        base = pl.multiple_of(chunk * CHUNK, CHUNK)
        first = start + chunk * CHUNK_GROUPS
        for part, (arrived, sem) in enumerate(((p2y, p2y_recv), (p2x, p2x_recv))):
            drain(arrived.at[ring], sem.at[chunk])

            @pl.loop(0, HALF // GROUP)
            def _(r):
                off = pl.multiple_of(r * GROUP, GROUP)
                row = pl.multiple_of(base + part * HALF + off, GROUP)
                total = acc[0, pl.ds(row, GROUP)] + arrived[ring, pl.ds(off, GROUP)]
                permuted = is_permuted(first + part * (HALF // GROUP) + r)

                @pl.when(permuted)
                def _():
                    for tile in range(4):
                        gflat[pl.ds(row + tile, 8, stride=4)] = total[8 * tile:8 * tile + 8]

                @pl.when(jnp.logical_not(permuted))
                def _():
                    gflat[pl.ds(row, GROUP)] = total

    def state_loads(block, size):
        slot = lax.rem(block, 2)
        at = pl.ds(pl.multiple_of(block * CHUNK, CHUNK), size)
        return [pltpu.make_async_copy(ref.at[at], m_in.at[slot, q, pl.ds(0, size)], in_sem.at[slot, q])
                for q, ref in enumerate((m_ref, v_ref, w_ref))]

    def start_loads(block):
        for last, size in ((False, CHUNK), (True, LAST_ROWS)):
            @pl.when((block == CHUNKS - 1) == last)
            def _():
                for copy in state_loads(block, size):
                    copy.start()

    def wait_loads(block):
        for last, size in ((False, CHUNK), (True, LAST_ROWS)):
            @pl.when((block == CHUNKS - 1) == last)
            def _():
                for copy in state_loads(block, size):
                    copy.wait()

    def adam_rows(slot, base, off, count):
        at = pl.ds(off, count)
        grad = gflat[pl.ds(base + off + shift, count)] / 8
        m_val = ADAM_BETA1 * m_in[slot, 0, at] + (1.0 - ADAM_BETA1) * grad
        v_val = ADAM_BETA2 * m_in[slot, 1, at] + (1.0 - ADAM_BETA2) * (grad * grad)
        m_hat = m_val / (1.0 - ADAM_BETA1 ** ADAM_STEP)
        v_hat = v_val / (1.0 - ADAM_BETA2 ** ADAM_STEP)
        w_val = m_in[slot, 2, at] - LEARN_RATE * m_hat / (jnp.sqrt(v_hat) + ADAM_EPS)
        out = pl.ds(pl.multiple_of(base + off, GROUP), count)
        m_out[out] = m_val
        v_out[out] = v_val
        w_out[out] = w_val
        wflat[pl.ds(pl.multiple_of(FRONT + base + off, GROUP), count)] = w_val

    def adam(block):
        slot = lax.rem(block, 2)
        base = pl.multiple_of(block * CHUNK, CHUNK)
        wait_loads(block)

        @pl.loop(0, jnp.where(block == CHUNKS - 1, LAST_ROWS // GROUP, CHUNK_GROUPS))
        def _(r):
            adam_rows(slot, base, pl.multiple_of(r * GROUP, GROUP), GROUP)

        @pl.when(block == CHUNKS - 1)
        def _():
            adam_rows((CHUNKS - 1) % 2, (CHUNKS - 1) * CHUNK, LAST_ROWS // GROUP * GROUP, LAST_ROWS % GROUP)

        @pl.loop(0, CHUNK_GROUPS)
        def _(r):
            row = pl.multiple_of(base + r * GROUP, GROUP)
            source = FRONT + row - shift
            permuted = is_permuted(start + block * CHUNK_GROUPS + r)

            @pl.when(permuted)
            def _():
                tiles = [wflat[pl.ds(source + tile, 8, stride=4)] for tile in range(4)]
                wg_ref[mine[0], pl.ds(row, GROUP)] = jnp.concatenate(tiles, axis=0).astype(BF16)

            @pl.when(jnp.logical_not(permuted))
            def _():
                wg_ref[mine[0], pl.ds(row, GROUP)] = wflat[pl.ds(source, GROUP)].astype(BF16)

        ours = wg_ref.at[mine[0], pl.ds(base, CHUNK)]
        remote(ours, ours, ag_send.at[0], agx_recv.at[block], x_dev)
        remote(ours, ours, ag_send.at[1], agy_recv.at[block], y_dev)
        remote(ours, ours, fwd_send.at[0], fwd_recv.at[0], p_dev)

    def relay(chunk):
        base = pl.multiple_of(chunk * CHUNK, CHUNK)
        at, head, tail = pl.ds(base, CHUNK), pl.ds(base, HALF), pl.ds(pl.multiple_of(base + HALF, HALF), HALF)
        drain(wg_ref.at[0, pl.ds(0, CHUNK)], agx_recv.at[chunk])
        remote(wg_ref.at[mine[1], head], wg_ref.at[mine[1], head], relay_send.at[0], rely_recv.at[chunk], y_dev)
        remote(wg_ref.at[mine[1], at], wg_ref.at[mine[1], at], fwd_send.at[1], fwd_recv.at[1], p_dev)
        drain(wg_ref.at[0, pl.ds(0, CHUNK)], agy_recv.at[chunk])
        remote(wg_ref.at[mine[2], tail], wg_ref.at[mine[2], tail], relay_send.at[1], relx_recv.at[chunk], x_dev)
        remote(wg_ref.at[mine[2], at], wg_ref.at[mine[2], at], fwd_send.at[2], fwd_recv.at[2], p_dev)

    def forward(chunk):
        base = pl.multiple_of(chunk * CHUNK, CHUNK)
        at = pl.ds(base, CHUNK)
        drain(wg_ref.at[0, pl.ds(0, HALF)], rely_recv.at[chunk])
        drain(wg_ref.at[0, pl.ds(0, HALF)], relx_recv.at[chunk])
        remote(wg_ref.at[mine[3], at], wg_ref.at[mine[3], at], fwd_send.at[3], fwd_recv.at[3], p_dev)

    issue_gradients(0)
    issue_gradients(1)

    stages = ((0, first_phase), (1, second_phase), (2, last_phase), (3, adam), (5, relay), (6, forward))

    @pl.loop(0, CHUNKS + stages[-1][0])
    def _(t):
        @pl.when(t + 2 < CHUNKS)
        def _():
            issue_gradients(t + 2)

        @pl.when((t >= 2) & (t - 2 < CHUNKS))
        def _():
            start_loads(t - 2)

        for lag, stage in stages:
            @pl.when((t >= lag) & (t - lag < CHUNKS))
            def _():
                stage(t - lag)

    drain(acc, d2d_send)
    for q in range(2):
        drain(acc.at[0], p1_send.at[q])
        drain(acc.at[0, pl.ds(0, WINDOW // 2)], p2_send.at[q])
        drain(wg_ref.at[0, pl.ds(0, WINDOW // 2)], relay_send.at[q])
        drain(wg_ref.at[0], ag_send.at[q])
    for q in range(4):
        drain(wg_ref.at[0], fwd_send.at[q])
        drain(wg_ref.at[0], fwd_recv.at[q])

    for d in range(1, 8):
        keep = SLICE_ROWS * d - FIRSTS[d] * GROUP
        row = lax.broadcasted_iota(jnp.int32, (GROUP, LANES), 0)
        if PERMUTED[0] <= FIRSTS[d] < PERMUTED[1]:
            row = 4 * (row % 8) + row // 8
        before = pl.ds((FIRSTS[d] - window_start(d - 1)) * GROUP, GROUP)
        after = pl.ds((FIRSTS[d] - window_start(d)) * GROUP, GROUP)
        wg_ref[d - 1, before] = jnp.where(row < keep, wg_ref[d - 1, before].astype(F32), wg_ref[d, after].astype(F32)).astype(BF16)


def step_call(tensors, state):
    hbm = pl.BlockSpec(memory_space=pl.ANY)
    dma = pltpu.SemaphoreType.DMA
    flat = pltpu.VMEM((SLICE_ROWS, LANES), F32)
    return pl.pallas_call(
        step_kernel,
        name='adam_step',
        out_shape=(flat, flat, flat, pltpu.VMEM((8, WINDOW, LANES), BF16)),
        in_specs=[hbm] * 8,
        out_specs=[pl.BlockSpec(memory_space=pltpu.VMEM)] * 4,
        scratch_shapes=[
            pltpu.VMEM((4, WINDOW, LANES), F32),
            pltpu.VMEM((3, 4, CHUNK, LANES), F32),
            pltpu.VMEM((RING, 2, HALF, LANES), F32),
            pltpu.VMEM((RING, 2, HALF, LANES), F32),
            pltpu.VMEM((RING, HALF, LANES), F32),
            pltpu.VMEM((RING, HALF, LANES), F32),
            pltpu.VMEM((WINDOW + 128, LANES), F32),
            pltpu.VMEM((WINDOW + FRONT, LANES), F32),
            pltpu.VMEM((2, 3, CHUNK, LANES), F32),
            dma((3,)), dma, dma((CHUNKS,)), dma((2,)), dma((CHUNKS,)), dma((CHUNKS,)), dma((2,)), dma((CHUNKS,)), dma((CHUNKS,)),
            dma((2, 3)), dma((2,)), dma((CHUNKS,)), dma((CHUNKS,)), dma((2,)), dma((CHUNKS,)), dma((CHUNKS,)),
            dma((4,)), dma((4,)),
        ],
        compiler_params=pltpu.CompilerParams(collective_id=0, has_side_effects=True, vmem_limit_bytes=32 * 1024 * 1024),
    )(*tensors, *state)


LAYERS = 16
PAIR_ROWS = 8192 + 3 * 2048 + 52
PAIR_SIZE = PAIR_ROWS * LANES
PARTS = 4


def place_kernel(mv_ref, vv_ref, wv_ref, wg_ref, m_out, v_out, w_out, e_ref, a_ref, f1_ref, f2_ref, b_ref, pair_ref, flat, wide, state_sem, out_sem, pair_sem):
    pair = lax.axis_index('outer') * 2 + lax.axis_index('middle')
    copies = []

    def put(src, dst, sem):
        copies.append(pltpu.make_async_copy(src, dst, sem))
        copies[-1].start()

    for q, (src, dst) in enumerate(((mv_ref, m_out), (vv_ref, v_out), (wv_ref, w_out))):
        put(src, dst, state_sem.at[q])
    count = 0
    for d in range(8):
        low, high = (FIRSTS[d] + 1 if d else 0), FIRSTS[d + 1] + 1
        for q, ref in enumerate((e_ref, a_ref, f1_ref, f2_ref, b_ref)):
            begin, end = max(low, BOUNDS[q]), min(high, BOUNDS[q + 1])
            if begin < end:
                offset = (begin - BOUNDS[q]) * GROUP
                size = min((end - begin) * GROUP, ref.shape[0] - offset)
                put(wg_ref.at[d, pl.ds((begin - window_start(d)) * GROUP, size)], ref.at[pl.ds(offset, size)], out_sem.at[count])
                count += 1

    def finish(begin, size, sem):
        put(flat.at[:, pl.ds(begin * LANES, size * LANES)], pair_ref.at[:, pl.ds(begin * LANES, size * LANES)], sem)

    def source(group, low, last, starts):
        late = group > last
        row = (group - jnp.where(late, starts[1], starts[0])) * GROUP
        return low + jnp.where(late, 1, 0), pl.multiple_of(row, GROUP)

    embed_starts = (window_start_traced(pair), window_start_traced(pair + 1))
    for part in range(PARTS):
        @pl.loop(part * 256 // PARTS, (part + 1) * 256 // PARTS, unroll=4)
        def _(g):
            d, row = source(pair * 256 + g, pair, embed_starts[1], embed_starts)
            flat[0:1, pl.ds(pl.multiple_of(g * 4096, 4096), 4096)] = wg_ref[d, pl.ds(row, GROUP)].reshape(1, 4096)

        finish(part * 8192 // PARTS, 8192 // PARTS, pair_sem.at[part])

    for q in (2, 0, 1):
        low = 4 + q
        base = 8192 + 2048 * q

        @pl.loop(0, LAYERS, unroll=2)
        def _(layer):
            for g in range(4):
                d, row = source(BOUNDS[1 + q] + layer * 16 + pair * 4 + g, low, FIRSTS[low + 1], (window_start(low), window_start(low + 1)))
                group = wg_ref[d, pl.ds(row, GROUP)]
                if q < 2:
                    turn = lax.rem(layer, 2)
                    group = group.astype(F32)
                    for tile in range(4):
                        wide[turn, g, pl.ds(tile, 8, stride=4)] = group[8 * tile:8 * tile + 8]
                    group = wide[turn, g].astype(BF16)
                flat[0:1, pl.ds(pl.multiple_of((base + layer * 128 + g * GROUP) * LANES, 4096), 4096)] = group.reshape(1, 4096)

        finish(base, 2048, pair_sem.at[PARTS + q])
    for copy in copies:
        copy.wait()


def place_call(m_new, v_new, w_new, gathered):
    hbm = pl.BlockSpec(memory_space=pl.ANY)
    dma = pltpu.SemaphoreType.DMA
    flat = jax.ShapeDtypeStruct((SLICE_ROWS, LANES), F32)
    return pl.pallas_call(
        place_kernel,
        name='place_weights',
        out_shape=(flat, flat, flat) + tuple(jax.ShapeDtypeStruct((size, LANES), BF16) for size in (32768, 8192, 8192, 8192, 208))
        + (jax.ShapeDtypeStruct((1, PAIR_SIZE), BF16),),
        in_specs=[pl.BlockSpec(memory_space=pltpu.VMEM)] * 4,
        out_specs=[hbm] * 9,
        scratch_shapes=[
            pltpu.VMEM((1, PAIR_SIZE), BF16),
            pltpu.VMEM((2, 4, GROUP, LANES), F32),
            dma((3,)), dma((12,)), dma((PARTS + 3,)),
        ],
        compiler_params=pltpu.CompilerParams(vmem_limit_bytes=12 * 1024 * 1024),
    )(*(pltpu.with_memory_space_constraint(x, pltpu.VMEM) for x in (m_new, v_new, w_new, gathered)))


def to_tiles(tensor):
    return tensor.reshape(256, 8, 4, LANES).transpose(0, 2, 1, 3).reshape(8192, LANES)


def from_tiles(rows):
    return rows.reshape(256, 4, 8, LANES).transpose(0, 2, 1, 3).reshape(16, 128, 512)


def solution(mesh):
    def local_step(g_embed, g_attn, g_ffn_in, g_ffn_out, g_vec, m_shard, v_shard, w_shard):
        vec_rows = jnp.pad(g_vec.reshape(208, LANES), ((0, 16), (0, 0)))
        tensors = (g_embed.reshape(32768, LANES), to_tiles(g_attn), to_tiles(g_ffn_in), g_ffn_out.reshape(8192, LANES), vec_rows)
        state = [shard.reshape(SLICE_ROWS, LANES) for shard in (m_shard, v_shard, w_shard)]
        m_new, v_new, w_new, gathered = step_call(tensors, state)
        m_new, v_new, w_new, embed, attn, ffn_in, ffn_out, vec, w_pair = place_call(m_new, v_new, w_new, gathered)
        wb_vec = vec.reshape(16, 1664)
        pair = lax.axis_index('outer') * 2 + lax.axis_index('middle')
        vec_block = lax.dynamic_slice_in_dim(wb_vec, pair * 416, 416, axis=1).reshape(1, -1)
        w_pair = lax.dynamic_update_slice(w_pair, vec_block, (0, PAIR_SIZE - 6656))
        return (m_new.reshape(-1), v_new.reshape(-1), w_new.reshape(-1), embed, from_tiles(attn), from_tiles(ffn_in),
                ffn_out.reshape(16, 512, 128), wb_vec, w_pair)

    return jax.shard_map(local_step, mesh=mesh, in_specs=(P(MESH_AXES),) * 8, out_specs=(P(MESH_AXES),) * 3 + (P(),) * 5 + (P(MESH_AXES),), check_vma=False)
```

```python
import functools
import math
import jax
import jax.numpy as jnp
from jax import lax
from jax.experimental import pallas as pl
from jax.experimental.pallas import tpu as pltpu
from jax.sharding import PartitionSpec as P

MESH_AXES = ('outer', 'middle', 'inner')
ADAM_BETA1 = 0.9
ADAM_BETA2 = 0.98
ADAM_EPS = 1e-9
LEARN_RATE = 0.05
ADAM_STEP = 3

MESH = pl.DeviceIdType.MESH
F32 = jnp.float32
BF16 = jnp.bfloat16

LANES = 128
GROUP = 32
ROWS = 7366656 // LANES
SLICE_ROWS = ROWS // 8
CHUNK_GROUPS = 12
CHUNK = CHUNK_GROUPS * GROUP
HALF = CHUNK // 2
MAIN = 18
LAST = (6, 4)
CHUNKS = MAIN + len(LAST)
RING = 4
WINDOW_GROUPS = MAIN * CHUNK_GROUPS + sum(LAST)
WINDOW = WINDOW_GROUPS * GROUP
MARGIN = GROUP
BOUNDS = (0, 1024, 1280, 1536, 1792, 1799)
PERMUTED = (1024, 1536)
VEC_ROWS = 208
VEC_AT = (BOUNDS[4] - SLICE_ROWS * 7 // GROUP) * GROUP


def window_start(device):
    return SLICE_ROWS * device // GROUP


def window_start_traced(device):
    return lax.div(device * SLICE_ROWS, GROUP)


def chunk_groups(chunk):
    return CHUNK_GROUPS if chunk < MAIN else LAST[chunk - MAIN]


def chunk_first(chunk):
    return chunk * CHUNK_GROUPS if chunk <= MAIN else MAIN * CHUNK_GROUPS + sum(LAST[:chunk - MAIN])


def pieces(first, groups):
    found = []
    for tensor in range(5):
        low, high = max(first, BOUNDS[tensor]), min(first + groups, BOUNDS[tensor + 1])
        if low < high:
            row, off, size = (low - BOUNDS[tensor]) * GROUP, (low - first) * GROUP, (high - low) * GROUP
            if tensor == 4 and row + size > VEC_ROWS:
                found.append((tensor, 0, off + VEC_ROWS - row, row + size - VEC_ROWS))
                size = VEC_ROWS - row
            found.append((tensor, row, off, size))
    return tuple(found)


def split_chunks(groups):
    spans = [window_start(d) + chunk_first(c) for d in range(8) for c in range(CHUNKS) if chunk_groups(c) == groups]
    return [(first, pieces(first, groups)) for first in spans if len(pieces(first, groups)) > 1 or first >= BOUNDS[4]]


FIRSTS = tuple(SLICE_ROWS * d // GROUP for d in range(8)) + (BOUNDS[-1] - 1,)


def step_kernel(e_ref, a_ref, f1_ref, f2_ref, b_ref, m_ref, v_ref, w_ref,
                m_out, v_out, w_out, wg_ref,
                acc, local, p1x, p1y, p2x, p2y, gflat, wflat, m_in, stage, vec,
                stage_sem, local_sem, d2d_send, d2d_recv, p1_send, p1x_recv, p1y_recv, p2_send, p2x_recv, p2y_recv,
                in_sem, ag_send, agx_recv, agy_recv, relay_send, relx_recv, rely_recv, fwd_send, fwd_recv):
    o, m, i = lax.axis_index('outer'), lax.axis_index('middle'), lax.axis_index('inner')
    x_dev, y_dev, p_dev = (o, 1 - m, i), (1 - o, m, i), (o, m, 1 - i)
    places = ((o, m), (o, 1 - m), (1 - o, m), (1 - o, 1 - m))
    mine = [(po * 2 + pm) * 2 + i for po, pm in places]
    theirs = [(po * 2 + pm) * 2 + (1 - i) for po, pm in places]
    start = window_start_traced(mine[0])
    shift = mine[0] * SLICE_ROWS - start * GROUP
    tensors = (e_ref, a_ref, f1_ref, f2_ref, b_ref)

    barrier = pltpu.get_barrier_semaphore()
    for device in (x_dev, y_dev, p_dev):
        pl.semaphore_signal(barrier, inc=1, device_id=device, device_id_type=MESH)

    def remote(src, dst, send, recv, device):
        pltpu.make_async_remote_copy(src_ref=src, dst_ref=dst, send_sem=send, recv_sem=recv, device_id=device, device_id_type=MESH).start()

    def drain(ref, sem):
        pltpu.make_async_copy(ref, ref, sem).wait()

    def mod(value, base):
        return value % base if isinstance(value, int) else lax.rem(value, base)

    def load_chunk(device, base, size, copy):
        groups = size // GROUP
        first = window_start_traced(device) + (base // GROUP if isinstance(base, int) else lax.div(base, GROUP))
        for tensor in range(4):
            @pl.when((first >= BOUNDS[tensor]) & (first + groups <= BOUNDS[tensor + 1]))
            def _():
                row = pl.multiple_of((first - BOUNDS[tensor]) * GROUP, GROUP)
                copy(tensors[tensor].at[pl.ds(row, size)], 0, size)
        for known, parts in split_chunks(groups):
            @pl.when(first == known)
            def _():
                for tensor, row, off, count in parts:
                    copy(tensors[tensor].at[pl.ds(row, count)], off, count)

    def load_ours(j, chunk, base, size):
        slot = mod(chunk, 3)
        load_chunk(mine[j], base, size, lambda src, off, count: pltpu.make_async_copy(
            src, local.at[slot, j, pl.ds(off, count)], local_sem.at[slot, j]).start())

    def issue_gradients(chunk, base, size):
        for j in (3, 1, 2, 0):
            load_chunk(theirs[j], base, size, lambda src, off, count: remote(
                src, acc.at[j, pl.ds(pl.multiple_of(base + off, 8), count)], d2d_send, d2d_recv.at[chunk, j], p_dev))
            load_ours(j, chunk, base, size)

    def add_rows(j, base, count, term):
        @pl.loop(0, count // GROUP)
        def _(r):
            off = pl.multiple_of(r * GROUP, GROUP)
            at = pl.ds(pl.multiple_of(base + off, GROUP), GROUP)
            acc[j, at] = acc[j, at] + term(off)

    def middle(base, size):
        return base + size // 2 if isinstance(base, int) else pl.multiple_of(base + size // 2, GROUP)

    def first_phase(chunk, base, size):
        slot, ring = mod(chunk, 3), mod(chunk, RING)
        half, second = size // 2, middle(base, size)
        near = pl.ds(0, half)

        def ready(j):
            drain(local.at[0, 0, pl.ds(0, size)], local_sem.at[slot, j])
            drain(local.at[0, 0, pl.ds(0, size)], d2d_recv.at[chunk, j])

        ready(3)
        add_rows(3, base, size, lambda off: local[slot, 3, pl.ds(off, GROUP)])
        remote(acc.at[3, pl.ds(base, half)], p1x.at[ring, 1, near], p1_send.at[0], p1x_recv.at[chunk], x_dev)
        remote(acc.at[3, pl.ds(second, half)], p1y.at[ring, 1, near], p1_send.at[1], p1y_recv.at[chunk], y_dev)
        ready(1)
        add_rows(1, base, half, lambda off: local[slot, 1, pl.ds(off, GROUP)])
        remote(acc.at[1, pl.ds(base, half)], p1x.at[ring, 0, near], p1_send.at[0], p1x_recv.at[chunk], x_dev)
        ready(2)
        add_rows(2, second, half, lambda off: local[slot, 2, pl.ds(half + off, GROUP)])
        remote(acc.at[2, pl.ds(second, half)], p1y.at[ring, 0, near], p1_send.at[1], p1y_recv.at[chunk], y_dev)
        add_rows(1, second, half, lambda off: local[slot, 1, pl.ds(half + off, GROUP)])
        add_rows(2, base, half, lambda off: local[slot, 2, pl.ds(off, GROUP)])
        ready(0)
        add_rows(0, base, size, lambda off: local[slot, 0, pl.ds(off, GROUP)])

    def second_phase(chunk, base, size):
        ring = mod(chunk, RING)
        half, second = size // 2, middle(base, size)
        near = pl.ds(0, half)
        drain(local.at[0, 0, pl.ds(0, size)], p1x_recv.at[chunk])
        add_rows(2, base, half, lambda off: p1x[ring, 1, pl.ds(off, GROUP)])
        drain(local.at[0, 0, pl.ds(0, size)], p1y_recv.at[chunk])
        add_rows(1, second, half, lambda off: p1y[ring, 1, pl.ds(off, GROUP)])
        remote(acc.at[2, pl.ds(base, half)], p2y.at[ring, near], p2_send.at[0], p2y_recv.at[chunk], y_dev)
        remote(acc.at[1, pl.ds(second, half)], p2x.at[ring, near], p2_send.at[1], p2x_recv.at[chunk], x_dev)
        add_rows(0, base, half, lambda off: p1x[ring, 0, pl.ds(off, GROUP)])
        add_rows(0, second, half, lambda off: p1y[ring, 0, pl.ds(off, GROUP)])

    def is_permuted(group):
        return (group >= PERMUTED[0]) & (group < PERMUTED[1])

    def last_phase(chunk, base, size):
        ring = mod(chunk, RING)
        half = size // 2
        first = start + (base // GROUP if isinstance(base, int) else lax.div(base, GROUP))
        for part, (arrived, sem) in enumerate(((p2y, p2y_recv), (p2x, p2x_recv))):
            drain(local.at[0, 0, pl.ds(0, half)], sem.at[chunk])

            @pl.loop(0, half // GROUP)
            def _(r):
                off = pl.multiple_of(r * GROUP, GROUP)
                row = pl.multiple_of(base + part * half + off, GROUP)
                total = acc[0, pl.ds(row, GROUP)] + arrived[ring, pl.ds(off, GROUP)]
                permuted = is_permuted(first + part * (half // GROUP) + r)

                @pl.when(permuted)
                def _():
                    for tile in range(4):
                        gflat[pl.ds(row + tile, 8, stride=4)] = total[8 * tile:8 * tile + 8]

                @pl.when(jnp.logical_not(permuted))
                def _():
                    gflat[pl.ds(row, GROUP)] = total

        if isinstance(chunk, int) and chunk == CHUNKS - 1:
            @pl.when(mine[0] == 7)
            def _():
                vec[...] = gflat[pl.ds(VEC_AT, VEC_ROWS)]
                for tile in range(26):
                    gflat[pl.ds(VEC_AT + tile // 13 * 104 + tile % 13, 8, stride=13)] = vec[8 * tile:8 * tile + 8]

    def state_loads(block, base, size):
        slot = mod(block, 2)
        count = size if not isinstance(base, int) else min(size, SLICE_ROWS - base)
        at = pl.ds(base, count)
        return [pltpu.make_async_copy(ref.at[at], m_in.at[slot, q, pl.ds(0, count)], in_sem.at[slot, q])
                for q, ref in enumerate((m_ref, v_ref, w_ref))]

    def start_loads(block, base, size):
        for copy in state_loads(block, base, size):
            copy.start()

    def adam_rows(slot, base, off, count):
        at = pl.ds(off, count)
        grad = gflat[pl.ds(base + off + shift, count)] / 8
        m_val = ADAM_BETA1 * m_in[slot, 0, at] + (1.0 - ADAM_BETA1) * grad
        v_val = ADAM_BETA2 * m_in[slot, 1, at] + (1.0 - ADAM_BETA2) * (grad * grad)
        m_hat = m_val / (1.0 - ADAM_BETA1 ** ADAM_STEP)
        v_hat = v_val / (1.0 - ADAM_BETA2 ** ADAM_STEP)
        w_val = m_in[slot, 2, at] - LEARN_RATE * m_hat / (jnp.sqrt(v_hat) + ADAM_EPS)
        out = pl.ds(pl.multiple_of(base + off, GROUP), count)
        m_out[out] = m_val
        v_out[out] = v_val
        w_out[out] = w_val
        wflat[pl.ds(pl.multiple_of(MARGIN + base + off, GROUP), count)] = w_val

    def adam(block, base, size):
        slot = mod(block, 2)
        rows = size if not isinstance(base, int) else min(size, SLICE_ROWS - base)
        for copy in state_loads(block, base, size):
            copy.wait()

        @pl.loop(0, rows // GROUP)
        def _(r):
            adam_rows(slot, base, pl.multiple_of(r * GROUP, GROUP), GROUP)

        if rows % GROUP:
            adam_rows(slot, base, rows // GROUP * GROUP, rows % GROUP)
        first = start + (base // GROUP if isinstance(base, int) else lax.div(base, GROUP))

        @pl.loop(0, size // GROUP)
        def _(r):
            row = pl.multiple_of(base + r * GROUP, GROUP)
            source = MARGIN + row - shift
            permuted = is_permuted(first + r)

            @pl.when(permuted)
            def _():
                tiles = [wflat[pl.ds(source + tile, 8, stride=4)] for tile in range(4)]
                wg_ref[mine[0], pl.ds(row, GROUP)] = jnp.concatenate(tiles, axis=0).astype(BF16)

            @pl.when(jnp.logical_not(permuted))
            def _():
                wg_ref[mine[0], pl.ds(row, GROUP)] = wflat[pl.ds(source, GROUP)].astype(BF16)

        if isinstance(base, int) and base + size > VEC_AT:
            @pl.when(mine[0] == 7)
            def _():
                for pair in range(13):
                    row = VEC_AT + 16 * pair
                    if base <= row < base + size:
                        tiles = [wflat[pl.ds(MARGIN + VEC_AT - shift + tile // 13 * 104 + tile % 13, 8, stride=13)] for tile in (2 * pair, 2 * pair + 1)]
                        wg_ref[7, pl.ds(row, 16)] = jnp.concatenate(tiles, axis=0).astype(BF16)

        ours = wg_ref.at[mine[0], pl.ds(base, size)]
        remote(ours, ours, ag_send.at[0], agx_recv.at[block], x_dev)
        remote(ours, ours, ag_send.at[1], agy_recv.at[block], y_dev)
        remote(ours, ours, fwd_send.at[0], fwd_recv.at[0], p_dev)

    def relay(chunk, base, size):
        half = size // 2
        at, head, tail = pl.ds(base, size), pl.ds(base, half), pl.ds(middle(base, size), half)
        drain(wg_ref.at[0, pl.ds(0, size)], agx_recv.at[chunk])
        remote(wg_ref.at[mine[1], head], wg_ref.at[mine[1], head], relay_send.at[0], rely_recv.at[chunk], y_dev)
        remote(wg_ref.at[mine[1], at], wg_ref.at[mine[1], at], fwd_send.at[1], fwd_recv.at[1], p_dev)
        drain(wg_ref.at[0, pl.ds(0, size)], agy_recv.at[chunk])
        remote(wg_ref.at[mine[2], tail], wg_ref.at[mine[2], tail], relay_send.at[1], relx_recv.at[chunk], x_dev)
        remote(wg_ref.at[mine[2], at], wg_ref.at[mine[2], at], fwd_send.at[2], fwd_recv.at[2], p_dev)

    def forward(chunk, base, size):
        half = size // 2
        at = pl.ds(base, size)
        drain(wg_ref.at[0, pl.ds(0, half)], rely_recv.at[chunk])
        drain(wg_ref.at[0, pl.ds(0, half)], relx_recv.at[chunk])
        remote(wg_ref.at[mine[3], at], wg_ref.at[mine[3], at], fwd_send.at[3], fwd_recv.at[3], p_dev)

    for j in (3, 1, 2, 0):
        load_chunk(theirs[j], 0, CHUNK, lambda src, off, count: pltpu.make_async_copy(
            src, stage.at[j, pl.ds(off, count)], stage_sem.at[j]).start())
        load_ours(j, 0, 0, CHUNK)
    pl.semaphore_wait(barrier, 3)
    for j in (3, 1, 2, 0):
        drain(stage.at[j], stage_sem.at[j])
        remote(stage.at[j], acc.at[j, pl.ds(0, CHUNK)], d2d_send, d2d_recv.at[0, j], p_dev)
    issue_gradients(1, CHUNK, CHUNK)

    def run(chunk, action):
        @pl.when((chunk >= 0) & (chunk < MAIN))
        def _():
            action(chunk, pl.multiple_of(chunk * CHUNK, CHUNK), CHUNK)

        for last in range(MAIN, CHUNKS):
            @pl.when(chunk == last)
            def _():
                action(last, chunk_first(last) * GROUP, chunk_groups(last) * GROUP)

    stages = ((-2, issue_gradients), (2, start_loads), (0, first_phase), (1, second_phase), (2, last_phase), (3, adam), (7, relay), (10, forward))

    @pl.loop(0, CHUNKS + stages[-1][0])
    def _(t):
        for lag, action in stages:
            run(t - lag, action)

    drain(acc, d2d_send)
    for q in range(2):
        drain(acc.at[0], p1_send.at[q])
        drain(acc.at[0, pl.ds(0, WINDOW // 2)], p2_send.at[q])
        drain(wg_ref.at[0, pl.ds(0, WINDOW // 2)], relay_send.at[q])
        drain(wg_ref.at[0], ag_send.at[q])
    for q in range(4):
        drain(wg_ref.at[0], fwd_send.at[q])
        drain(wg_ref.at[0], fwd_recv.at[q])

    for d in range(1, 8):
        keep = SLICE_ROWS * d - FIRSTS[d] * GROUP
        row = lax.broadcasted_iota(jnp.int32, (GROUP, LANES), 0)
        if PERMUTED[0] <= FIRSTS[d] < PERMUTED[1]:
            row = 4 * (row % 8) + row // 8
        before = pl.ds((FIRSTS[d] - window_start(d - 1)) * GROUP, GROUP)
        after = pl.ds((FIRSTS[d] - window_start(d)) * GROUP, GROUP)
        wg_ref[d - 1, before] = jnp.where(row < keep, wg_ref[d - 1, before].astype(F32), wg_ref[d, after].astype(F32)).astype(BF16)


def step_call(tensors, state):
    hbm = pl.BlockSpec(memory_space=pl.ANY)
    dma = pltpu.SemaphoreType.DMA
    flat = pltpu.VMEM((SLICE_ROWS, LANES), F32)
    return pl.pallas_call(
        step_kernel,
        name='adam_step',
        out_shape=(flat, flat, flat, pltpu.VMEM((8, WINDOW, LANES), BF16)),
        in_specs=[hbm] * 8,
        out_specs=[pl.BlockSpec(memory_space=pltpu.VMEM)] * 4,
        scratch_shapes=[
            pltpu.VMEM((4, WINDOW, LANES), F32),
            pltpu.VMEM((3, 4, CHUNK, LANES), F32),
            pltpu.VMEM((RING, 2, HALF, LANES), F32),
            pltpu.VMEM((RING, 2, HALF, LANES), F32),
            pltpu.VMEM((RING, HALF, LANES), F32),
            pltpu.VMEM((RING, HALF, LANES), F32),
            pltpu.VMEM((WINDOW + MARGIN, LANES), F32),
            pltpu.VMEM((WINDOW + MARGIN, LANES), F32),
            pltpu.VMEM((2, 3, CHUNK, LANES), F32),
            pltpu.VMEM((4, CHUNK, LANES), F32),
            pltpu.VMEM((VEC_ROWS, LANES), F32),
            dma((4,)), dma((3, 4)), dma, dma((CHUNKS, 4)), dma((2,)), dma((CHUNKS,)), dma((CHUNKS,)), dma((2,)), dma((CHUNKS,)), dma((CHUNKS,)),
            dma((2, 3)), dma((2,)), dma((CHUNKS,)), dma((CHUNKS,)), dma((2,)), dma((CHUNKS,)), dma((CHUNKS,)),
            dma((4,)), dma((4,)),
        ],
        compiler_params=pltpu.CompilerParams(collective_id=0, has_side_effects=True, vmem_limit_bytes=32 * 1024 * 1024),
    )(*tensors, *state)


LAYERS = 16
PAIR_ROWS = 8192 + 3 * 2048 + 52
PAIR_SIZE = PAIR_ROWS * LANES
PARTS = 4


def place_kernel(mv_ref, vv_ref, wv_ref, wg_ref, m_out, v_out, w_out, e_ref, a_ref, f1_ref, f2_ref, b_ref, pair_ref, flat, wide, state_sem, out_sem, pair_sem):
    pair = lax.axis_index('outer') * 2 + lax.axis_index('middle')
    copies = []

    def put(src, dst, sem):
        copies.append(pltpu.make_async_copy(src, dst, sem))
        copies[-1].start()

    for q, (src, dst) in enumerate(((mv_ref, m_out), (vv_ref, v_out), (wv_ref, w_out))):
        put(src, dst, state_sem.at[q])
    count = 0
    for d in range(8):
        low, high = (FIRSTS[d] + 1 if d else 0), FIRSTS[d + 1] + 1
        for q, ref in enumerate((e_ref, a_ref, f1_ref, f2_ref, b_ref)):
            begin, end = max(low, BOUNDS[q]), min(high, BOUNDS[q + 1])
            if begin < end:
                offset = (begin - BOUNDS[q]) * GROUP
                size = min((end - begin) * GROUP, ref.shape[0] - offset)
                put(wg_ref.at[d, pl.ds((begin - window_start(d)) * GROUP, size)], ref.at[pl.ds(offset, size)], out_sem.at[count])
                count += 1

    def finish(begin, size, sem):
        put(flat.at[:, pl.ds(begin * LANES, size * LANES)], pair_ref.at[:, pl.ds(begin * LANES, size * LANES)], sem)

    def source(group, low, last, starts):
        late = group > last
        row = (group - jnp.where(late, starts[1], starts[0])) * GROUP
        return low + jnp.where(late, 1, 0), pl.multiple_of(row, GROUP)

    embed_starts = (window_start_traced(pair), window_start_traced(pair + 1))
    for part in range(PARTS):
        @pl.loop(part * 256 // PARTS, (part + 1) * 256 // PARTS, unroll=4)
        def _(g):
            d, row = source(pair * 256 + g, pair, embed_starts[1], embed_starts)
            flat[0:1, pl.ds(pl.multiple_of(g * 4096, 4096), 4096)] = wg_ref[d, pl.ds(row, GROUP)].reshape(1, 4096)

        finish(part * 8192 // PARTS, 8192 // PARTS, pair_sem.at[part])

    for q in (2, 0, 1):
        low = 4 + q
        base = 8192 + 2048 * q

        @pl.loop(0, LAYERS, unroll=2)
        def _(layer):
            for g in range(4):
                d, row = source(BOUNDS[1 + q] + layer * 16 + pair * 4 + g, low, FIRSTS[low + 1], (window_start(low), window_start(low + 1)))
                group = wg_ref[d, pl.ds(row, GROUP)]
                if q < 2:
                    turn = lax.rem(layer, 2)
                    group = group.astype(F32)
                    for tile in range(4):
                        wide[turn, g, pl.ds(tile, 8, stride=4)] = group[8 * tile:8 * tile + 8]
                    group = wide[turn, g].astype(BF16)
                flat[0:1, pl.ds(pl.multiple_of((base + layer * 128 + g * GROUP) * LANES, 4096), 4096)] = group.reshape(1, 4096)

        finish(base, 2048, pair_sem.at[PARTS + q])
    lines = []
    for half in range(2):
        tiles = [wg_ref[7, pl.ds(pl.multiple_of(VEC_AT + half * 104 + jnp.minimum(3 * pair + tile, 12) * 8, 8), 8)].astype(F32) for tile in range(5)]
        turned = pltpu.roll(jnp.concatenate(tiles, axis=1), 5 * LANES - 32 * pair, 1)
        lines += [turned[line:line + 1, :416] for line in range(8)]
    flat[0:1, pl.ds(14336 * LANES, 52 * LANES)] = jnp.concatenate(lines, axis=1).astype(BF16)
    finish(14336, 52, pair_sem.at[PARTS + 3])
    for copy in copies:
        copy.wait()


def place_call(m_new, v_new, w_new, gathered):
    hbm = pl.BlockSpec(memory_space=pl.ANY)
    dma = pltpu.SemaphoreType.DMA
    flat = jax.ShapeDtypeStruct((SLICE_ROWS, LANES), F32)
    return pl.pallas_call(
        place_kernel,
        name='place_weights',
        out_shape=(flat, flat, flat) + tuple(jax.ShapeDtypeStruct((size, LANES), BF16) for size in (32768, 8192, 8192, 8192, 208))
        + (jax.ShapeDtypeStruct((1, PAIR_SIZE), BF16),),
        in_specs=[pl.BlockSpec(memory_space=pltpu.VMEM)] * 4,
        out_specs=[hbm] * 9,
        scratch_shapes=[
            pltpu.VMEM((1, PAIR_SIZE), BF16),
            pltpu.VMEM((2, 4, GROUP, LANES), F32),
            dma((3,)), dma((12,)), dma((PARTS + 4,)),
        ],
        compiler_params=pltpu.CompilerParams(vmem_limit_bytes=12 * 1024 * 1024),
    )(*(pltpu.with_memory_space_constraint(x, pltpu.VMEM) for x in (m_new, v_new, w_new, gathered)))


def to_tiles(tensor):
    return tensor.reshape(256, 8, 4, LANES).transpose(0, 2, 1, 3).reshape(8192, LANES)


def from_tiles(rows):
    return rows.reshape(256, 4, 8, LANES).transpose(0, 2, 1, 3).reshape(16, 128, 512)


def solution(mesh):
    def local_step(g_embed, g_attn, g_ffn_in, g_ffn_out, g_vec, m_shard, v_shard, w_shard):
        vec_rows = g_vec.reshape(2, 8, 13, LANES).transpose(0, 2, 1, 3).reshape(VEC_ROWS, LANES)
        tensors = (g_embed.reshape(32768, LANES), to_tiles(g_attn), to_tiles(g_ffn_in), g_ffn_out.reshape(8192, LANES), vec_rows)
        state = [shard.reshape(SLICE_ROWS, LANES) for shard in (m_shard, v_shard, w_shard)]
        m_new, v_new, w_new, gathered = step_call(tensors, state)
        m_new, v_new, w_new, embed, attn, ffn_in, ffn_out, vec, w_pair = place_call(m_new, v_new, w_new, gathered)
        wb_vec = vec.reshape(2, 13, 8, LANES).transpose(0, 2, 1, 3).reshape(16, 1664)
        return (m_new.reshape(-1), v_new.reshape(-1), w_new.reshape(-1), embed, from_tiles(attn), from_tiles(ffn_in),
                ffn_out.reshape(16, 512, 128), wb_vec, w_pair)

    return jax.shard_map(local_step, mesh=mesh, in_specs=(P(MESH_AXES),) * 8, out_specs=(P(MESH_AXES),) * 3 + (P(),) * 5 + (P(MESH_AXES),), check_vma=False)
```

```python
import functools
import math
import jax
import jax.numpy as jnp
from jax import lax
from jax.experimental import pallas as pl
from jax.experimental.pallas import tpu as pltpu
from jax.sharding import PartitionSpec as P

MESH_AXES = ('outer', 'middle', 'inner')
ADAM_BETA1 = 0.9
ADAM_BETA2 = 0.98
ADAM_EPS = 1e-9
LEARN_RATE = 0.05
ADAM_STEP = 3

MESH = pl.DeviceIdType.MESH
F32 = jnp.float32
BF16 = jnp.bfloat16

LANES = 128
GROUP = 32
ROWS = 7366656 // LANES
SLICE_ROWS = ROWS // 8
CHUNK_GROUPS = 24
CHUNK = CHUNK_GROUPS * GROUP
HALF = CHUNK // 2
LEAD = (4, 12)
MAIN = 8
LAST = (18,)
SIZES = LEAD + (CHUNK_GROUPS,) * MAIN + LAST
CHUNKS = len(SIZES)
RING = 4
WINDOW_GROUPS = sum(SIZES)
WINDOW = WINDOW_GROUPS * GROUP
MARGIN = GROUP
BOUNDS = (0, 1024, 1280, 1536, 1792, 1799)
PERMUTED = (1024, 1536)
VEC_ROWS = 208
VEC_AT = (BOUNDS[4] - SLICE_ROWS * 7 // GROUP) * GROUP


def window_start(device):
    return SLICE_ROWS * device // GROUP


def window_start_traced(device):
    return lax.div(device * SLICE_ROWS, GROUP)


def chunk_first(chunk):
    return sum(SIZES[:chunk])


def pieces(first, groups):
    found = []
    for tensor in range(5):
        low, high = max(first, BOUNDS[tensor]), min(first + groups, BOUNDS[tensor + 1])
        if low < high:
            row, off, size = (low - BOUNDS[tensor]) * GROUP, (low - first) * GROUP, (high - low) * GROUP
            if tensor == 4 and row + size > VEC_ROWS:
                found.append((tensor, 0, off + VEC_ROWS - row, row + size - VEC_ROWS))
                size = VEC_ROWS - row
            found.append((tensor, row, off, size))
    return tuple(found)


def split_chunks(groups):
    spans = [window_start(d) + chunk_first(c) for d in range(8) for c in range(CHUNKS) if SIZES[c] == groups]
    return [(first, pieces(first, groups)) for first in spans if len(pieces(first, groups)) > 1 or first >= BOUNDS[4]]


FIRSTS = tuple(SLICE_ROWS * d // GROUP for d in range(8)) + (BOUNDS[-1] - 1,)


def step_kernel(e_ref, a_ref, f1_ref, f2_ref, b_ref, m_ref, v_ref, w_ref,
                m_out, v_out, w_out, wg_ref,
                acc, local, p1x, p1y, p2x, p2y, gflat, wflat, m_in, stage, vec,
                stage_sem, local_sem, d2d_send, d2d_recv, p1_send, p1x_recv, p1y_recv, p2_send, p2x_recv, p2y_recv,
                in_sem, ag_send, agx_recv, agy_recv, relay_send, relx_recv, rely_recv, fwd_send, fwd_recv):
    o, m, i = lax.axis_index('outer'), lax.axis_index('middle'), lax.axis_index('inner')
    x_dev, y_dev, p_dev = (o, 1 - m, i), (1 - o, m, i), (o, m, 1 - i)
    places = ((o, m), (o, 1 - m), (1 - o, m), (1 - o, 1 - m))
    mine = [(po * 2 + pm) * 2 + i for po, pm in places]
    theirs = [(po * 2 + pm) * 2 + (1 - i) for po, pm in places]
    start = window_start_traced(mine[0])
    shift = mine[0] * SLICE_ROWS - start * GROUP
    tensors = (e_ref, a_ref, f1_ref, f2_ref, b_ref)

    barrier = pltpu.get_barrier_semaphore()
    for device in (x_dev, y_dev, p_dev):
        pl.semaphore_signal(barrier, inc=1, device_id=device, device_id_type=MESH)

    def remote(src, dst, send, recv, device):
        pltpu.make_async_remote_copy(src_ref=src, dst_ref=dst, send_sem=send, recv_sem=recv, device_id=device, device_id_type=MESH).start()

    def drain(ref, sem):
        pltpu.make_async_copy(ref, ref, sem).wait()

    def mod(value, base):
        return value % base if isinstance(value, int) else lax.rem(value, base)

    def load_chunk(device, base, size, copy):
        groups = size // GROUP
        first = window_start_traced(device) + (base // GROUP if isinstance(base, int) else lax.div(base, GROUP))
        for tensor in range(4):
            @pl.when((first >= BOUNDS[tensor]) & (first + groups <= BOUNDS[tensor + 1]))
            def _():
                row = pl.multiple_of((first - BOUNDS[tensor]) * GROUP, GROUP)
                copy(tensors[tensor].at[pl.ds(row, size)], 0, size)
        for known, parts in split_chunks(groups):
            @pl.when(first == known)
            def _():
                for tensor, row, off, count in parts:
                    copy(tensors[tensor].at[pl.ds(row, count)], off, count)

    def load_ours(j, chunk, base, size):
        slot = mod(chunk, 3)
        load_chunk(mine[j], base, size, lambda src, off, count: pltpu.make_async_copy(
            src, local.at[slot, j, pl.ds(off, count)], local_sem.at[slot, j]).start())

    def issue_gradients(chunk, base, size):
        for j in (3, 1, 2, 0):
            load_chunk(theirs[j], base, size, lambda src, off, count: remote(
                src, acc.at[j, pl.ds(pl.multiple_of(base + off, 8), count)], d2d_send, d2d_recv.at[chunk, j], p_dev))
            load_ours(j, chunk, base, size)

    def add_rows(j, base, count, term):
        @pl.loop(0, count // GROUP)
        def _(r):
            off = pl.multiple_of(r * GROUP, GROUP)
            at = pl.ds(pl.multiple_of(base + off, GROUP), GROUP)
            acc[j, at] = acc[j, at] + term(off)

    def middle(base, size):
        return base + size // 2 if isinstance(base, int) else pl.multiple_of(base + size // 2, GROUP)

    def first_phase(chunk, base, size):
        slot, ring = mod(chunk, 3), mod(chunk, RING)
        half, second = size // 2, middle(base, size)
        near = pl.ds(0, half)

        def ready(j):
            drain(local.at[0, 0, pl.ds(0, size)], local_sem.at[slot, j])
            drain(local.at[0, 0, pl.ds(0, size)], d2d_recv.at[chunk, j])

        ready(3)
        add_rows(3, base, size, lambda off: local[slot, 3, pl.ds(off, GROUP)])
        remote(acc.at[3, pl.ds(base, half)], p1x.at[ring, 1, near], p1_send.at[0], p1x_recv.at[chunk], x_dev)
        remote(acc.at[3, pl.ds(second, half)], p1y.at[ring, 1, near], p1_send.at[1], p1y_recv.at[chunk], y_dev)
        ready(1)
        add_rows(1, base, half, lambda off: local[slot, 1, pl.ds(off, GROUP)])
        remote(acc.at[1, pl.ds(base, half)], p1x.at[ring, 0, near], p1_send.at[0], p1x_recv.at[chunk], x_dev)
        ready(2)
        add_rows(2, second, half, lambda off: local[slot, 2, pl.ds(half + off, GROUP)])
        remote(acc.at[2, pl.ds(second, half)], p1y.at[ring, 0, near], p1_send.at[1], p1y_recv.at[chunk], y_dev)
        add_rows(1, second, half, lambda off: local[slot, 1, pl.ds(half + off, GROUP)])
        add_rows(2, base, half, lambda off: local[slot, 2, pl.ds(off, GROUP)])
        ready(0)
        add_rows(0, base, size, lambda off: local[slot, 0, pl.ds(off, GROUP)])

    def second_phase(chunk, base, size):
        ring = mod(chunk, RING)
        half, second = size // 2, middle(base, size)
        near = pl.ds(0, half)
        drain(local.at[0, 0, pl.ds(0, size)], p1x_recv.at[chunk])
        add_rows(2, base, half, lambda off: p1x[ring, 1, pl.ds(off, GROUP)])
        drain(local.at[0, 0, pl.ds(0, size)], p1y_recv.at[chunk])
        add_rows(1, second, half, lambda off: p1y[ring, 1, pl.ds(off, GROUP)])
        remote(acc.at[2, pl.ds(base, half)], p2y.at[ring, near], p2_send.at[0], p2y_recv.at[chunk], y_dev)
        remote(acc.at[1, pl.ds(second, half)], p2x.at[ring, near], p2_send.at[1], p2x_recv.at[chunk], x_dev)
        add_rows(0, base, half, lambda off: p1x[ring, 0, pl.ds(off, GROUP)])
        add_rows(0, second, half, lambda off: p1y[ring, 0, pl.ds(off, GROUP)])

    def is_permuted(group):
        return (group >= PERMUTED[0]) & (group < PERMUTED[1])

    def last_phase(chunk, base, size):
        ring = mod(chunk, RING)
        half = size // 2
        first = start + (base // GROUP if isinstance(base, int) else lax.div(base, GROUP))
        for part, (arrived, sem) in enumerate(((p2y, p2y_recv), (p2x, p2x_recv))):
            drain(local.at[0, 0, pl.ds(0, half)], sem.at[chunk])

            @pl.loop(0, half // GROUP)
            def _(r):
                off = pl.multiple_of(r * GROUP, GROUP)
                row = pl.multiple_of(base + part * half + off, GROUP)
                total = acc[0, pl.ds(row, GROUP)] + arrived[ring, pl.ds(off, GROUP)]
                permuted = is_permuted(first + part * (half // GROUP) + r)

                @pl.when(permuted)
                def _():
                    for tile in range(4):
                        gflat[pl.ds(row + tile, 8, stride=4)] = total[8 * tile:8 * tile + 8]

                @pl.when(jnp.logical_not(permuted))
                def _():
                    gflat[pl.ds(row, GROUP)] = total

        if isinstance(chunk, int) and chunk == CHUNKS - 1:
            @pl.when(mine[0] == 7)
            def _():
                vec[...] = gflat[pl.ds(VEC_AT, VEC_ROWS)]
                for tile in range(26):
                    gflat[pl.ds(VEC_AT + tile // 13 * 104 + tile % 13, 8, stride=13)] = vec[8 * tile:8 * tile + 8]

    def state_loads(block, base, size):
        slot = mod(block, 2)
        count = size if not isinstance(base, int) else min(size, SLICE_ROWS - base)
        at = pl.ds(base, count)
        return [pltpu.make_async_copy(ref.at[at], m_in.at[slot, q, pl.ds(0, count)], in_sem.at[slot, q])
                for q, ref in enumerate((m_ref, v_ref, w_ref))]

    def start_loads(block, base, size):
        for copy in state_loads(block, base, size):
            copy.start()

    def adam_rows(slot, base, off, count):
        at = pl.ds(off, count)
        grad = gflat[pl.ds(base + off + shift, count)] / 8
        m_val = ADAM_BETA1 * m_in[slot, 0, at] + (1.0 - ADAM_BETA1) * grad
        v_val = ADAM_BETA2 * m_in[slot, 1, at] + (1.0 - ADAM_BETA2) * (grad * grad)
        m_hat = m_val / (1.0 - ADAM_BETA1 ** ADAM_STEP)
        v_hat = v_val / (1.0 - ADAM_BETA2 ** ADAM_STEP)
        w_val = m_in[slot, 2, at] - LEARN_RATE * m_hat / (jnp.sqrt(v_hat) + ADAM_EPS)
        out = pl.ds(pl.multiple_of(base + off, GROUP), count)
        m_out[out] = m_val
        v_out[out] = v_val
        w_out[out] = w_val
        wflat[pl.ds(pl.multiple_of(MARGIN + base + off, GROUP), count)] = w_val

    def adam(block, base, size):
        slot = mod(block, 2)
        rows = size if not isinstance(base, int) else min(size, SLICE_ROWS - base)
        for copy in state_loads(block, base, size):
            copy.wait()

        @pl.loop(0, rows // GROUP)
        def _(r):
            adam_rows(slot, base, pl.multiple_of(r * GROUP, GROUP), GROUP)

        if rows % GROUP:
            adam_rows(slot, base, rows // GROUP * GROUP, rows % GROUP)
        first = start + (base // GROUP if isinstance(base, int) else lax.div(base, GROUP))

        @pl.loop(0, size // GROUP)
        def _(r):
            row = pl.multiple_of(base + r * GROUP, GROUP)
            source = MARGIN + row - shift
            permuted = is_permuted(first + r)

            @pl.when(permuted)
            def _():
                tiles = [wflat[pl.ds(source + tile, 8, stride=4)] for tile in range(4)]
                wg_ref[mine[0], pl.ds(row, GROUP)] = jnp.concatenate(tiles, axis=0).astype(BF16)

            @pl.when(jnp.logical_not(permuted))
            def _():
                wg_ref[mine[0], pl.ds(row, GROUP)] = wflat[pl.ds(source, GROUP)].astype(BF16)

        if isinstance(base, int) and base + size > VEC_AT:
            @pl.when(mine[0] == 7)
            def _():
                for pair in range(13):
                    row = VEC_AT + 16 * pair
                    if base <= row < base + size:
                        tiles = [wflat[pl.ds(MARGIN + VEC_AT - shift + tile // 13 * 104 + tile % 13, 8, stride=13)] for tile in (2 * pair, 2 * pair + 1)]
                        wg_ref[7, pl.ds(row, 16)] = jnp.concatenate(tiles, axis=0).astype(BF16)

        ours = wg_ref.at[mine[0], pl.ds(base, size)]
        remote(ours, ours, ag_send.at[0], agx_recv.at[block], x_dev)
        remote(ours, ours, ag_send.at[1], agy_recv.at[block], y_dev)
        remote(ours, ours, fwd_send.at[0], fwd_recv.at[0], p_dev)

    def relay(chunk, base, size):
        half = size // 2
        at, head, tail = pl.ds(base, size), pl.ds(base, half), pl.ds(middle(base, size), half)
        drain(wg_ref.at[0, pl.ds(0, size)], agx_recv.at[chunk])
        remote(wg_ref.at[mine[1], head], wg_ref.at[mine[1], head], relay_send.at[0], rely_recv.at[chunk], y_dev)
        remote(wg_ref.at[mine[1], at], wg_ref.at[mine[1], at], fwd_send.at[1], fwd_recv.at[1], p_dev)
        drain(wg_ref.at[0, pl.ds(0, size)], agy_recv.at[chunk])
        remote(wg_ref.at[mine[2], tail], wg_ref.at[mine[2], tail], relay_send.at[1], relx_recv.at[chunk], x_dev)
        remote(wg_ref.at[mine[2], at], wg_ref.at[mine[2], at], fwd_send.at[2], fwd_recv.at[2], p_dev)

    def forward(chunk, base, size):
        half = size // 2
        at = pl.ds(base, size)
        drain(wg_ref.at[0, pl.ds(0, half)], rely_recv.at[chunk])
        drain(wg_ref.at[0, pl.ds(0, half)], relx_recv.at[chunk])
        remote(wg_ref.at[mine[3], at], wg_ref.at[mine[3], at], fwd_send.at[3], fwd_recv.at[3], p_dev)

    begin = SIZES[0] * GROUP
    for j in (3, 1, 2, 0):
        load_chunk(theirs[j], 0, begin, lambda src, off, count: pltpu.make_async_copy(
            src, stage.at[j, pl.ds(off, count)], stage_sem.at[j]).start())
        load_ours(j, 0, 0, begin)
    pl.semaphore_wait(barrier, 3)
    for j in (3, 1, 2, 0):
        drain(stage.at[j], stage_sem.at[j])
        remote(stage.at[j], acc.at[j, pl.ds(0, begin)], d2d_send, d2d_recv.at[0, j], p_dev)
    issue_gradients(1, chunk_first(1) * GROUP, SIZES[1] * GROUP)

    def run(chunk, action):
        lead = len(LEAD)

        @pl.when((chunk >= lead) & (chunk < lead + MAIN))
        def _():
            action(chunk, pl.multiple_of(chunk * CHUNK + (sum(LEAD) - lead * CHUNK_GROUPS) * GROUP, GROUP), CHUNK)

        for other in [*range(lead), *range(lead + MAIN, CHUNKS)]:
            @pl.when(chunk == other)
            def _():
                action(other, chunk_first(other) * GROUP, SIZES[other] * GROUP)

    stages = ((-2, issue_gradients), (2, start_loads), (0, first_phase), (1, second_phase), (2, last_phase), (3, adam), (7, relay), (10, forward))

    @pl.loop(0, CHUNKS + stages[-1][0])
    def _(t):
        for lag, action in stages:
            run(t - lag, action)

    drain(acc, d2d_send)
    for q in range(2):
        drain(acc.at[0], p1_send.at[q])
        drain(acc.at[0, pl.ds(0, WINDOW // 2)], p2_send.at[q])
        drain(wg_ref.at[0, pl.ds(0, WINDOW // 2)], relay_send.at[q])
        drain(wg_ref.at[0], ag_send.at[q])
    for q in range(4):
        drain(wg_ref.at[0], fwd_send.at[q])
        drain(wg_ref.at[0], fwd_recv.at[q])

    for d in range(1, 8):
        keep = SLICE_ROWS * d - FIRSTS[d] * GROUP
        row = lax.broadcasted_iota(jnp.int32, (GROUP, LANES), 0)
        if PERMUTED[0] <= FIRSTS[d] < PERMUTED[1]:
            row = 4 * (row % 8) + row // 8
        before = pl.ds((FIRSTS[d] - window_start(d - 1)) * GROUP, GROUP)
        after = pl.ds((FIRSTS[d] - window_start(d)) * GROUP, GROUP)
        wg_ref[d - 1, before] = jnp.where(row < keep, wg_ref[d - 1, before].astype(F32), wg_ref[d, after].astype(F32)).astype(BF16)


def step_call(tensors, state):
    hbm = pl.BlockSpec(memory_space=pl.ANY)
    dma = pltpu.SemaphoreType.DMA
    flat = pltpu.VMEM((SLICE_ROWS, LANES), F32)
    return pl.pallas_call(
        step_kernel,
        name='adam_step',
        out_shape=(flat, flat, flat, pltpu.VMEM((8, WINDOW, LANES), BF16)),
        in_specs=[hbm] * 8,
        out_specs=[pl.BlockSpec(memory_space=pltpu.VMEM)] * 4,
        scratch_shapes=[
            pltpu.VMEM((4, WINDOW, LANES), F32),
            pltpu.VMEM((3, 4, CHUNK, LANES), F32),
            pltpu.VMEM((RING, 2, HALF, LANES), F32),
            pltpu.VMEM((RING, 2, HALF, LANES), F32),
            pltpu.VMEM((RING, HALF, LANES), F32),
            pltpu.VMEM((RING, HALF, LANES), F32),
            pltpu.VMEM((WINDOW + MARGIN, LANES), F32),
            pltpu.VMEM((WINDOW + MARGIN, LANES), F32),
            pltpu.VMEM((2, 3, CHUNK, LANES), F32),
            pltpu.VMEM((4, SIZES[0] * GROUP, LANES), F32),
            pltpu.VMEM((VEC_ROWS, LANES), F32),
            dma((4,)), dma((3, 4)), dma, dma((CHUNKS, 4)), dma((2,)), dma((CHUNKS,)), dma((CHUNKS,)), dma((2,)), dma((CHUNKS,)), dma((CHUNKS,)),
            dma((2, 3)), dma((2,)), dma((CHUNKS,)), dma((CHUNKS,)), dma((2,)), dma((CHUNKS,)), dma((CHUNKS,)),
            dma((4,)), dma((4,)),
        ],
        compiler_params=pltpu.CompilerParams(collective_id=0, has_side_effects=True, vmem_limit_bytes=36 * 1024 * 1024),
    )(*tensors, *state)


LAYERS = 16
PAIR_ROWS = 8192 + 3 * 2048 + 52
PAIR_SIZE = PAIR_ROWS * LANES
PARTS = 4


def place_kernel(mv_ref, vv_ref, wv_ref, wg_ref, m_out, v_out, w_out, e_ref, a_ref, f1_ref, f2_ref, b_ref, pair_ref, flat, wide, state_sem, out_sem, pair_sem):
    pair = lax.axis_index('outer') * 2 + lax.axis_index('middle')
    copies = []

    def put(src, dst, sem):
        copies.append(pltpu.make_async_copy(src, dst, sem))
        copies[-1].start()

    for q, (src, dst) in enumerate(((mv_ref, m_out), (vv_ref, v_out), (wv_ref, w_out))):
        put(src, dst, state_sem.at[q])
    count = 0
    for d in range(8):
        low, high = (FIRSTS[d] + 1 if d else 0), FIRSTS[d + 1] + 1
        for q, ref in enumerate((e_ref, a_ref, f1_ref, f2_ref, b_ref)):
            begin, end = max(low, BOUNDS[q]), min(high, BOUNDS[q + 1])
            if begin < end:
                offset = (begin - BOUNDS[q]) * GROUP
                size = min((end - begin) * GROUP, ref.shape[0] - offset)
                put(wg_ref.at[d, pl.ds((begin - window_start(d)) * GROUP, size)], ref.at[pl.ds(offset, size)], out_sem.at[count])
                count += 1

    def finish(begin, size, sem):
        put(flat.at[:, pl.ds(begin * LANES, size * LANES)], pair_ref.at[:, pl.ds(begin * LANES, size * LANES)], sem)

    def source(group, low, last, starts):
        late = group > last
        row = (group - jnp.where(late, starts[1], starts[0])) * GROUP
        return low + jnp.where(late, 1, 0), pl.multiple_of(row, GROUP)

    embed_starts = (window_start_traced(pair), window_start_traced(pair + 1))
    for part in range(PARTS):
        @pl.loop(part * 256 // PARTS, (part + 1) * 256 // PARTS, unroll=4)
        def _(g):
            d, row = source(pair * 256 + g, pair, embed_starts[1], embed_starts)
            flat[0:1, pl.ds(pl.multiple_of(g * 4096, 4096), 4096)] = wg_ref[d, pl.ds(row, GROUP)].reshape(1, 4096)

        finish(part * 8192 // PARTS, 8192 // PARTS, pair_sem.at[part])

    for q in (2, 0, 1):
        low = 4 + q
        base = 8192 + 2048 * q

        @pl.loop(0, LAYERS, unroll=2)
        def _(layer):
            for g in range(4):
                d, row = source(BOUNDS[1 + q] + layer * 16 + pair * 4 + g, low, FIRSTS[low + 1], (window_start(low), window_start(low + 1)))
                group = wg_ref[d, pl.ds(row, GROUP)]
                if q < 2:
                    turn = lax.rem(layer, 2)
                    group = group.astype(F32)
                    for tile in range(4):
                        wide[turn, g, pl.ds(tile, 8, stride=4)] = group[8 * tile:8 * tile + 8]
                    group = wide[turn, g].astype(BF16)
                flat[0:1, pl.ds(pl.multiple_of((base + layer * 128 + g * GROUP) * LANES, 4096), 4096)] = group.reshape(1, 4096)

        finish(base, 2048, pair_sem.at[PARTS + q])
    lines = []
    for half in range(2):
        tiles = [wg_ref[7, pl.ds(pl.multiple_of(VEC_AT + half * 104 + jnp.minimum(3 * pair + tile, 12) * 8, 8), 8)].astype(F32) for tile in range(5)]
        turned = pltpu.roll(jnp.concatenate(tiles, axis=1), 5 * LANES - 32 * pair, 1)
        lines += [turned[line:line + 1, :416] for line in range(8)]
    flat[0:1, pl.ds(14336 * LANES, 52 * LANES)] = jnp.concatenate(lines, axis=1).astype(BF16)
    finish(14336, 52, pair_sem.at[PARTS + 3])
    for copy in copies:
        copy.wait()


def place_call(m_new, v_new, w_new, gathered):
    hbm = pl.BlockSpec(memory_space=pl.ANY)
    dma = pltpu.SemaphoreType.DMA
    flat = jax.ShapeDtypeStruct((SLICE_ROWS, LANES), F32)
    return pl.pallas_call(
        place_kernel,
        name='place_weights',
        out_shape=(flat, flat, flat) + tuple(jax.ShapeDtypeStruct((size, LANES), BF16) for size in (32768, 8192, 8192, 8192, 208))
        + (jax.ShapeDtypeStruct((1, PAIR_SIZE), BF16),),
        in_specs=[pl.BlockSpec(memory_space=pltpu.VMEM)] * 4,
        out_specs=[hbm] * 9,
        scratch_shapes=[
            pltpu.VMEM((1, PAIR_SIZE), BF16),
            pltpu.VMEM((2, 4, GROUP, LANES), F32),
            dma((3,)), dma((12,)), dma((PARTS + 4,)),
        ],
        compiler_params=pltpu.CompilerParams(vmem_limit_bytes=12 * 1024 * 1024),
    )(*(pltpu.with_memory_space_constraint(x, pltpu.VMEM) for x in (m_new, v_new, w_new, gathered)))


def to_tiles(tensor):
    return tensor.reshape(256, 8, 4, LANES).transpose(0, 2, 1, 3).reshape(8192, LANES)


def from_tiles(rows):
    return rows.reshape(256, 4, 8, LANES).transpose(0, 2, 1, 3).reshape(16, 128, 512)


def solution(mesh):
    def local_step(g_embed, g_attn, g_ffn_in, g_ffn_out, g_vec, m_shard, v_shard, w_shard):
        vec_rows = g_vec.reshape(2, 8, 13, LANES).transpose(0, 2, 1, 3).reshape(VEC_ROWS, LANES)
        tensors = (g_embed.reshape(32768, LANES), to_tiles(g_attn), to_tiles(g_ffn_in), g_ffn_out.reshape(8192, LANES), vec_rows)
        state = [shard.reshape(SLICE_ROWS, LANES) for shard in (m_shard, v_shard, w_shard)]
        m_new, v_new, w_new, gathered = step_call(tensors, state)
        m_new, v_new, w_new, embed, attn, ffn_in, ffn_out, vec, w_pair = place_call(m_new, v_new, w_new, gathered)
        wb_vec = vec.reshape(2, 13, 8, LANES).transpose(0, 2, 1, 3).reshape(16, 1664)
        return (m_new.reshape(-1), v_new.reshape(-1), w_new.reshape(-1), embed, from_tiles(attn), from_tiles(ffn_in),
                ffn_out.reshape(16, 512, 128), wb_vec, w_pair)

    return jax.shard_map(local_step, mesh=mesh, in_specs=(P(MESH_AXES),) * 8, out_specs=(P(MESH_AXES),) * 3 + (P(),) * 5 + (P(MESH_AXES),), check_vma=False)
```

```python
import functools
import math
import jax
import jax.numpy as jnp
from jax import lax
from jax.experimental import pallas as pl
from jax.experimental.pallas import tpu as pltpu
from jax.sharding import PartitionSpec as P

MESH_AXES = ('outer', 'middle', 'inner')
ADAM_BETA1 = 0.9
ADAM_BETA2 = 0.98
ADAM_EPS = 1e-9
LEARN_RATE = 0.05
ADAM_STEP = 3
STEP_RATE = LEARN_RATE / (1.0 - ADAM_BETA1 ** ADAM_STEP)

MESH = pl.DeviceIdType.MESH
F32 = jnp.float32
BF16 = jnp.bfloat16

LANES = 128
GROUP = 32
ROWS = 7366656 // LANES
SLICE_ROWS = ROWS // 8
CHUNK_GROUPS = 24
CHUNK = CHUNK_GROUPS * GROUP
HALF = CHUNK // 2
LEAD = (4, 12)
MAIN = 8
LAST = (18,)
SIZES = LEAD + (CHUNK_GROUPS,) * MAIN + LAST
CHUNKS = len(SIZES)
RING = 4
WINDOW_GROUPS = sum(SIZES)
WINDOW = WINDOW_GROUPS * GROUP
MARGIN = GROUP
BOUNDS = (0, 1024, 1280, 1536, 1792, 1799)
PERMUTED = (1024, 1536)
VEC_ROWS = 208
VEC_AT = (BOUNDS[4] - SLICE_ROWS * 7 // GROUP) * GROUP


def window_start(device):
    return SLICE_ROWS * device // GROUP


def window_start_traced(device):
    return lax.div(device * SLICE_ROWS, GROUP)


def chunk_first(chunk):
    return sum(SIZES[:chunk])


def pieces(first, groups):
    found = []
    for tensor in range(5):
        low, high = max(first, BOUNDS[tensor]), min(first + groups, BOUNDS[tensor + 1])
        if low < high:
            row, off, size = (low - BOUNDS[tensor]) * GROUP, (low - first) * GROUP, (high - low) * GROUP
            if tensor == 4 and row + size > VEC_ROWS:
                found.append((tensor, 0, off + VEC_ROWS - row, row + size - VEC_ROWS))
                size = VEC_ROWS - row
            found.append((tensor, row, off, size))
    return tuple(found)


def split_chunks(groups):
    spans = [window_start(d) + chunk_first(c) for d in range(8) for c in range(CHUNKS) if SIZES[c] == groups]
    return [(first, pieces(first, groups)) for first in spans if len(pieces(first, groups)) > 1 or first >= BOUNDS[4]]


FIRSTS = tuple(SLICE_ROWS * d // GROUP for d in range(8)) + (BOUNDS[-1] - 1,)


def step_kernel(e_ref, a_ref, f1_ref, f2_ref, b_ref, m_ref, v_ref, w_ref,
                m_out, v_out, w_out, wg_ref,
                acc, local, p1x, p1y, p2x, p2y, gflat, wflat, m_in, stage, vec,
                stage_sem, local_sem, d2d_send, d2d_recv, p1_send, p1x_recv, p1y_recv, p2_send, p2x_recv, p2y_recv,
                in_sem, ag_send, agx_recv, agy_recv, relay_send, relx_recv, rely_recv, fwd_send, fwd_recv):
    o, m, i = lax.axis_index('outer'), lax.axis_index('middle'), lax.axis_index('inner')
    x_dev, y_dev, p_dev = (o, 1 - m, i), (1 - o, m, i), (o, m, 1 - i)
    places = ((o, m), (o, 1 - m), (1 - o, m), (1 - o, 1 - m))
    mine = [(po * 2 + pm) * 2 + i for po, pm in places]
    theirs = [(po * 2 + pm) * 2 + (1 - i) for po, pm in places]
    start = window_start_traced(mine[0])
    shift = mine[0] * SLICE_ROWS - start * GROUP
    tensors = (e_ref, a_ref, f1_ref, f2_ref, b_ref)

    barrier = pltpu.get_barrier_semaphore()
    for device in (x_dev, y_dev, p_dev):
        pl.semaphore_signal(barrier, inc=1, device_id=device, device_id_type=MESH)

    def remote(src, dst, send, recv, device):
        pltpu.make_async_remote_copy(src_ref=src, dst_ref=dst, send_sem=send, recv_sem=recv, device_id=device, device_id_type=MESH).start()

    def drain(ref, sem):
        pltpu.make_async_copy(ref, ref, sem).wait()

    def mod(value, base):
        return value % base if isinstance(value, int) else lax.rem(value, base)

    def load_chunk(device, base, size, copy):
        groups = size // GROUP
        first = window_start_traced(device) + (base // GROUP if isinstance(base, int) else lax.div(base, GROUP))
        for tensor in range(4):
            @pl.when((first >= BOUNDS[tensor]) & (first + groups <= BOUNDS[tensor + 1]))
            def _():
                row = pl.multiple_of((first - BOUNDS[tensor]) * GROUP, GROUP)
                copy(tensors[tensor].at[pl.ds(row, size)], 0, size)
        for known, parts in split_chunks(groups):
            @pl.when(first == known)
            def _():
                for tensor, row, off, count in parts:
                    copy(tensors[tensor].at[pl.ds(row, count)], off, count)

    def load_ours(j, chunk, base, size):
        slot = mod(chunk, 3)
        load_chunk(mine[j], base, size, lambda src, off, count: pltpu.make_async_copy(
            src, local.at[slot, j, pl.ds(off, count)], local_sem.at[slot, j]).start())

    def issue_gradients(chunk, base, size):
        for j in (3, 1, 2, 0):
            load_chunk(theirs[j], base, size, lambda src, off, count: remote(
                src, acc.at[j, pl.ds(pl.multiple_of(base + off, 8), count)], d2d_send, d2d_recv.at[chunk, j], p_dev))
            load_ours(j, chunk, base, size)

    def add_rows(j, base, count, term):
        @pl.loop(0, count // GROUP)
        def _(r):
            off = pl.multiple_of(r * GROUP, GROUP)
            at = pl.ds(pl.multiple_of(base + off, GROUP), GROUP)
            acc[j, at] = acc[j, at] + term(off)

    def middle(base, size):
        return base + size // 2 if isinstance(base, int) else pl.multiple_of(base + size // 2, GROUP)

    def first_phase(chunk, base, size):
        slot, ring = mod(chunk, 3), mod(chunk, RING)
        half, second = size // 2, middle(base, size)
        near = pl.ds(0, half)

        def ready(j):
            drain(local.at[0, 0, pl.ds(0, size)], local_sem.at[slot, j])
            drain(local.at[0, 0, pl.ds(0, size)], d2d_recv.at[chunk, j])

        ready(3)
        add_rows(3, base, size, lambda off: local[slot, 3, pl.ds(off, GROUP)])
        remote(acc.at[3, pl.ds(base, half)], p1x.at[ring, 1, near], p1_send.at[0], p1x_recv.at[chunk], x_dev)
        remote(acc.at[3, pl.ds(second, half)], p1y.at[ring, 1, near], p1_send.at[1], p1y_recv.at[chunk], y_dev)
        ready(1)
        add_rows(1, base, half, lambda off: local[slot, 1, pl.ds(off, GROUP)])
        remote(acc.at[1, pl.ds(base, half)], p1x.at[ring, 0, near], p1_send.at[0], p1x_recv.at[chunk], x_dev)
        ready(2)
        add_rows(2, second, half, lambda off: local[slot, 2, pl.ds(half + off, GROUP)])
        remote(acc.at[2, pl.ds(second, half)], p1y.at[ring, 0, near], p1_send.at[1], p1y_recv.at[chunk], y_dev)
        add_rows(1, second, half, lambda off: local[slot, 1, pl.ds(half + off, GROUP)])
        add_rows(2, base, half, lambda off: local[slot, 2, pl.ds(off, GROUP)])
        ready(0)
        add_rows(0, base, size, lambda off: local[slot, 0, pl.ds(off, GROUP)])

    def second_phase(chunk, base, size):
        ring = mod(chunk, RING)
        half, second = size // 2, middle(base, size)
        near = pl.ds(0, half)
        drain(local.at[0, 0, pl.ds(0, size)], p1x_recv.at[chunk])
        add_rows(2, base, half, lambda off: p1x[ring, 1, pl.ds(off, GROUP)])
        drain(local.at[0, 0, pl.ds(0, size)], p1y_recv.at[chunk])
        add_rows(1, second, half, lambda off: p1y[ring, 1, pl.ds(off, GROUP)])
        remote(acc.at[2, pl.ds(base, half)], p2y.at[ring, near], p2_send.at[0], p2y_recv.at[chunk], y_dev)
        remote(acc.at[1, pl.ds(second, half)], p2x.at[ring, near], p2_send.at[1], p2x_recv.at[chunk], x_dev)
        add_rows(0, base, half, lambda off: p1x[ring, 0, pl.ds(off, GROUP)])
        add_rows(0, second, half, lambda off: p1y[ring, 0, pl.ds(off, GROUP)])

    def is_permuted(group):
        return (group >= PERMUTED[0]) & (group < PERMUTED[1])

    def last_phase(chunk, base, size):
        ring = mod(chunk, RING)
        half = size // 2
        first = start + (base // GROUP if isinstance(base, int) else lax.div(base, GROUP))
        for part, (arrived, sem) in enumerate(((p2y, p2y_recv), (p2x, p2x_recv))):
            drain(local.at[0, 0, pl.ds(0, half)], sem.at[chunk])

            @pl.loop(0, half // GROUP)
            def _(r):
                off = pl.multiple_of(r * GROUP, GROUP)
                row = pl.multiple_of(base + part * half + off, GROUP)
                total = acc[0, pl.ds(row, GROUP)] + arrived[ring, pl.ds(off, GROUP)]
                permuted = is_permuted(first + part * (half // GROUP) + r)

                @pl.when(permuted)
                def _():
                    for tile in range(4):
                        gflat[pl.ds(row + tile, 8, stride=4)] = total[8 * tile:8 * tile + 8]

                @pl.when(jnp.logical_not(permuted))
                def _():
                    gflat[pl.ds(row, GROUP)] = total

        if isinstance(chunk, int) and chunk == CHUNKS - 1:
            @pl.when(mine[0] == 7)
            def _():
                vec[...] = gflat[pl.ds(VEC_AT, VEC_ROWS)]
                for tile in range(26):
                    gflat[pl.ds(VEC_AT + tile // 13 * 104 + tile % 13, 8, stride=13)] = vec[8 * tile:8 * tile + 8]

    def state_loads(block, base, size):
        slot = mod(block, 2)
        count = size if not isinstance(base, int) else min(size, SLICE_ROWS - base)
        at = pl.ds(base, count)
        return [pltpu.make_async_copy(ref.at[at], m_in.at[slot, q, pl.ds(0, count)], in_sem.at[slot, q])
                for q, ref in enumerate((m_ref, v_ref, w_ref))]

    def start_loads(block, base, size):
        for copy in state_loads(block, base, size):
            copy.start()

    def adam_rows(slot, base, off, count):
        at = pl.ds(off, count)
        grad = gflat[pl.ds(base + off + shift, count)] / 8
        m_val = ADAM_BETA1 * m_in[slot, 0, at] + (1.0 - ADAM_BETA1) * grad
        v_val = ADAM_BETA2 * m_in[slot, 1, at] + (1.0 - ADAM_BETA2) * (grad * grad)
        v_hat = v_val / (1.0 - ADAM_BETA2 ** ADAM_STEP)
        w_val = m_in[slot, 2, at] - STEP_RATE * m_val / (jnp.sqrt(v_hat) + ADAM_EPS)
        out = pl.ds(pl.multiple_of(base + off, GROUP), count)
        m_out[out] = m_val
        v_out[out] = v_val
        w_out[out] = w_val
        wflat[pl.ds(pl.multiple_of(MARGIN + base + off, GROUP), count)] = w_val

    def adam(block, base, size):
        slot = mod(block, 2)
        rows = size if not isinstance(base, int) else min(size, SLICE_ROWS - base)
        for copy in state_loads(block, base, size):
            copy.wait()

        @pl.loop(0, rows // GROUP)
        def _(r):
            adam_rows(slot, base, pl.multiple_of(r * GROUP, GROUP), GROUP)

        if rows % GROUP:
            adam_rows(slot, base, rows // GROUP * GROUP, rows % GROUP)
        first = start + (base // GROUP if isinstance(base, int) else lax.div(base, GROUP))

        @pl.loop(0, size // GROUP)
        def _(r):
            row = pl.multiple_of(base + r * GROUP, GROUP)
            source = MARGIN + row - shift
            permuted = is_permuted(first + r)

            @pl.when(permuted)
            def _():
                tiles = [wflat[pl.ds(source + tile, 8, stride=4)] for tile in range(4)]
                wg_ref[mine[0], pl.ds(row, GROUP)] = jnp.concatenate(tiles, axis=0).astype(BF16)

            @pl.when(jnp.logical_not(permuted))
            def _():
                wg_ref[mine[0], pl.ds(row, GROUP)] = wflat[pl.ds(source, GROUP)].astype(BF16)

        if isinstance(base, int) and base + size > VEC_AT:
            @pl.when(mine[0] == 7)
            def _():
                for pair in range(13):
                    row = VEC_AT + 16 * pair
                    if base <= row < base + size:
                        tiles = [wflat[pl.ds(MARGIN + VEC_AT - shift + tile // 13 * 104 + tile % 13, 8, stride=13)] for tile in (2 * pair, 2 * pair + 1)]
                        wg_ref[7, pl.ds(row, 16)] = jnp.concatenate(tiles, axis=0).astype(BF16)

        ours = wg_ref.at[mine[0], pl.ds(base, size)]
        remote(ours, ours, ag_send.at[0], agx_recv.at[block], x_dev)
        remote(ours, ours, ag_send.at[1], agy_recv.at[block], y_dev)
        remote(ours, ours, fwd_send.at[0], fwd_recv.at[0], p_dev)

    def relay(chunk, base, size):
        half = size // 2
        at, head, tail = pl.ds(base, size), pl.ds(base, half), pl.ds(middle(base, size), half)
        drain(wg_ref.at[0, pl.ds(0, size)], agx_recv.at[chunk])
        remote(wg_ref.at[mine[1], head], wg_ref.at[mine[1], head], relay_send.at[0], rely_recv.at[chunk], y_dev)
        remote(wg_ref.at[mine[1], at], wg_ref.at[mine[1], at], fwd_send.at[1], fwd_recv.at[1], p_dev)
        drain(wg_ref.at[0, pl.ds(0, size)], agy_recv.at[chunk])
        remote(wg_ref.at[mine[2], tail], wg_ref.at[mine[2], tail], relay_send.at[1], relx_recv.at[chunk], x_dev)
        remote(wg_ref.at[mine[2], at], wg_ref.at[mine[2], at], fwd_send.at[2], fwd_recv.at[2], p_dev)

    def forward(chunk, base, size):
        half = size // 2
        at = pl.ds(base, size)
        drain(wg_ref.at[0, pl.ds(0, half)], rely_recv.at[chunk])
        drain(wg_ref.at[0, pl.ds(0, half)], relx_recv.at[chunk])
        remote(wg_ref.at[mine[3], at], wg_ref.at[mine[3], at], fwd_send.at[3], fwd_recv.at[3], p_dev)

    begin = SIZES[0] * GROUP
    for j in (3, 1, 2, 0):
        load_chunk(theirs[j], 0, begin, lambda src, off, count: pltpu.make_async_copy(
            src, stage.at[j, pl.ds(off, count)], stage_sem.at[j]).start())
        load_ours(j, 0, 0, begin)
    pl.semaphore_wait(barrier, 3)
    for j in (3, 1, 2, 0):
        drain(stage.at[j], stage_sem.at[j])
        remote(stage.at[j], acc.at[j, pl.ds(0, begin)], d2d_send, d2d_recv.at[0, j], p_dev)
    issue_gradients(1, chunk_first(1) * GROUP, SIZES[1] * GROUP)

    def run(chunk, action):
        lead = len(LEAD)

        @pl.when((chunk >= lead) & (chunk < lead + MAIN))
        def _():
            action(chunk, pl.multiple_of(chunk * CHUNK + (sum(LEAD) - lead * CHUNK_GROUPS) * GROUP, GROUP), CHUNK)

        for other in [*range(lead), *range(lead + MAIN, CHUNKS)]:
            @pl.when(chunk == other)
            def _():
                action(other, chunk_first(other) * GROUP, SIZES[other] * GROUP)

    stages = ((-2, issue_gradients), (2, start_loads), (0, first_phase), (1, second_phase), (2, last_phase), (3, adam), (7, relay), (10, forward))

    @pl.loop(0, CHUNKS + stages[-1][0])
    def _(t):
        for lag, action in stages:
            run(t - lag, action)

    drain(acc, d2d_send)
    for q in range(2):
        drain(acc.at[0], p1_send.at[q])
        drain(acc.at[0, pl.ds(0, WINDOW // 2)], p2_send.at[q])
        drain(wg_ref.at[0, pl.ds(0, WINDOW // 2)], relay_send.at[q])
        drain(wg_ref.at[0], ag_send.at[q])
    for q in range(4):
        drain(wg_ref.at[0], fwd_send.at[q])
        drain(wg_ref.at[0], fwd_recv.at[q])

    for d in range(1, 8):
        keep = SLICE_ROWS * d - FIRSTS[d] * GROUP
        row = lax.broadcasted_iota(jnp.int32, (GROUP, LANES), 0)
        if PERMUTED[0] <= FIRSTS[d] < PERMUTED[1]:
            row = 4 * (row % 8) + row // 8
        before = pl.ds((FIRSTS[d] - window_start(d - 1)) * GROUP, GROUP)
        after = pl.ds((FIRSTS[d] - window_start(d)) * GROUP, GROUP)
        wg_ref[d - 1, before] = jnp.where(row < keep, wg_ref[d - 1, before].astype(F32), wg_ref[d, after].astype(F32)).astype(BF16)


def step_call(tensors, state):
    hbm = pl.BlockSpec(memory_space=pl.ANY)
    dma = pltpu.SemaphoreType.DMA
    flat = pltpu.VMEM((SLICE_ROWS, LANES), F32)
    return pl.pallas_call(
        step_kernel,
        name='adam_step',
        out_shape=(flat, flat, flat, pltpu.VMEM((8, WINDOW, LANES), BF16)),
        in_specs=[hbm] * 8,
        out_specs=[pl.BlockSpec(memory_space=pltpu.VMEM)] * 4,
        scratch_shapes=[
            pltpu.VMEM((4, WINDOW, LANES), F32),
            pltpu.VMEM((3, 4, CHUNK, LANES), F32),
            pltpu.VMEM((RING, 2, HALF, LANES), F32),
            pltpu.VMEM((RING, 2, HALF, LANES), F32),
            pltpu.VMEM((RING, HALF, LANES), F32),
            pltpu.VMEM((RING, HALF, LANES), F32),
            pltpu.VMEM((WINDOW + MARGIN, LANES), F32),
            pltpu.VMEM((WINDOW + MARGIN, LANES), F32),
            pltpu.VMEM((2, 3, CHUNK, LANES), F32),
            pltpu.VMEM((4, SIZES[0] * GROUP, LANES), F32),
            pltpu.VMEM((VEC_ROWS, LANES), F32),
            dma((4,)), dma((3, 4)), dma, dma((CHUNKS, 4)), dma((2,)), dma((CHUNKS,)), dma((CHUNKS,)), dma((2,)), dma((CHUNKS,)), dma((CHUNKS,)),
            dma((2, 3)), dma((2,)), dma((CHUNKS,)), dma((CHUNKS,)), dma((2,)), dma((CHUNKS,)), dma((CHUNKS,)),
            dma((4,)), dma((4,)),
        ],
        compiler_params=pltpu.CompilerParams(collective_id=0, has_side_effects=True, vmem_limit_bytes=36 * 1024 * 1024),
    )(*tensors, *state)


LAYERS = 16
PAIR_ROWS = 8192 + 3 * 2048 + 52
PAIR_SIZE = PAIR_ROWS * LANES
PARTS = 4


def place_kernel(mv_ref, vv_ref, wv_ref, wg_ref, m_out, v_out, w_out, e_ref, a_ref, f1_ref, f2_ref, b_ref, pair_ref, flat, wide, state_sem, out_sem, pair_sem):
    pair = lax.axis_index('outer') * 2 + lax.axis_index('middle')
    copies = []

    def put(src, dst, sem):
        copies.append(pltpu.make_async_copy(src, dst, sem))
        copies[-1].start()

    for q, (src, dst) in enumerate(((mv_ref, m_out), (vv_ref, v_out), (wv_ref, w_out))):
        put(src, dst, state_sem.at[q])
    count = 0
    for d in range(8):
        low, high = (FIRSTS[d] + 1 if d else 0), FIRSTS[d + 1] + 1
        for q, ref in enumerate((e_ref, a_ref, f1_ref, f2_ref, b_ref)):
            begin, end = max(low, BOUNDS[q]), min(high, BOUNDS[q + 1])
            if begin < end:
                offset = (begin - BOUNDS[q]) * GROUP
                size = min((end - begin) * GROUP, ref.shape[0] - offset)
                put(wg_ref.at[d, pl.ds((begin - window_start(d)) * GROUP, size)], ref.at[pl.ds(offset, size)], out_sem.at[count])
                count += 1

    def finish(begin, size, sem):
        put(flat.at[:, pl.ds(begin * LANES, size * LANES)], pair_ref.at[:, pl.ds(begin * LANES, size * LANES)], sem)

    def source(group, low, last, starts):
        late = group > last
        row = (group - jnp.where(late, starts[1], starts[0])) * GROUP
        return low + jnp.where(late, 1, 0), pl.multiple_of(row, GROUP)

    embed_starts = (window_start_traced(pair), window_start_traced(pair + 1))
    for part in range(PARTS):
        @pl.loop(part * 256 // PARTS, (part + 1) * 256 // PARTS, unroll=4)
        def _(g):
            d, row = source(pair * 256 + g, pair, embed_starts[1], embed_starts)
            flat[0:1, pl.ds(pl.multiple_of(g * 4096, 4096), 4096)] = wg_ref[d, pl.ds(row, GROUP)].reshape(1, 4096)

        finish(part * 8192 // PARTS, 8192 // PARTS, pair_sem.at[part])

    for q in (2, 0, 1):
        low = 4 + q
        base = 8192 + 2048 * q

        @pl.loop(0, LAYERS, unroll=2)
        def _(layer):
            for g in range(4):
                d, row = source(BOUNDS[1 + q] + layer * 16 + pair * 4 + g, low, FIRSTS[low + 1], (window_start(low), window_start(low + 1)))
                group = wg_ref[d, pl.ds(row, GROUP)]
                if q < 2:
                    turn = lax.rem(layer, 2)
                    group = group.astype(F32)
                    for tile in range(4):
                        wide[turn, g, pl.ds(tile, 8, stride=4)] = group[8 * tile:8 * tile + 8]
                    group = wide[turn, g].astype(BF16)
                flat[0:1, pl.ds(pl.multiple_of((base + layer * 128 + g * GROUP) * LANES, 4096), 4096)] = group.reshape(1, 4096)

        finish(base, 2048, pair_sem.at[PARTS + q])
    lines = []
    for half in range(2):
        tiles = [wg_ref[7, pl.ds(pl.multiple_of(VEC_AT + half * 104 + jnp.minimum(3 * pair + tile, 12) * 8, 8), 8)].astype(F32) for tile in range(5)]
        turned = pltpu.roll(jnp.concatenate(tiles, axis=1), 5 * LANES - 32 * pair, 1)
        lines += [turned[line:line + 1, :416] for line in range(8)]
    flat[0:1, pl.ds(14336 * LANES, 52 * LANES)] = jnp.concatenate(lines, axis=1).astype(BF16)
    finish(14336, 52, pair_sem.at[PARTS + 3])
    for copy in copies:
        copy.wait()


def place_call(m_new, v_new, w_new, gathered):
    hbm = pl.BlockSpec(memory_space=pl.ANY)
    dma = pltpu.SemaphoreType.DMA
    flat = jax.ShapeDtypeStruct((SLICE_ROWS, LANES), F32)
    return pl.pallas_call(
        place_kernel,
        name='place_weights',
        out_shape=(flat, flat, flat) + tuple(jax.ShapeDtypeStruct((size, LANES), BF16) for size in (32768, 8192, 8192, 8192, 208))
        + (jax.ShapeDtypeStruct((1, PAIR_SIZE), BF16),),
        in_specs=[pl.BlockSpec(memory_space=pltpu.VMEM)] * 4,
        out_specs=[hbm] * 9,
        scratch_shapes=[
            pltpu.VMEM((1, PAIR_SIZE), BF16),
            pltpu.VMEM((2, 4, GROUP, LANES), F32),
            dma((3,)), dma((12,)), dma((PARTS + 4,)),
        ],
        compiler_params=pltpu.CompilerParams(vmem_limit_bytes=12 * 1024 * 1024),
    )(*(pltpu.with_memory_space_constraint(x, pltpu.VMEM) for x in (m_new, v_new, w_new, gathered)))


def to_tiles(tensor):
    return tensor.reshape(256, 8, 4, LANES).transpose(0, 2, 1, 3).reshape(8192, LANES)


def from_tiles(rows):
    return rows.reshape(256, 4, 8, LANES).transpose(0, 2, 1, 3).reshape(16, 128, 512)


def solution(mesh):
    def local_step(g_embed, g_attn, g_ffn_in, g_ffn_out, g_vec, m_shard, v_shard, w_shard):
        vec_rows = g_vec.reshape(2, 8, 13, LANES).transpose(0, 2, 1, 3).reshape(VEC_ROWS, LANES)
        tensors = (g_embed.reshape(32768, LANES), to_tiles(g_attn), to_tiles(g_ffn_in), g_ffn_out.reshape(8192, LANES), vec_rows)
        state = [shard.reshape(SLICE_ROWS, LANES) for shard in (m_shard, v_shard, w_shard)]
        m_new, v_new, w_new, gathered = step_call(tensors, state)
        m_new, v_new, w_new, embed, attn, ffn_in, ffn_out, vec, w_pair = place_call(m_new, v_new, w_new, gathered)
        wb_vec = vec.reshape(2, 13, 8, LANES).transpose(0, 2, 1, 3).reshape(16, 1664)
        return (m_new.reshape(-1), v_new.reshape(-1), w_new.reshape(-1), embed, from_tiles(attn), from_tiles(ffn_in),
                ffn_out.reshape(16, 512, 128), wb_vec, w_pair)

    return jax.shard_map(local_step, mesh=mesh, in_specs=(P(MESH_AXES),) * 8, out_specs=(P(MESH_AXES),) * 3 + (P(),) * 5 + (P(MESH_AXES),), check_vma=False)
```

```python
import functools
import math
import jax
import jax.numpy as jnp
from jax import lax
from jax.experimental import pallas as pl
from jax.experimental.pallas import tpu as pltpu
from jax.sharding import PartitionSpec as P

MESH_AXES = ('outer', 'middle', 'inner')
ADAM_BETA1 = 0.9
ADAM_BETA2 = 0.98
ADAM_EPS = 1e-9
LEARN_RATE = 0.05
ADAM_STEP = 3
STEP_RATE = LEARN_RATE / (1.0 - ADAM_BETA1 ** ADAM_STEP)

MESH = pl.DeviceIdType.MESH
F32 = jnp.float32
BF16 = jnp.bfloat16

LANES = 128
GROUP = 32
ROWS = 7366656 // LANES
SLICE_ROWS = ROWS // 8
CHUNK_GROUPS = 24
CHUNK = CHUNK_GROUPS * GROUP
HALF = CHUNK // 2
LEAD = (4, 12)
MAIN = 8
LAST = (18,)
SIZES = LEAD + (CHUNK_GROUPS,) * MAIN + LAST
CHUNKS = len(SIZES)
RING = 4
D2D_RING = 6
OUT_RING = 5
WINDOW_GROUPS = sum(SIZES)
WINDOW = WINDOW_GROUPS * GROUP
MARGIN = GROUP
BOUNDS = (0, 1024, 1280, 1536, 1792, 1799)
PERMUTED = (1024, 1536)
VEC_ROWS = 208
VEC_AT = (BOUNDS[4] - SLICE_ROWS * 7 // GROUP) * GROUP


def window_start(device):
    return SLICE_ROWS * device // GROUP


def window_start_traced(device):
    return lax.div(device * SLICE_ROWS, GROUP)


def chunk_first(chunk):
    return sum(SIZES[:chunk])


def pieces(first, groups):
    found = []
    for tensor in range(5):
        low, high = max(first, BOUNDS[tensor]), min(first + groups, BOUNDS[tensor + 1])
        if low < high:
            row, off, size = (low - BOUNDS[tensor]) * GROUP, (low - first) * GROUP, (high - low) * GROUP
            if tensor == 4 and row + size > VEC_ROWS:
                found.append((tensor, 0, off + VEC_ROWS - row, row + size - VEC_ROWS))
                size = VEC_ROWS - row
            found.append((tensor, row, off, size))
    return tuple(found)


def split_chunks(groups):
    spans = [window_start(d) + chunk_first(c) for d in range(8) for c in range(CHUNKS) if SIZES[c] == groups]
    return [(first, pieces(first, groups)) for first in spans if len(pieces(first, groups)) > 1 or first >= BOUNDS[4]]


FIRSTS = tuple(SLICE_ROWS * d // GROUP for d in range(8)) + (BOUNDS[-1] - 1,)


def step_kernel(e_ref, a_ref, f1_ref, f2_ref, b_ref, m_ref, v_ref, w_ref,
                m_out, v_out, w_out, wg_ref,
                acc, local, p1x, p1y, p2x, p2y, gflat, wflat, m_in, stage, vec,
                stage_sem, local_sem, d2d_send, d2d_recv, sum_send, p1_recv, p2_recv, in_sem, out_send, ag_recv, relay_recv, fwd_recv):
    o, m, i = lax.axis_index('outer'), lax.axis_index('middle'), lax.axis_index('inner')
    x_dev, y_dev, p_dev = (o, 1 - m, i), (1 - o, m, i), (o, m, 1 - i)
    places = ((o, m), (o, 1 - m), (1 - o, m), (1 - o, 1 - m))
    mine = [(po * 2 + pm) * 2 + i for po, pm in places]
    theirs = [(po * 2 + pm) * 2 + (1 - i) for po, pm in places]
    start = window_start_traced(mine[0])
    shift = mine[0] * SLICE_ROWS - start * GROUP
    tensors = (e_ref, a_ref, f1_ref, f2_ref, b_ref)

    barrier = pltpu.get_barrier_semaphore()
    for device in (x_dev, y_dev, p_dev):
        pl.semaphore_signal(barrier, inc=1, device_id=device, device_id_type=MESH)

    def remote(src, dst, send, recv, device):
        pltpu.make_async_remote_copy(src_ref=src, dst_ref=dst, send_sem=send, recv_sem=recv, device_id=device, device_id_type=MESH).start()

    def drain(ref, sem):
        pltpu.make_async_copy(ref, ref, sem).wait()

    def mod(value, base):
        return value % base if isinstance(value, int) else lax.rem(value, base)

    def load_chunk(device, base, size, copy):
        groups = size // GROUP
        first = window_start_traced(device) + (base // GROUP if isinstance(base, int) else lax.div(base, GROUP))
        for tensor in range(4):
            @pl.when((first >= BOUNDS[tensor]) & (first + groups <= BOUNDS[tensor + 1]))
            def _():
                row = pl.multiple_of((first - BOUNDS[tensor]) * GROUP, GROUP)
                copy(tensors[tensor].at[pl.ds(row, size)], 0, size)
        for known, parts in split_chunks(groups):
            @pl.when(first == known)
            def _():
                for tensor, row, off, count in parts:
                    copy(tensors[tensor].at[pl.ds(row, count)], off, count)

    def load_ours(j, chunk, base, size):
        slot = mod(chunk, 3)
        load_chunk(mine[j], base, size, lambda src, off, count: pltpu.make_async_copy(
            src, local.at[slot, j, pl.ds(off, count)], local_sem.at[slot, int(j != 3)]).start())

    def issue_gradients(chunk, base, size):
        for j in (3, 1, 2, 0):
            load_chunk(theirs[j], base, size, lambda src, off, count: remote(
                src, acc.at[j, pl.ds(pl.multiple_of(base + off, 8), count)], d2d_send, d2d_recv.at[mod(chunk, D2D_RING), int(j != 3)], p_dev))
            load_ours(j, chunk, base, size)

    def add_rows(j, base, count, term):
        @pl.loop(0, count // GROUP)
        def _(r):
            off = pl.multiple_of(r * GROUP, GROUP)
            at = pl.ds(pl.multiple_of(base + off, GROUP), GROUP)
            acc[j, at] = acc[j, at] + term(off)

    def middle(base, size):
        return base + size // 2 if isinstance(base, int) else pl.multiple_of(base + size // 2, GROUP)

    def first_phase(chunk, base, size):
        slot, ring = mod(chunk, 3), mod(chunk, RING)
        half, second = size // 2, middle(base, size)
        near = pl.ds(0, half)

        def ready(j, count):
            arrived = local.at[0, pl.ds(0, count), pl.ds(0, size)]
            drain(arrived, local_sem.at[slot, j])
            drain(arrived, d2d_recv.at[mod(chunk, D2D_RING), j])

        ready(0, 1)
        add_rows(3, base, size, lambda off: local[slot, 3, pl.ds(off, GROUP)])
        remote(acc.at[3, pl.ds(base, half)], p1x.at[ring, 1, near], sum_send, p1_recv.at[ring], x_dev)
        remote(acc.at[3, pl.ds(second, half)], p1y.at[ring, 1, near], sum_send, p1_recv.at[ring], y_dev)
        ready(1, 3)
        add_rows(1, base, half, lambda off: local[slot, 1, pl.ds(off, GROUP)])
        remote(acc.at[1, pl.ds(base, half)], p1x.at[ring, 0, near], sum_send, p1_recv.at[ring], x_dev)
        add_rows(2, second, half, lambda off: local[slot, 2, pl.ds(half + off, GROUP)])
        remote(acc.at[2, pl.ds(second, half)], p1y.at[ring, 0, near], sum_send, p1_recv.at[ring], y_dev)
        add_rows(1, second, half, lambda off: local[slot, 1, pl.ds(half + off, GROUP)])
        add_rows(2, base, half, lambda off: local[slot, 2, pl.ds(off, GROUP)])
        add_rows(0, base, size, lambda off: local[slot, 0, pl.ds(off, GROUP)])

    def second_phase(chunk, base, size):
        ring = mod(chunk, RING)
        half, second = size // 2, middle(base, size)
        near = pl.ds(0, half)
        drain(local.at[0, pl.ds(0, 2), pl.ds(0, size)], p1_recv.at[ring])
        add_rows(2, base, half, lambda off: p1x[ring, 1, pl.ds(off, GROUP)])
        add_rows(1, second, half, lambda off: p1y[ring, 1, pl.ds(off, GROUP)])
        remote(acc.at[2, pl.ds(base, half)], p2y.at[ring, near], sum_send, p2_recv.at[ring], y_dev)
        remote(acc.at[1, pl.ds(second, half)], p2x.at[ring, near], sum_send, p2_recv.at[ring], x_dev)
        add_rows(0, base, half, lambda off: p1x[ring, 0, pl.ds(off, GROUP)])
        add_rows(0, second, half, lambda off: p1y[ring, 0, pl.ds(off, GROUP)])

    def is_permuted(group):
        return (group >= PERMUTED[0]) & (group < PERMUTED[1])

    def last_phase(chunk, base, size):
        ring = mod(chunk, RING)
        half = size // 2
        first = start + (base // GROUP if isinstance(base, int) else lax.div(base, GROUP))
        drain(local.at[0, 0, pl.ds(0, size)], p2_recv.at[ring])
        for part, arrived in enumerate((p2y, p2x)):
            @pl.loop(0, half // GROUP)
            def _(r):
                off = pl.multiple_of(r * GROUP, GROUP)
                row = pl.multiple_of(base + part * half + off, GROUP)
                total = acc[0, pl.ds(row, GROUP)] + arrived[ring, pl.ds(off, GROUP)]
                permuted = is_permuted(first + part * (half // GROUP) + r)

                @pl.when(permuted)
                def _():
                    for tile in range(4):
                        gflat[pl.ds(row + tile, 8, stride=4)] = total[8 * tile:8 * tile + 8]

                @pl.when(jnp.logical_not(permuted))
                def _():
                    gflat[pl.ds(row, GROUP)] = total

        if isinstance(chunk, int) and chunk == CHUNKS - 1:
            @pl.when(mine[0] == 7)
            def _():
                vec[...] = gflat[pl.ds(VEC_AT, VEC_ROWS)]
                for tile in range(26):
                    gflat[pl.ds(VEC_AT + tile // 13 * 104 + tile % 13, 8, stride=13)] = vec[8 * tile:8 * tile + 8]

    def start_loads(block, base, size):
        slot = mod(block, 2)
        count = size if not isinstance(base, int) else min(size, SLICE_ROWS - base)
        for q, ref in enumerate((m_ref, v_ref, w_ref)):
            pltpu.make_async_copy(ref.at[pl.ds(base, count)], m_in.at[slot, q, pl.ds(0, count)], in_sem.at[slot]).start()

    def adam_rows(slot, base, off, count):
        at = pl.ds(off, count)
        grad = gflat[pl.ds(base + off + shift, count)] / 8
        m_val = ADAM_BETA1 * m_in[slot, 0, at] + (1.0 - ADAM_BETA1) * grad
        v_val = ADAM_BETA2 * m_in[slot, 1, at] + (1.0 - ADAM_BETA2) * (grad * grad)
        v_hat = v_val / (1.0 - ADAM_BETA2 ** ADAM_STEP)
        w_val = m_in[slot, 2, at] - STEP_RATE * m_val / (jnp.sqrt(v_hat) + ADAM_EPS)
        out = pl.ds(pl.multiple_of(base + off, GROUP), count)
        m_out[out] = m_val
        v_out[out] = v_val
        w_out[out] = w_val
        wflat[pl.ds(pl.multiple_of(MARGIN + base + off, GROUP), count)] = w_val

    def adam(block, base, size):
        slot = mod(block, 2)
        rows = size if not isinstance(base, int) else min(size, SLICE_ROWS - base)
        drain(m_in.at[slot, :, pl.ds(0, rows)], in_sem.at[slot])

        @pl.loop(0, rows // GROUP)
        def _(r):
            adam_rows(slot, base, pl.multiple_of(r * GROUP, GROUP), GROUP)

        if rows % GROUP:
            adam_rows(slot, base, rows // GROUP * GROUP, rows % GROUP)
        first = start + (base // GROUP if isinstance(base, int) else lax.div(base, GROUP))

        @pl.loop(0, size // GROUP)
        def _(r):
            row = pl.multiple_of(base + r * GROUP, GROUP)
            source = MARGIN + row - shift
            permuted = is_permuted(first + r)

            @pl.when(permuted)
            def _():
                tiles = [wflat[pl.ds(source + tile, 8, stride=4)] for tile in range(4)]
                wg_ref[mine[0], pl.ds(row, GROUP)] = jnp.concatenate(tiles, axis=0).astype(BF16)

            @pl.when(jnp.logical_not(permuted))
            def _():
                wg_ref[mine[0], pl.ds(row, GROUP)] = wflat[pl.ds(source, GROUP)].astype(BF16)

        if isinstance(base, int) and base + size > VEC_AT:
            @pl.when(mine[0] == 7)
            def _():
                for pair in range(13):
                    row = VEC_AT + 16 * pair
                    if base <= row < base + size:
                        tiles = [wflat[pl.ds(MARGIN + VEC_AT - shift + tile // 13 * 104 + tile % 13, 8, stride=13)] for tile in (2 * pair, 2 * pair + 1)]
                        wg_ref[7, pl.ds(row, 16)] = jnp.concatenate(tiles, axis=0).astype(BF16)

        ours = wg_ref.at[mine[0], pl.ds(base, size)]
        remote(ours, ours, out_send, ag_recv.at[mod(block, OUT_RING)], x_dev)
        remote(ours, ours, out_send, ag_recv.at[mod(block, OUT_RING)], y_dev)
        remote(ours, ours, out_send, fwd_recv, p_dev)

    def relay(chunk, base, size):
        half, turn = size // 2, mod(chunk, OUT_RING)
        at, head, tail = pl.ds(base, size), pl.ds(base, half), pl.ds(middle(base, size), half)
        drain(wg_ref.at[pl.ds(0, 2), pl.ds(0, size)], ag_recv.at[turn])
        remote(wg_ref.at[mine[1], head], wg_ref.at[mine[1], head], out_send, relay_recv.at[turn], y_dev)
        remote(wg_ref.at[mine[2], tail], wg_ref.at[mine[2], tail], out_send, relay_recv.at[turn], x_dev)
        remote(wg_ref.at[mine[1], at], wg_ref.at[mine[1], at], out_send, fwd_recv, p_dev)
        remote(wg_ref.at[mine[2], at], wg_ref.at[mine[2], at], out_send, fwd_recv, p_dev)

    def forward(chunk, base, size):
        at = pl.ds(base, size)
        drain(wg_ref.at[0, pl.ds(0, size)], relay_recv.at[mod(chunk, OUT_RING)])
        remote(wg_ref.at[mine[3], at], wg_ref.at[mine[3], at], out_send, fwd_recv, p_dev)

    begin = SIZES[0] * GROUP
    for j in (3, 1, 2, 0):
        load_chunk(theirs[j], 0, begin, lambda src, off, count: pltpu.make_async_copy(
            src, stage.at[j, pl.ds(off, count)], stage_sem.at[int(j != 3)]).start())
        load_ours(j, 0, 0, begin)
    pl.semaphore_wait(barrier, 3)
    for j in (3, 1, 2, 0):
        if j == 3:
            drain(stage.at[3], stage_sem.at[0])
        elif j == 1:
            drain(stage.at[pl.ds(0, 3)], stage_sem.at[1])
        remote(stage.at[j], acc.at[j, pl.ds(0, begin)], d2d_send, d2d_recv.at[0, int(j != 3)], p_dev)
    issue_gradients(1, chunk_first(1) * GROUP, SIZES[1] * GROUP)

    def run(chunk, action):
        lead = len(LEAD)

        @pl.when((chunk >= lead) & (chunk < lead + MAIN))
        def _():
            action(chunk, pl.multiple_of(chunk * CHUNK + (sum(LEAD) - lead * CHUNK_GROUPS) * GROUP, GROUP), CHUNK)

        for other in [*range(lead), *range(lead + MAIN, CHUNKS)]:
            @pl.when(chunk == other)
            def _():
                action(other, chunk_first(other) * GROUP, SIZES[other] * GROUP)

    stages = ((-2, issue_gradients), (2, start_loads), (0, first_phase), (1, second_phase), (2, last_phase), (3, adam), (5, relay), (7, forward))

    @pl.loop(0, CHUNKS + stages[-1][0])
    def _(t):
        for lag, action in stages:
            run(t - lag, action)

    drain(acc, d2d_send)
    drain(acc.at[pl.ds(0, 3)], sum_send)
    drain(wg_ref.at[pl.ds(0, 7)], out_send)
    drain(wg_ref.at[pl.ds(0, 4)], fwd_recv)

    for d in range(1, 8):
        keep = SLICE_ROWS * d - FIRSTS[d] * GROUP
        row = lax.broadcasted_iota(jnp.int32, (GROUP, LANES), 0)
        if PERMUTED[0] <= FIRSTS[d] < PERMUTED[1]:
            row = 4 * (row % 8) + row // 8
        before = pl.ds((FIRSTS[d] - window_start(d - 1)) * GROUP, GROUP)
        after = pl.ds((FIRSTS[d] - window_start(d)) * GROUP, GROUP)
        wg_ref[d - 1, before] = jnp.where(row < keep, wg_ref[d - 1, before].astype(F32), wg_ref[d, after].astype(F32)).astype(BF16)


def step_call(tensors, state):
    hbm = pl.BlockSpec(memory_space=pl.ANY)
    dma = pltpu.SemaphoreType.DMA
    flat = pltpu.VMEM((SLICE_ROWS, LANES), F32)
    return pl.pallas_call(
        step_kernel,
        name='adam_step',
        out_shape=(flat, flat, flat, pltpu.VMEM((8, WINDOW, LANES), BF16)),
        in_specs=[hbm] * 8,
        out_specs=[pl.BlockSpec(memory_space=pltpu.VMEM)] * 4,
        scratch_shapes=[
            pltpu.VMEM((4, WINDOW, LANES), F32),
            pltpu.VMEM((3, 4, CHUNK, LANES), F32),
            pltpu.VMEM((RING, 2, HALF, LANES), F32),
            pltpu.VMEM((RING, 2, HALF, LANES), F32),
            pltpu.VMEM((RING, HALF, LANES), F32),
            pltpu.VMEM((RING, HALF, LANES), F32),
            pltpu.VMEM((WINDOW + MARGIN, LANES), F32),
            pltpu.VMEM((WINDOW + MARGIN, LANES), F32),
            pltpu.VMEM((2, 3, CHUNK, LANES), F32),
            pltpu.VMEM((4, SIZES[0] * GROUP, LANES), F32),
            pltpu.VMEM((VEC_ROWS, LANES), F32),
            dma((2,)), dma((3, 2)), dma, dma((D2D_RING, 2)), dma, dma((RING,)), dma((RING,)), dma((2,)), dma,
            dma((OUT_RING,)), dma((OUT_RING,)), dma,
        ],
        compiler_params=pltpu.CompilerParams(collective_id=0, has_side_effects=True, vmem_limit_bytes=36 * 1024 * 1024),
    )(*tensors, *state)


LAYERS = 16
PAIR_ROWS = 8192 + 3 * 2048 + 52
PAIR_SIZE = PAIR_ROWS * LANES
PARTS = 4


def place_kernel(mv_ref, vv_ref, wv_ref, wg_ref, m_out, v_out, w_out, e_ref, a_ref, f1_ref, f2_ref, b_ref, pair_ref, flat, wide, state_sem, out_sem, pair_sem):
    pair = lax.axis_index('outer') * 2 + lax.axis_index('middle')

    def put(src, dst, sem):
        pltpu.make_async_copy(src, dst, sem).start()

    for q, (src, dst) in enumerate(((mv_ref, m_out), (vv_ref, v_out), (wv_ref, w_out))):
        put(src, dst, state_sem.at[q])
    for d in range(8):
        low, high = (FIRSTS[d] + 1 if d else 0), FIRSTS[d + 1] + 1
        for q, ref in enumerate((e_ref, a_ref, f1_ref, f2_ref, b_ref)):
            begin, end = max(low, BOUNDS[q]), min(high, BOUNDS[q + 1])
            if begin < end:
                offset = (begin - BOUNDS[q]) * GROUP
                size = min((end - begin) * GROUP, ref.shape[0] - offset)
                put(wg_ref.at[d, pl.ds((begin - window_start(d)) * GROUP, size)], ref.at[pl.ds(offset, size)], out_sem)

    def finish(begin, size):
        put(flat.at[:, pl.ds(begin * LANES, size * LANES)], pair_ref.at[:, pl.ds(begin * LANES, size * LANES)], pair_sem)

    def source(group, low, last, starts):
        late = group > last
        row = (group - jnp.where(late, starts[1], starts[0])) * GROUP
        return low + jnp.where(late, 1, 0), pl.multiple_of(row, GROUP)

    embed_starts = (window_start_traced(pair), window_start_traced(pair + 1))
    for part in range(PARTS):
        @pl.loop(part * 256 // PARTS, (part + 1) * 256 // PARTS, unroll=4)
        def _(g):
            d, row = source(pair * 256 + g, pair, embed_starts[1], embed_starts)
            flat[0:1, pl.ds(pl.multiple_of(g * 4096, 4096), 4096)] = wg_ref[d, pl.ds(row, GROUP)].reshape(1, 4096)

        finish(part * 8192 // PARTS, 8192 // PARTS)

    for q in (2, 0, 1):
        low = 4 + q
        base = 8192 + 2048 * q

        @pl.loop(0, LAYERS, unroll=2)
        def _(layer):
            for g in range(4):
                d, row = source(BOUNDS[1 + q] + layer * 16 + pair * 4 + g, low, FIRSTS[low + 1], (window_start(low), window_start(low + 1)))
                group = wg_ref[d, pl.ds(row, GROUP)]
                if q < 2:
                    turn = lax.rem(layer, 2)
                    group = group.astype(F32)
                    for tile in range(4):
                        wide[turn, g, pl.ds(tile, 8, stride=4)] = group[8 * tile:8 * tile + 8]
                    group = wide[turn, g].astype(BF16)
                flat[0:1, pl.ds(pl.multiple_of((base + layer * 128 + g * GROUP) * LANES, 4096), 4096)] = group.reshape(1, 4096)

        finish(base, 2048)
    lines = []
    for half in range(2):
        tiles = [wg_ref[7, pl.ds(pl.multiple_of(VEC_AT + half * 104 + jnp.minimum(3 * pair + tile, 12) * 8, 8), 8)].astype(F32) for tile in range(5)]
        turned = pltpu.roll(jnp.concatenate(tiles, axis=1), 5 * LANES - 32 * pair, 1)
        lines += [turned[line:line + 1, :416] for line in range(8)]
    flat[0:1, pl.ds(14336 * LANES, 52 * LANES)] = jnp.concatenate(lines, axis=1).astype(BF16)
    finish(14336, 52)
    for q, (src, dst) in enumerate(((mv_ref, m_out), (vv_ref, v_out), (wv_ref, w_out))):
        pltpu.make_async_copy(src, dst, state_sem.at[q]).wait()
    every = wg_ref.at[:, pl.ds(0, SLICE_ROWS)]
    pltpu.make_async_copy(every, every, out_sem).wait()
    pltpu.make_async_copy(flat, pair_ref, pair_sem).wait()


def place_call(m_new, v_new, w_new, gathered):
    hbm = pl.BlockSpec(memory_space=pl.ANY)
    dma = pltpu.SemaphoreType.DMA
    flat = jax.ShapeDtypeStruct((SLICE_ROWS, LANES), F32)
    return pl.pallas_call(
        place_kernel,
        name='place_weights',
        out_shape=(flat, flat, flat) + tuple(jax.ShapeDtypeStruct((size, LANES), BF16) for size in (32768, 8192, 8192, 8192, 208))
        + (jax.ShapeDtypeStruct((1, PAIR_SIZE), BF16),),
        in_specs=[pl.BlockSpec(memory_space=pltpu.VMEM)] * 4,
        out_specs=[hbm] * 9,
        scratch_shapes=[
            pltpu.VMEM((1, PAIR_SIZE), BF16),
            pltpu.VMEM((2, 4, GROUP, LANES), F32),
            dma((3,)), dma, dma,
        ],
        compiler_params=pltpu.CompilerParams(vmem_limit_bytes=12 * 1024 * 1024),
    )(*(pltpu.with_memory_space_constraint(x, pltpu.VMEM) for x in (m_new, v_new, w_new, gathered)))


def to_tiles(tensor):
    return tensor.reshape(256, 8, 4, LANES).transpose(0, 2, 1, 3).reshape(8192, LANES)


def from_tiles(rows):
    return rows.reshape(256, 4, 8, LANES).transpose(0, 2, 1, 3).reshape(16, 128, 512)


def solution(mesh):
    def local_step(g_embed, g_attn, g_ffn_in, g_ffn_out, g_vec, m_shard, v_shard, w_shard):
        vec_rows = g_vec.reshape(2, 8, 13, LANES).transpose(0, 2, 1, 3).reshape(VEC_ROWS, LANES)
        tensors = (g_embed.reshape(32768, LANES), to_tiles(g_attn), to_tiles(g_ffn_in), g_ffn_out.reshape(8192, LANES), vec_rows)
        state = [shard.reshape(SLICE_ROWS, LANES) for shard in (m_shard, v_shard, w_shard)]
        m_new, v_new, w_new, gathered = step_call(tensors, state)
        m_new, v_new, w_new, embed, attn, ffn_in, ffn_out, vec, w_pair = place_call(m_new, v_new, w_new, gathered)
        wb_vec = vec.reshape(2, 13, 8, LANES).transpose(0, 2, 1, 3).reshape(16, 1664)
        return (m_new.reshape(-1), v_new.reshape(-1), w_new.reshape(-1), embed, from_tiles(attn), from_tiles(ffn_in),
                ffn_out.reshape(16, 512, 128), wb_vec, w_pair)

    return jax.shard_map(local_step, mesh=mesh, in_specs=(P(MESH_AXES),) * 8, out_specs=(P(MESH_AXES),) * 3 + (P(),) * 5 + (P(MESH_AXES),), check_vma=False)
```

```python
import functools
import math
import jax
import jax.numpy as jnp
from jax import lax
from jax.experimental import pallas as pl
from jax.experimental.pallas import tpu as pltpu
from jax.sharding import PartitionSpec as P

MESH_AXES = ('outer', 'middle', 'inner')
ADAM_BETA1 = 0.9
ADAM_BETA2 = 0.98
ADAM_EPS = 1e-9
LEARN_RATE = 0.05
ADAM_STEP = 3
STEP_RATE = LEARN_RATE / (1.0 - ADAM_BETA1 ** ADAM_STEP)

MESH = pl.DeviceIdType.MESH
F32 = jnp.float32
BF16 = jnp.bfloat16

LANES = 128
GROUP = 32
ROWS = 7366656 // LANES
SLICE_ROWS = ROWS // 8
CHUNK_GROUPS = 24
CHUNK = CHUNK_GROUPS * GROUP
HALF = CHUNK // 2
LEAD = (4, 14)
MAIN = 8
LAST = (16,)
SIZES = LEAD + (CHUNK_GROUPS,) * MAIN + LAST
CHUNKS = len(SIZES)
RING = 4
D2D_RING = 6
SKEW = 4
OUT_RING = 5
WINDOW_GROUPS = sum(SIZES)
WINDOW = WINDOW_GROUPS * GROUP
MARGIN = GROUP
BOUNDS = (0, 1024, 1280, 1536, 1792, 1799)
PERMUTED = (1024, 1536)
VEC_ROWS = 208
VEC_AT = (BOUNDS[4] - SLICE_ROWS * 7 // GROUP) * GROUP


def window_start(device):
    return SLICE_ROWS * device // GROUP


def window_start_traced(device):
    return lax.div(device * SLICE_ROWS, GROUP)


def chunk_first(chunk):
    return sum(SIZES[:chunk])


def pieces(first, groups):
    found = []
    for tensor in range(5):
        low, high = max(first, BOUNDS[tensor]), min(first + groups, BOUNDS[tensor + 1])
        if low < high:
            row, off, size = (low - BOUNDS[tensor]) * GROUP, (low - first) * GROUP, (high - low) * GROUP
            if tensor == 4 and row + size > VEC_ROWS:
                found.append((tensor, 0, off + VEC_ROWS - row, row + size - VEC_ROWS))
                size = VEC_ROWS - row
            found.append((tensor, row, off, size))
    return tuple(found)


def split_chunks(groups):
    spans = [window_start(d) + chunk_first(c) for d in range(8) for c in range(CHUNKS) if SIZES[c] == groups]
    return [(first, pieces(first, groups)) for first in spans if len(pieces(first, groups)) > 1 or first >= BOUNDS[4]]


FIRSTS = tuple(SLICE_ROWS * d // GROUP for d in range(8)) + (BOUNDS[-1] - 1,)


def step_kernel(e_ref, a_ref, f1_ref, f2_ref, b_ref, m_ref, v_ref, w_ref,
                m_out, v_out, w_out, wg_ref,
                acc, local, p1x, p1y, p2x, p2y, gflat, wflat, m_in, stage, vec,
                stage_sem, local_sem, d2d_send, d2d_recv, sum_send, p1_recv, p2_recv, in_sem, out_send, ag_recv, relay_recv, fwd_recv):
    o, m, i = lax.axis_index('outer'), lax.axis_index('middle'), lax.axis_index('inner')
    x_dev, y_dev, p_dev = (o, 1 - m, i), (1 - o, m, i), (o, m, 1 - i)
    places = ((o, m), (o, 1 - m), (1 - o, m), (1 - o, 1 - m))
    mine = [(po * 2 + pm) * 2 + i for po, pm in places]
    theirs = [(po * 2 + pm) * 2 + (1 - i) for po, pm in places]
    start = window_start_traced(mine[0])
    shift = mine[0] * SLICE_ROWS - start * GROUP
    tensors = (e_ref, a_ref, f1_ref, f2_ref, b_ref)

    barrier = pltpu.get_barrier_semaphore()
    for device in (x_dev, y_dev, p_dev):
        pl.semaphore_signal(barrier, inc=1, device_id=device, device_id_type=MESH)

    def remote(src, dst, send, recv, device):
        pltpu.make_async_remote_copy(src_ref=src, dst_ref=dst, send_sem=send, recv_sem=recv, device_id=device, device_id_type=MESH).start()

    def drain(ref, sem):
        pltpu.make_async_copy(ref, ref, sem).wait()

    def mod(value, base):
        return value % base if isinstance(value, int) else lax.rem(value, base)

    def load_chunk(device, base, size, copy):
        groups = size // GROUP
        first = window_start_traced(device) + (base // GROUP if isinstance(base, int) else lax.div(base, GROUP))
        for tensor in range(4):
            @pl.when((first >= BOUNDS[tensor]) & (first + groups <= BOUNDS[tensor + 1]))
            def _():
                row = pl.multiple_of((first - BOUNDS[tensor]) * GROUP, GROUP)
                copy(tensors[tensor].at[pl.ds(row, size)], 0, size)
        for known, parts in split_chunks(groups):
            @pl.when(first == known)
            def _():
                for tensor, row, off, count in parts:
                    copy(tensors[tensor].at[pl.ds(row, count)], off, count)

    def load_ours(j, chunk, base, size):
        slot = mod(chunk, 3)
        load_chunk(mine[j], base, size, lambda src, off, count: pltpu.make_async_copy(
            src, local.at[slot, j, pl.ds(off, count)], local_sem.at[slot, int(j != 3)]).start())

    def issue_gradients(chunk, base, size):
        for j in (3, 1, 2, 0):
            load_chunk(theirs[j], base, size, lambda src, off, count: remote(
                src, acc.at[j, pl.ds(pl.multiple_of(base + off, 8), count)], d2d_send, d2d_recv.at[mod(chunk, D2D_RING), int(j != 3)], p_dev))
            load_ours(j, chunk, base, size)

    def add_rows(j, base, count, term):
        @pl.loop(0, count // GROUP)
        def _(r):
            off = pl.multiple_of(r * GROUP, GROUP)
            at = pl.ds(pl.multiple_of(base + off, GROUP), GROUP)
            acc[j, at] = acc[j, at] + term(off)

    def shifted(base, count):
        return base + count if isinstance(base, int) else pl.multiple_of(base + count, GROUP)

    def first_phase(chunk, base, size, cuts):
        slot, ring = mod(chunk, 3), mod(chunk, RING)
        _, x_cut, y_cut, d_cut = cuts

        def ready(j, count):
            arrived = local.at[0, pl.ds(0, count), pl.ds(0, size)]
            drain(arrived, local_sem.at[slot, j])
            drain(arrived, d2d_recv.at[mod(chunk, D2D_RING), j])

        def add(j, first, count):
            add_rows(j, shifted(base, first), count, lambda off: local[slot, j, pl.ds(first + off, GROUP)])

        def send(j, first, count, dst, place, device):
            remote(acc.at[j, pl.ds(shifted(base, first), count)], dst.at[ring, place, pl.ds(0, count)], sum_send, p1_recv.at[ring], device)

        ready(0, 1)
        add(3, 0, size)
        send(3, 0, d_cut, p1x, 1, x_dev)
        send(3, d_cut, size - d_cut, p1y, 1, y_dev)
        ready(1, 3)
        add(1, 0, x_cut)
        send(1, 0, x_cut, p1x, 0, x_dev)
        add(2, y_cut, size - y_cut)
        send(2, y_cut, size - y_cut, p1y, 0, y_dev)
        add(1, x_cut, size - x_cut)
        add(2, 0, y_cut)
        add(0, 0, size)

    def second_phase(chunk, base, size, cuts):
        ring = mod(chunk, RING)
        cut, x_cut, y_cut, _ = cuts
        drain(local.at[0, pl.ds(0, 2), pl.ds(0, size + (y_cut - x_cut) // 2)], p1_recv.at[ring])
        far = shifted(base, x_cut)
        add_rows(2, base, y_cut, lambda off: p1x[ring, 1, pl.ds(off, GROUP)])
        add_rows(1, far, size - x_cut, lambda off: p1y[ring, 1, pl.ds(off, GROUP)])
        remote(acc.at[2, pl.ds(base, y_cut)], p2y.at[ring, pl.ds(0, y_cut)], sum_send, p2_recv.at[ring], y_dev)
        remote(acc.at[1, pl.ds(far, size - x_cut)], p2x.at[ring, pl.ds(0, size - x_cut)], sum_send, p2_recv.at[ring], x_dev)
        add_rows(0, base, cut, lambda off: p1x[ring, 0, pl.ds(off, GROUP)])
        add_rows(0, shifted(base, cut), size - cut, lambda off: p1y[ring, 0, pl.ds(off, GROUP)])

    def is_permuted(group):
        return (group >= PERMUTED[0]) & (group < PERMUTED[1])

    def last_phase(chunk, base, size, cuts):
        ring = mod(chunk, RING)
        cut = cuts[0]
        first = start + (base // GROUP if isinstance(base, int) else lax.div(base, GROUP))
        drain(local.at[0, 0, pl.ds(0, size)], p2_recv.at[ring])
        for arrived, begin, count in ((p2y, 0, cut), (p2x, cut, size - cut)):
            @pl.loop(0, count // GROUP)
            def _(r):
                off = pl.multiple_of(r * GROUP, GROUP)
                row = pl.multiple_of(base + begin + off, GROUP)
                total = acc[0, pl.ds(row, GROUP)] + arrived[ring, pl.ds(off, GROUP)]
                permuted = is_permuted(first + begin // GROUP + r)

                @pl.when(permuted)
                def _():
                    for tile in range(4):
                        gflat[pl.ds(row + tile, 8, stride=4)] = total[8 * tile:8 * tile + 8]

                @pl.when(jnp.logical_not(permuted))
                def _():
                    gflat[pl.ds(row, GROUP)] = total

        if isinstance(chunk, int) and chunk == CHUNKS - 1:
            @pl.when(mine[0] == 7)
            def _():
                vec[...] = gflat[pl.ds(VEC_AT, VEC_ROWS)]
                for tile in range(26):
                    gflat[pl.ds(VEC_AT + tile // 13 * 104 + tile % 13, 8, stride=13)] = vec[8 * tile:8 * tile + 8]

    def start_loads(block, base, size):
        slot = mod(block, 2)
        count = size if not isinstance(base, int) else min(size, SLICE_ROWS - base)
        for q, ref in enumerate((m_ref, v_ref, w_ref)):
            pltpu.make_async_copy(ref.at[pl.ds(base, count)], m_in.at[slot, q, pl.ds(0, count)], in_sem.at[slot]).start()

    def adam_rows(slot, base, off, count):
        at = pl.ds(off, count)
        grad = gflat[pl.ds(base + off + shift, count)] / 8
        m_val = ADAM_BETA1 * m_in[slot, 0, at] + (1.0 - ADAM_BETA1) * grad
        v_val = ADAM_BETA2 * m_in[slot, 1, at] + (1.0 - ADAM_BETA2) * (grad * grad)
        v_hat = v_val / (1.0 - ADAM_BETA2 ** ADAM_STEP)
        w_val = m_in[slot, 2, at] - STEP_RATE * m_val / (jnp.sqrt(v_hat) + ADAM_EPS)
        out = pl.ds(pl.multiple_of(base + off, GROUP), count)
        m_out[out] = m_val
        v_out[out] = v_val
        w_out[out] = w_val
        wflat[pl.ds(pl.multiple_of(MARGIN + base + off, GROUP), count)] = w_val

    def adam(block, base, size):
        slot = mod(block, 2)
        rows = size if not isinstance(base, int) else min(size, SLICE_ROWS - base)
        drain(m_in.at[slot, :, pl.ds(0, rows)], in_sem.at[slot])

        @pl.loop(0, rows // GROUP)
        def _(r):
            adam_rows(slot, base, pl.multiple_of(r * GROUP, GROUP), GROUP)

        if rows % GROUP:
            adam_rows(slot, base, rows // GROUP * GROUP, rows % GROUP)
        first = start + (base // GROUP if isinstance(base, int) else lax.div(base, GROUP))

        @pl.loop(0, size // GROUP)
        def _(r):
            row = pl.multiple_of(base + r * GROUP, GROUP)
            source = MARGIN + row - shift
            permuted = is_permuted(first + r)

            @pl.when(permuted)
            def _():
                tiles = [wflat[pl.ds(source + tile, 8, stride=4)] for tile in range(4)]
                wg_ref[mine[0], pl.ds(row, GROUP)] = jnp.concatenate(tiles, axis=0).astype(BF16)

            @pl.when(jnp.logical_not(permuted))
            def _():
                wg_ref[mine[0], pl.ds(row, GROUP)] = wflat[pl.ds(source, GROUP)].astype(BF16)

        if isinstance(base, int) and base + size > VEC_AT:
            @pl.when(mine[0] == 7)
            def _():
                for pair in range(13):
                    row = VEC_AT + 16 * pair
                    if base <= row < base + size:
                        tiles = [wflat[pl.ds(MARGIN + VEC_AT - shift + tile // 13 * 104 + tile % 13, 8, stride=13)] for tile in (2 * pair, 2 * pair + 1)]
                        wg_ref[7, pl.ds(row, 16)] = jnp.concatenate(tiles, axis=0).astype(BF16)

        ours = wg_ref.at[mine[0], pl.ds(base, size)]
        remote(ours, ours, out_send, ag_recv.at[mod(block, OUT_RING)], x_dev)
        remote(ours, ours, out_send, ag_recv.at[mod(block, OUT_RING)], y_dev)
        remote(ours, ours, out_send, fwd_recv, p_dev)

    def relay(chunk, base, size):
        half, turn = size // 2, mod(chunk, OUT_RING)
        at, head, tail = pl.ds(base, size), pl.ds(base, half), pl.ds(shifted(base, half), half)
        drain(wg_ref.at[pl.ds(0, 2), pl.ds(0, size)], ag_recv.at[turn])
        remote(wg_ref.at[mine[1], head], wg_ref.at[mine[1], head], out_send, relay_recv.at[turn], y_dev)
        remote(wg_ref.at[mine[2], tail], wg_ref.at[mine[2], tail], out_send, relay_recv.at[turn], x_dev)
        remote(wg_ref.at[mine[1], at], wg_ref.at[mine[1], at], out_send, fwd_recv, p_dev)
        remote(wg_ref.at[mine[2], at], wg_ref.at[mine[2], at], out_send, fwd_recv, p_dev)

    def forward(chunk, base, size):
        at = pl.ds(base, size)
        drain(wg_ref.at[0, pl.ds(0, size)], relay_recv.at[mod(chunk, OUT_RING)])
        remote(wg_ref.at[mine[3], at], wg_ref.at[mine[3], at], out_send, fwd_recv, p_dev)

    begin = SIZES[0] * GROUP
    for j in (3, 1, 2, 0):
        load_chunk(theirs[j], 0, begin, lambda src, off, count: pltpu.make_async_copy(
            src, stage.at[j, pl.ds(off, count)], stage_sem.at[int(j != 3)]).start())
        load_ours(j, 0, 0, begin)
    pl.semaphore_wait(barrier, 3)
    for j in (3, 1, 2, 0):
        if j == 3:
            drain(stage.at[3], stage_sem.at[0])
        elif j == 1:
            drain(stage.at[pl.ds(0, 3)], stage_sem.at[1])
        remote(stage.at[j], acc.at[j, pl.ds(0, begin)], d2d_send, d2d_recv.at[0, int(j != 3)], p_dev)
    issue_gradients(1, chunk_first(1) * GROUP, SIZES[1] * GROUP)

    def cut_of(chip, size):
        return size // 2 + SKEW * GROUP * ((chip == 1) - (chip == 2))

    def run(chunk, action, summing):
        lead = len(LEAD)

        def halves(size):
            return ((size // 2,) * 4,) if summing else ()

        @pl.when((chunk >= lead) & (chunk < lead + MAIN))
        def _():
            action(chunk, pl.multiple_of(chunk * CHUNK + (sum(LEAD) - lead * CHUNK_GROUPS) * GROUP, GROUP), CHUNK, *halves(CHUNK))

        for other in [*range(lead), *range(lead + MAIN, CHUNKS)]:
            @pl.when(chunk == other)
            def _():
                size = SIZES[other] * GROUP
                if other < CHUNKS - 1 or not halves(size):
                    action(other, chunk_first(other) * GROUP, size, *halves(size))
                else:
                    for chip in range(4):
                        @pl.when(mine[0] // 2 == chip)
                        def _():
                            action(other, chunk_first(other) * GROUP, size, tuple(cut_of(chip ^ j, size) for j in range(4)))

    stages = ((-2, issue_gradients), (2, start_loads), (0, first_phase), (1, second_phase), (2, last_phase), (3, adam), (5, relay), (7, forward))

    @pl.loop(0, CHUNKS + stages[-1][0])
    def _(t):
        for lag, action in stages:
            run(t - lag, action, action in (first_phase, second_phase, last_phase))

    drain(acc, d2d_send)
    drain(acc.at[pl.ds(0, 3)], sum_send)
    drain(wg_ref.at[pl.ds(0, 7)], out_send)
    drain(wg_ref.at[pl.ds(0, 4)], fwd_recv)

    for d in range(1, 8):
        keep = SLICE_ROWS * d - FIRSTS[d] * GROUP
        row = lax.broadcasted_iota(jnp.int32, (GROUP, LANES), 0)
        if PERMUTED[0] <= FIRSTS[d] < PERMUTED[1]:
            row = 4 * (row % 8) + row // 8
        before = pl.ds((FIRSTS[d] - window_start(d - 1)) * GROUP, GROUP)
        after = pl.ds((FIRSTS[d] - window_start(d)) * GROUP, GROUP)
        wg_ref[d - 1, before] = jnp.where(row < keep, wg_ref[d - 1, before].astype(F32), wg_ref[d, after].astype(F32)).astype(BF16)


def step_call(tensors, state):
    hbm = pl.BlockSpec(memory_space=pl.ANY)
    dma = pltpu.SemaphoreType.DMA
    flat = pltpu.VMEM((SLICE_ROWS, LANES), F32)
    return pl.pallas_call(
        step_kernel,
        name='adam_step',
        out_shape=(flat, flat, flat, pltpu.VMEM((8, WINDOW, LANES), BF16)),
        in_specs=[hbm] * 8,
        out_specs=[pl.BlockSpec(memory_space=pltpu.VMEM)] * 4,
        scratch_shapes=[
            pltpu.VMEM((4, WINDOW, LANES), F32),
            pltpu.VMEM((3, 4, CHUNK, LANES), F32),
            pltpu.VMEM((RING, 2, HALF, LANES), F32),
            pltpu.VMEM((RING, 2, HALF, LANES), F32),
            pltpu.VMEM((RING, HALF, LANES), F32),
            pltpu.VMEM((RING, HALF, LANES), F32),
            pltpu.VMEM((WINDOW + MARGIN, LANES), F32),
            pltpu.VMEM((WINDOW + MARGIN, LANES), F32),
            pltpu.VMEM((2, 3, CHUNK, LANES), F32),
            pltpu.VMEM((4, SIZES[0] * GROUP, LANES), F32),
            pltpu.VMEM((VEC_ROWS, LANES), F32),
            dma((2,)), dma((3, 2)), dma, dma((D2D_RING, 2)), dma, dma((RING,)), dma((RING,)), dma((2,)), dma,
            dma((OUT_RING,)), dma((OUT_RING,)), dma,
        ],
        compiler_params=pltpu.CompilerParams(collective_id=0, has_side_effects=True, vmem_limit_bytes=36 * 1024 * 1024),
    )(*tensors, *state)


LAYERS = 16
PAIR_ROWS = 8192 + 3 * 2048 + 52
PAIR_SIZE = PAIR_ROWS * LANES
PARTS = 4


def place_kernel(mv_ref, vv_ref, wv_ref, wg_ref, m_out, v_out, w_out, e_ref, a_ref, f1_ref, f2_ref, b_ref, pair_ref, flat, wide, state_sem, out_sem, pair_sem):
    pair = lax.axis_index('outer') * 2 + lax.axis_index('middle')

    def put(src, dst, sem):
        pltpu.make_async_copy(src, dst, sem).start()

    for q, (src, dst) in enumerate(((mv_ref, m_out), (vv_ref, v_out), (wv_ref, w_out))):
        put(src, dst, state_sem.at[q])
    for d in range(8):
        low, high = (FIRSTS[d] + 1 if d else 0), FIRSTS[d + 1] + 1
        for q, ref in enumerate((e_ref, a_ref, f1_ref, f2_ref, b_ref)):
            begin, end = max(low, BOUNDS[q]), min(high, BOUNDS[q + 1])
            if begin < end:
                offset = (begin - BOUNDS[q]) * GROUP
                size = min((end - begin) * GROUP, ref.shape[0] - offset)
                put(wg_ref.at[d, pl.ds((begin - window_start(d)) * GROUP, size)], ref.at[pl.ds(offset, size)], out_sem)

    def finish(begin, size):
        put(flat.at[:, pl.ds(begin * LANES, size * LANES)], pair_ref.at[:, pl.ds(begin * LANES, size * LANES)], pair_sem)

    def source(group, low, last, starts):
        late = group > last
        row = (group - jnp.where(late, starts[1], starts[0])) * GROUP
        return low + jnp.where(late, 1, 0), pl.multiple_of(row, GROUP)

    embed_starts = (window_start_traced(pair), window_start_traced(pair + 1))
    for part in range(PARTS):
        @pl.loop(part * 256 // PARTS, (part + 1) * 256 // PARTS, unroll=4)
        def _(g):
            d, row = source(pair * 256 + g, pair, embed_starts[1], embed_starts)
            flat[0:1, pl.ds(pl.multiple_of(g * 4096, 4096), 4096)] = wg_ref[d, pl.ds(row, GROUP)].reshape(1, 4096)

        finish(part * 8192 // PARTS, 8192 // PARTS)

    for q in (2, 0, 1):
        low = 4 + q
        base = 8192 + 2048 * q

        @pl.loop(0, LAYERS, unroll=2)
        def _(layer):
            for g in range(4):
                d, row = source(BOUNDS[1 + q] + layer * 16 + pair * 4 + g, low, FIRSTS[low + 1], (window_start(low), window_start(low + 1)))
                group = wg_ref[d, pl.ds(row, GROUP)]
                if q < 2:
                    turn = lax.rem(layer, 2)
                    group = group.astype(F32)
                    for tile in range(4):
                        wide[turn, g, pl.ds(tile, 8, stride=4)] = group[8 * tile:8 * tile + 8]
                    group = wide[turn, g].astype(BF16)
                flat[0:1, pl.ds(pl.multiple_of((base + layer * 128 + g * GROUP) * LANES, 4096), 4096)] = group.reshape(1, 4096)

        finish(base, 2048)
    lines = []
    for half in range(2):
        tiles = [wg_ref[7, pl.ds(pl.multiple_of(VEC_AT + half * 104 + jnp.minimum(3 * pair + tile, 12) * 8, 8), 8)].astype(F32) for tile in range(5)]
        turned = pltpu.roll(jnp.concatenate(tiles, axis=1), 5 * LANES - 32 * pair, 1)
        lines += [turned[line:line + 1, :416] for line in range(8)]
    flat[0:1, pl.ds(14336 * LANES, 52 * LANES)] = jnp.concatenate(lines, axis=1).astype(BF16)
    finish(14336, 52)
    for q, (src, dst) in enumerate(((mv_ref, m_out), (vv_ref, v_out), (wv_ref, w_out))):
        pltpu.make_async_copy(src, dst, state_sem.at[q]).wait()
    every = wg_ref.at[:, pl.ds(0, SLICE_ROWS)]
    pltpu.make_async_copy(every, every, out_sem).wait()
    pltpu.make_async_copy(flat, pair_ref, pair_sem).wait()


def place_call(m_new, v_new, w_new, gathered):
    hbm = pl.BlockSpec(memory_space=pl.ANY)
    dma = pltpu.SemaphoreType.DMA
    flat = jax.ShapeDtypeStruct((SLICE_ROWS, LANES), F32)
    return pl.pallas_call(
        place_kernel,
        name='place_weights',
        out_shape=(flat, flat, flat) + tuple(jax.ShapeDtypeStruct((size, LANES), BF16) for size in (32768, 8192, 8192, 8192, 208))
        + (jax.ShapeDtypeStruct((1, PAIR_SIZE), BF16),),
        in_specs=[pl.BlockSpec(memory_space=pltpu.VMEM)] * 4,
        out_specs=[hbm] * 9,
        scratch_shapes=[
            pltpu.VMEM((1, PAIR_SIZE), BF16),
            pltpu.VMEM((2, 4, GROUP, LANES), F32),
            dma((3,)), dma, dma,
        ],
        compiler_params=pltpu.CompilerParams(vmem_limit_bytes=12 * 1024 * 1024),
    )(*(pltpu.with_memory_space_constraint(x, pltpu.VMEM) for x in (m_new, v_new, w_new, gathered)))


def to_tiles(tensor):
    return tensor.reshape(256, 8, 4, LANES).transpose(0, 2, 1, 3).reshape(8192, LANES)


def from_tiles(rows):
    return rows.reshape(256, 4, 8, LANES).transpose(0, 2, 1, 3).reshape(16, 128, 512)


def solution(mesh):
    def local_step(g_embed, g_attn, g_ffn_in, g_ffn_out, g_vec, m_shard, v_shard, w_shard):
        vec_rows = g_vec.reshape(2, 8, 13, LANES).transpose(0, 2, 1, 3).reshape(VEC_ROWS, LANES)
        tensors = (g_embed.reshape(32768, LANES), to_tiles(g_attn), to_tiles(g_ffn_in), g_ffn_out.reshape(8192, LANES), vec_rows)
        state = [shard.reshape(SLICE_ROWS, LANES) for shard in (m_shard, v_shard, w_shard)]
        m_new, v_new, w_new, gathered = step_call(tensors, state)
        m_new, v_new, w_new, embed, attn, ffn_in, ffn_out, vec, w_pair = place_call(m_new, v_new, w_new, gathered)
        wb_vec = vec.reshape(2, 13, 8, LANES).transpose(0, 2, 1, 3).reshape(16, 1664)
        return (m_new.reshape(-1), v_new.reshape(-1), w_new.reshape(-1), embed, from_tiles(attn), from_tiles(ffn_in),
                ffn_out.reshape(16, 512, 128), wb_vec, w_pair)

    return jax.shard_map(local_step, mesh=mesh, in_specs=(P(MESH_AXES),) * 8, out_specs=(P(MESH_AXES),) * 3 + (P(),) * 5 + (P(MESH_AXES),), check_vma=False)
```

```python
import functools
import math
import jax
import jax.numpy as jnp
from jax import lax
from jax.experimental import pallas as pl
from jax.experimental.pallas import tpu as pltpu
from jax.sharding import PartitionSpec as P

MESH_AXES = ('outer', 'middle', 'inner')
ADAM_BETA1 = 0.9
ADAM_BETA2 = 0.98
ADAM_EPS = 1e-9
LEARN_RATE = 0.05
ADAM_STEP = 3
STEP_RATE = LEARN_RATE / (1.0 - ADAM_BETA1 ** ADAM_STEP)

MESH = pl.DeviceIdType.MESH
F32 = jnp.float32
BF16 = jnp.bfloat16

LANES = 128
GROUP = 32
ROWS = 7366656 // LANES
SLICE_ROWS = ROWS // 8
CHUNK_GROUPS = 24
CHUNK = CHUNK_GROUPS * GROUP
HALF = CHUNK // 2
LEAD = (4, 12)
MAIN = 8
LAST = (18,)
SIZES = LEAD + (CHUNK_GROUPS,) * MAIN + LAST
CHUNKS = len(SIZES)
RING = 4
D2D_RING = 6
SKEW = 3
OUT_RING = 5
WINDOW_GROUPS = sum(SIZES)
WINDOW = WINDOW_GROUPS * GROUP
MARGIN = GROUP
BOUNDS = (0, 1024, 1280, 1536, 1792, 1799)
PERMUTED = (1024, 1536)
VEC_ROWS = 208
VEC_AT = (BOUNDS[4] - SLICE_ROWS * 7 // GROUP) * GROUP


def window_start(device):
    return SLICE_ROWS * device // GROUP


def window_start_traced(device):
    return lax.div(device * SLICE_ROWS, GROUP)


def chunk_first(chunk):
    return sum(SIZES[:chunk])


def pieces(first, groups):
    found = []
    for tensor in range(5):
        low, high = max(first, BOUNDS[tensor]), min(first + groups, BOUNDS[tensor + 1])
        if low < high:
            row, off, size = (low - BOUNDS[tensor]) * GROUP, (low - first) * GROUP, (high - low) * GROUP
            if tensor == 4 and row + size > VEC_ROWS:
                found.append((tensor, 0, off + VEC_ROWS - row, row + size - VEC_ROWS))
                size = VEC_ROWS - row
            found.append((tensor, row, off, size))
    return tuple(found)


def split_chunks(groups):
    spans = [window_start(d) + chunk_first(c) for d in range(8) for c in range(CHUNKS) if SIZES[c] == groups]
    return [(first, pieces(first, groups)) for first in spans if len(pieces(first, groups)) > 1 or first >= BOUNDS[4]]


FIRSTS = tuple(SLICE_ROWS * d // GROUP for d in range(8)) + (BOUNDS[-1] - 1,)


def step_kernel(e_ref, a_ref, f1_ref, f2_ref, b_ref, m_ref, v_ref, w_ref,
                m_out, v_out, w_out, wg_ref,
                acc, local, p1x, p1y, p2x, p2y, gflat, wflat, m_in, stage, vec,
                stage_sem, local_sem, d2d_send, d2d_recv, sum_send, p1_recv, p2_recv, in_sem, out_send, ag_recv, relay_recv, fwd_recv):
    o, m, i = lax.axis_index('outer'), lax.axis_index('middle'), lax.axis_index('inner')
    x_dev, y_dev, p_dev = (o, 1 - m, i), (1 - o, m, i), (o, m, 1 - i)
    places = ((o, m), (o, 1 - m), (1 - o, m), (1 - o, 1 - m))
    mine = [(po * 2 + pm) * 2 + i for po, pm in places]
    theirs = [(po * 2 + pm) * 2 + (1 - i) for po, pm in places]
    start = window_start_traced(mine[0])
    shift = mine[0] * SLICE_ROWS - start * GROUP
    tensors = (e_ref, a_ref, f1_ref, f2_ref, b_ref)

    barrier = pltpu.get_barrier_semaphore()
    for device in (x_dev, y_dev, p_dev):
        pl.semaphore_signal(barrier, inc=1, device_id=device, device_id_type=MESH)

    def remote(src, dst, send, recv, device):
        pltpu.make_async_remote_copy(src_ref=src, dst_ref=dst, send_sem=send, recv_sem=recv, device_id=device, device_id_type=MESH).start()

    def drain(ref, sem):
        pltpu.make_async_copy(ref, ref, sem).wait()

    def mod(value, base):
        return value % base if isinstance(value, int) else lax.rem(value, base)

    def load_chunk(device, base, size, copy):
        groups = size // GROUP
        first = window_start_traced(device) + (base // GROUP if isinstance(base, int) else lax.div(base, GROUP))
        for tensor in range(4):
            @pl.when((first >= BOUNDS[tensor]) & (first + groups <= BOUNDS[tensor + 1]))
            def _():
                row = pl.multiple_of((first - BOUNDS[tensor]) * GROUP, GROUP)
                copy(tensors[tensor].at[pl.ds(row, size)], 0, size)
        for known, parts in split_chunks(groups):
            @pl.when(first == known)
            def _():
                for tensor, row, off, count in parts:
                    copy(tensors[tensor].at[pl.ds(row, count)], off, count)

    def load_ours(j, chunk, base, size):
        slot = mod(chunk, 3)
        load_chunk(mine[j], base, size, lambda src, off, count: pltpu.make_async_copy(
            src, local.at[slot, j, pl.ds(off, count)], local_sem.at[slot, int(j != 3)]).start())

    def issue_gradients(chunk, base, size):
        for j in (3, 1, 2, 0):
            load_chunk(theirs[j], base, size, lambda src, off, count: remote(
                src, acc.at[j, pl.ds(pl.multiple_of(base + off, 8), count)], d2d_send, d2d_recv.at[mod(chunk, D2D_RING), int(j != 3)], p_dev))
            load_ours(j, chunk, base, size)

    def add_rows(j, base, count, term):
        @pl.loop(0, count // GROUP)
        def _(r):
            off = pl.multiple_of(r * GROUP, GROUP)
            at = pl.ds(pl.multiple_of(base + off, GROUP), GROUP)
            acc[j, at] = acc[j, at] + term(off)

    def shifted(base, count):
        return base + count if isinstance(base, int) else pl.multiple_of(base + count, GROUP)

    def first_phase(chunk, base, size, cuts):
        slot, ring = mod(chunk, 3), mod(chunk, RING)
        _, x_cut, y_cut, d_cut = cuts

        def ready(j, count):
            arrived = local.at[0, pl.ds(0, count), pl.ds(0, size)]
            drain(arrived, local_sem.at[slot, j])
            drain(arrived, d2d_recv.at[mod(chunk, D2D_RING), j])

        def add(j, first, count):
            add_rows(j, shifted(base, first), count, lambda off: local[slot, j, pl.ds(first + off, GROUP)])

        def send(j, first, count, dst, place, device):
            remote(acc.at[j, pl.ds(shifted(base, first), count)], dst.at[ring, place, pl.ds(0, count)], sum_send, p1_recv.at[ring], device)

        ready(0, 1)
        add(3, 0, size)
        send(3, 0, d_cut, p1x, 1, x_dev)
        send(3, d_cut, size - d_cut, p1y, 1, y_dev)
        ready(1, 3)
        add(1, 0, x_cut)
        send(1, 0, x_cut, p1x, 0, x_dev)
        add(2, y_cut, size - y_cut)
        send(2, y_cut, size - y_cut, p1y, 0, y_dev)
        add(1, x_cut, size - x_cut)
        add(2, 0, y_cut)
        add(0, 0, size)

    def second_phase(chunk, base, size, cuts):
        ring = mod(chunk, RING)
        cut, x_cut, y_cut, _ = cuts
        drain(local.at[0, pl.ds(0, 2), pl.ds(0, size + (y_cut - x_cut) // 2)], p1_recv.at[ring])
        far = shifted(base, x_cut)
        add_rows(2, base, y_cut, lambda off: p1x[ring, 1, pl.ds(off, GROUP)])
        add_rows(1, far, size - x_cut, lambda off: p1y[ring, 1, pl.ds(off, GROUP)])
        remote(acc.at[2, pl.ds(base, y_cut)], p2y.at[ring, pl.ds(0, y_cut)], sum_send, p2_recv.at[ring], y_dev)
        remote(acc.at[1, pl.ds(far, size - x_cut)], p2x.at[ring, pl.ds(0, size - x_cut)], sum_send, p2_recv.at[ring], x_dev)
        add_rows(0, base, cut, lambda off: p1x[ring, 0, pl.ds(off, GROUP)])
        add_rows(0, shifted(base, cut), size - cut, lambda off: p1y[ring, 0, pl.ds(off, GROUP)])

    def is_permuted(group):
        return (group >= PERMUTED[0]) & (group < PERMUTED[1])

    def last_phase(chunk, base, size, cuts):
        ring = mod(chunk, RING)
        cut = cuts[0]
        first = start + (base // GROUP if isinstance(base, int) else lax.div(base, GROUP))
        drain(local.at[0, 0, pl.ds(0, size)], p2_recv.at[ring])
        for arrived, begin, count in ((p2y, 0, cut), (p2x, cut, size - cut)):
            @pl.loop(0, count // GROUP)
            def _(r):
                off = pl.multiple_of(r * GROUP, GROUP)
                row = pl.multiple_of(base + begin + off, GROUP)
                total = acc[0, pl.ds(row, GROUP)] + arrived[ring, pl.ds(off, GROUP)]
                permuted = is_permuted(first + begin // GROUP + r)

                @pl.when(permuted)
                def _():
                    for tile in range(4):
                        gflat[pl.ds(row + tile, 8, stride=4)] = total[8 * tile:8 * tile + 8]

                @pl.when(jnp.logical_not(permuted))
                def _():
                    gflat[pl.ds(row, GROUP)] = total

        if isinstance(chunk, int) and chunk == CHUNKS - 1:
            @pl.when(mine[0] == 7)
            def _():
                vec[...] = gflat[pl.ds(VEC_AT, VEC_ROWS)]
                for tile in range(26):
                    gflat[pl.ds(VEC_AT + tile // 13 * 104 + tile % 13, 8, stride=13)] = vec[8 * tile:8 * tile + 8]

    def start_loads(block, base, size):
        slot = mod(block, 2)
        count = size if not isinstance(base, int) else min(size, SLICE_ROWS - base)
        for q, ref in enumerate((m_ref, v_ref, w_ref)):
            pltpu.make_async_copy(ref.at[pl.ds(base, count)], m_in.at[slot, q, pl.ds(0, count)], in_sem.at[slot]).start()

    def adam_rows(slot, base, off, count):
        at = pl.ds(off, count)
        grad = gflat[pl.ds(base + off + shift, count)] / 8
        m_val = ADAM_BETA1 * m_in[slot, 0, at] + (1.0 - ADAM_BETA1) * grad
        v_val = ADAM_BETA2 * m_in[slot, 1, at] + (1.0 - ADAM_BETA2) * (grad * grad)
        v_hat = v_val / (1.0 - ADAM_BETA2 ** ADAM_STEP)
        w_val = m_in[slot, 2, at] - STEP_RATE * m_val / (jnp.sqrt(v_hat) + ADAM_EPS)
        out = pl.ds(pl.multiple_of(base + off, GROUP), count)
        m_out[out] = m_val
        v_out[out] = v_val
        w_out[out] = w_val
        wflat[pl.ds(pl.multiple_of(MARGIN + base + off, GROUP), count)] = w_val

    def adam(block, base, size):
        slot = mod(block, 2)
        rows = size if not isinstance(base, int) else min(size, SLICE_ROWS - base)
        drain(m_in.at[slot, :, pl.ds(0, rows)], in_sem.at[slot])

        @pl.loop(0, rows // GROUP)
        def _(r):
            adam_rows(slot, base, pl.multiple_of(r * GROUP, GROUP), GROUP)

        if rows % GROUP:
            adam_rows(slot, base, rows // GROUP * GROUP, rows % GROUP)
        first = start + (base // GROUP if isinstance(base, int) else lax.div(base, GROUP))

        @pl.loop(0, size // GROUP)
        def _(r):
            row = pl.multiple_of(base + r * GROUP, GROUP)
            source = MARGIN + row - shift
            permuted = is_permuted(first + r)

            @pl.when(permuted)
            def _():
                tiles = [wflat[pl.ds(source + tile, 8, stride=4)] for tile in range(4)]
                wg_ref[mine[0], pl.ds(row, GROUP)] = jnp.concatenate(tiles, axis=0).astype(BF16)

            @pl.when(jnp.logical_not(permuted))
            def _():
                wg_ref[mine[0], pl.ds(row, GROUP)] = wflat[pl.ds(source, GROUP)].astype(BF16)

        if isinstance(base, int) and base + size > VEC_AT:
            @pl.when(mine[0] == 7)
            def _():
                for pair in range(13):
                    row = VEC_AT + 16 * pair
                    if base <= row < base + size:
                        tiles = [wflat[pl.ds(MARGIN + VEC_AT - shift + tile // 13 * 104 + tile % 13, 8, stride=13)] for tile in (2 * pair, 2 * pair + 1)]
                        wg_ref[7, pl.ds(row, 16)] = jnp.concatenate(tiles, axis=0).astype(BF16)

        ours = wg_ref.at[mine[0], pl.ds(base, size)]
        remote(ours, ours, out_send, ag_recv.at[mod(block, OUT_RING)], x_dev)
        remote(ours, ours, out_send, ag_recv.at[mod(block, OUT_RING)], y_dev)
        remote(ours, ours, out_send, fwd_recv, p_dev)

    def relay(chunk, base, size):
        half, turn = size // 2, mod(chunk, OUT_RING)
        at, head, tail = pl.ds(base, size), pl.ds(base, half), pl.ds(shifted(base, half), half)
        drain(wg_ref.at[pl.ds(0, 2), pl.ds(0, size)], ag_recv.at[turn])
        remote(wg_ref.at[mine[1], head], wg_ref.at[mine[1], head], out_send, relay_recv.at[turn], y_dev)
        remote(wg_ref.at[mine[2], tail], wg_ref.at[mine[2], tail], out_send, relay_recv.at[turn], x_dev)
        remote(wg_ref.at[mine[1], at], wg_ref.at[mine[1], at], out_send, fwd_recv, p_dev)
        remote(wg_ref.at[mine[2], at], wg_ref.at[mine[2], at], out_send, fwd_recv, p_dev)

    def forward(chunk, base, size):
        at = pl.ds(base, size)
        drain(wg_ref.at[0, pl.ds(0, size)], relay_recv.at[mod(chunk, OUT_RING)])
        remote(wg_ref.at[mine[3], at], wg_ref.at[mine[3], at], out_send, fwd_recv, p_dev)

    begin = SIZES[0] * GROUP
    for j in (3, 1, 2, 0):
        load_chunk(theirs[j], 0, begin, lambda src, off, count: pltpu.make_async_copy(
            src, stage.at[j, pl.ds(off, count)], stage_sem.at[int(j != 3)]).start())
        load_ours(j, 0, 0, begin)
    pl.semaphore_wait(barrier, 3)
    for j in (3, 1, 2, 0):
        if j == 3:
            drain(stage.at[3], stage_sem.at[0])
        elif j == 1:
            drain(stage.at[pl.ds(0, 3)], stage_sem.at[1])
        remote(stage.at[j], acc.at[j, pl.ds(0, begin)], d2d_send, d2d_recv.at[0, int(j != 3)], p_dev)
    issue_gradients(1, chunk_first(1) * GROUP, SIZES[1] * GROUP)

    def cut_of(chip, size):
        return size // 2 + SKEW * GROUP * ((chip == 1) - (chip == 2))

    def run(chunk, action, summing):
        lead = len(LEAD)

        def halves(size):
            return ((size // 2,) * 4,) if summing else ()

        @pl.when((chunk >= lead) & (chunk < lead + MAIN))
        def _():
            action(chunk, pl.multiple_of(chunk * CHUNK + (sum(LEAD) - lead * CHUNK_GROUPS) * GROUP, GROUP), CHUNK, *halves(CHUNK))

        for other in [*range(lead), *range(lead + MAIN, CHUNKS)]:
            @pl.when(chunk == other)
            def _():
                size = SIZES[other] * GROUP
                if other < CHUNKS - 1 or not halves(size):
                    action(other, chunk_first(other) * GROUP, size, *halves(size))
                else:
                    for chip in range(4):
                        @pl.when(mine[0] // 2 == chip)
                        def _():
                            action(other, chunk_first(other) * GROUP, size, tuple(cut_of(chip ^ j, size) for j in range(4)))

    stages = ((-2, issue_gradients), (2, start_loads), (0, first_phase), (1, second_phase), (2, last_phase), (3, adam), (5, relay), (7, forward))

    @pl.loop(0, CHUNKS + stages[-1][0])
    def _(t):
        for lag, action in stages:
            run(t - lag, action, action in (first_phase, second_phase, last_phase))

    drain(acc, d2d_send)
    drain(acc.at[pl.ds(0, 3)], sum_send)
    drain(wg_ref.at[pl.ds(0, 7)], out_send)
    drain(wg_ref.at[pl.ds(0, 4)], fwd_recv)

    for d in range(1, 8):
        keep = SLICE_ROWS * d - FIRSTS[d] * GROUP
        row = lax.broadcasted_iota(jnp.int32, (GROUP, LANES), 0)
        if PERMUTED[0] <= FIRSTS[d] < PERMUTED[1]:
            row = 4 * (row % 8) + row // 8
        before = pl.ds((FIRSTS[d] - window_start(d - 1)) * GROUP, GROUP)
        after = pl.ds((FIRSTS[d] - window_start(d)) * GROUP, GROUP)
        wg_ref[d - 1, before] = jnp.where(row < keep, wg_ref[d - 1, before].astype(F32), wg_ref[d, after].astype(F32)).astype(BF16)


def step_call(tensors, state):
    hbm = pl.BlockSpec(memory_space=pl.ANY)
    dma = pltpu.SemaphoreType.DMA
    flat = pltpu.VMEM((SLICE_ROWS, LANES), F32)
    return pl.pallas_call(
        step_kernel,
        name='adam_step',
        out_shape=(flat, flat, flat, pltpu.VMEM((8, WINDOW, LANES), BF16)),
        in_specs=[hbm] * 8,
        out_specs=[pl.BlockSpec(memory_space=pltpu.VMEM)] * 4,
        scratch_shapes=[
            pltpu.VMEM((4, WINDOW, LANES), F32),
            pltpu.VMEM((3, 4, CHUNK, LANES), F32),
            pltpu.VMEM((RING, 2, HALF, LANES), F32),
            pltpu.VMEM((RING, 2, HALF, LANES), F32),
            pltpu.VMEM((RING, HALF, LANES), F32),
            pltpu.VMEM((RING, HALF, LANES), F32),
            pltpu.VMEM((WINDOW + MARGIN, LANES), F32),
            pltpu.VMEM((WINDOW + MARGIN, LANES), F32),
            pltpu.VMEM((2, 3, CHUNK, LANES), F32),
            pltpu.VMEM((4, SIZES[0] * GROUP, LANES), F32),
            pltpu.VMEM((VEC_ROWS, LANES), F32),
            dma((2,)), dma((3, 2)), dma, dma((D2D_RING, 2)), dma, dma((RING,)), dma((RING,)), dma((2,)), dma,
            dma((OUT_RING,)), dma((OUT_RING,)), dma,
        ],
        compiler_params=pltpu.CompilerParams(collective_id=0, has_side_effects=True, vmem_limit_bytes=36 * 1024 * 1024),
    )(*tensors, *state)


LAYERS = 16
PAIR_ROWS = 8192 + 3 * 2048 + 52
PAIR_SIZE = PAIR_ROWS * LANES
PARTS = 4


def place_kernel(mv_ref, vv_ref, wv_ref, wg_ref, m_out, v_out, w_out, e_ref, a_ref, f1_ref, f2_ref, b_ref, pair_ref, flat, wide, state_sem, out_sem, pair_sem):
    pair = lax.axis_index('outer') * 2 + lax.axis_index('middle')

    def put(src, dst, sem):
        pltpu.make_async_copy(src, dst, sem).start()

    for q, (src, dst) in enumerate(((mv_ref, m_out), (vv_ref, v_out), (wv_ref, w_out))):
        put(src, dst, state_sem.at[q])
    for d in range(8):
        low, high = (FIRSTS[d] + 1 if d else 0), FIRSTS[d + 1] + 1
        for q, ref in enumerate((e_ref, a_ref, f1_ref, f2_ref, b_ref)):
            begin, end = max(low, BOUNDS[q]), min(high, BOUNDS[q + 1])
            if begin < end:
                offset = (begin - BOUNDS[q]) * GROUP
                size = min((end - begin) * GROUP, ref.shape[0] - offset)
                put(wg_ref.at[d, pl.ds((begin - window_start(d)) * GROUP, size)], ref.at[pl.ds(offset, size)], out_sem)

    def finish(begin, size):
        put(flat.at[:, pl.ds(begin * LANES, size * LANES)], pair_ref.at[:, pl.ds(begin * LANES, size * LANES)], pair_sem)

    def source(group, low, last, starts):
        late = group > last
        row = (group - jnp.where(late, starts[1], starts[0])) * GROUP
        return low + jnp.where(late, 1, 0), pl.multiple_of(row, GROUP)

    embed_starts = (window_start_traced(pair), window_start_traced(pair + 1))
    for part in range(PARTS):
        @pl.loop(part * 256 // PARTS, (part + 1) * 256 // PARTS, unroll=4)
        def _(g):
            d, row = source(pair * 256 + g, pair, embed_starts[1], embed_starts)
            flat[0:1, pl.ds(pl.multiple_of(g * 4096, 4096), 4096)] = wg_ref[d, pl.ds(row, GROUP)].reshape(1, 4096)

        finish(part * 8192 // PARTS, 8192 // PARTS)

    for q in (2, 0, 1):
        low = 4 + q
        base = 8192 + 2048 * q

        @pl.loop(0, LAYERS, unroll=2)
        def _(layer):
            for g in range(4):
                d, row = source(BOUNDS[1 + q] + layer * 16 + pair * 4 + g, low, FIRSTS[low + 1], (window_start(low), window_start(low + 1)))
                group = wg_ref[d, pl.ds(row, GROUP)]
                if q < 2:
                    turn = lax.rem(layer, 2)
                    group = group.astype(F32)
                    for tile in range(4):
                        wide[turn, g, pl.ds(tile, 8, stride=4)] = group[8 * tile:8 * tile + 8]
                    group = wide[turn, g].astype(BF16)
                flat[0:1, pl.ds(pl.multiple_of((base + layer * 128 + g * GROUP) * LANES, 4096), 4096)] = group.reshape(1, 4096)

        finish(base, 2048)
    lines = []
    for half in range(2):
        tiles = [wg_ref[7, pl.ds(pl.multiple_of(VEC_AT + half * 104 + jnp.minimum(3 * pair + tile, 12) * 8, 8), 8)].astype(F32) for tile in range(5)]
        turned = pltpu.roll(jnp.concatenate(tiles, axis=1), 5 * LANES - 32 * pair, 1)
        lines += [turned[line:line + 1, :416] for line in range(8)]
    flat[0:1, pl.ds(14336 * LANES, 52 * LANES)] = jnp.concatenate(lines, axis=1).astype(BF16)
    finish(14336, 52)
    for q, (src, dst) in enumerate(((mv_ref, m_out), (vv_ref, v_out), (wv_ref, w_out))):
        pltpu.make_async_copy(src, dst, state_sem.at[q]).wait()
    every = wg_ref.at[:, pl.ds(0, SLICE_ROWS)]
    pltpu.make_async_copy(every, every, out_sem).wait()
    pltpu.make_async_copy(flat, pair_ref, pair_sem).wait()


def place_call(m_new, v_new, w_new, gathered):
    hbm = pl.BlockSpec(memory_space=pl.ANY)
    dma = pltpu.SemaphoreType.DMA
    flat = jax.ShapeDtypeStruct((SLICE_ROWS, LANES), F32)
    return pl.pallas_call(
        place_kernel,
        name='place_weights',
        out_shape=(flat, flat, flat) + tuple(jax.ShapeDtypeStruct((size, LANES), BF16) for size in (32768, 8192, 8192, 8192, 208))
        + (jax.ShapeDtypeStruct((1, PAIR_SIZE), BF16),),
        in_specs=[pl.BlockSpec(memory_space=pltpu.VMEM)] * 4,
        out_specs=[hbm] * 9,
        scratch_shapes=[
            pltpu.VMEM((1, PAIR_SIZE), BF16),
            pltpu.VMEM((2, 4, GROUP, LANES), F32),
            dma((3,)), dma, dma,
        ],
        compiler_params=pltpu.CompilerParams(vmem_limit_bytes=12 * 1024 * 1024),
    )(*(pltpu.with_memory_space_constraint(x, pltpu.VMEM) for x in (m_new, v_new, w_new, gathered)))


def to_tiles(tensor):
    return tensor.reshape(256, 8, 4, LANES).transpose(0, 2, 1, 3).reshape(8192, LANES)


def from_tiles(rows):
    return rows.reshape(256, 4, 8, LANES).transpose(0, 2, 1, 3).reshape(16, 128, 512)


def solution(mesh):
    def local_step(g_embed, g_attn, g_ffn_in, g_ffn_out, g_vec, m_shard, v_shard, w_shard):
        vec_rows = g_vec.reshape(2, 8, 13, LANES).transpose(0, 2, 1, 3).reshape(VEC_ROWS, LANES)
        tensors = (g_embed.reshape(32768, LANES), to_tiles(g_attn), to_tiles(g_ffn_in), g_ffn_out.reshape(8192, LANES), vec_rows)
        state = [shard.reshape(SLICE_ROWS, LANES) for shard in (m_shard, v_shard, w_shard)]
        m_new, v_new, w_new, gathered = step_call(tensors, state)
        m_new, v_new, w_new, embed, attn, ffn_in, ffn_out, vec, w_pair = place_call(m_new, v_new, w_new, gathered)
        wb_vec = vec.reshape(2, 13, 8, LANES).transpose(0, 2, 1, 3).reshape(16, 1664)
        return (m_new.reshape(-1), v_new.reshape(-1), w_new.reshape(-1), embed, from_tiles(attn), from_tiles(ffn_in),
                ffn_out.reshape(16, 512, 128), wb_vec, w_pair)

    return jax.shard_map(local_step, mesh=mesh, in_specs=(P(MESH_AXES),) * 8, out_specs=(P(MESH_AXES),) * 3 + (P(),) * 5 + (P(MESH_AXES),), check_vma=False)
```

```python
import functools
import math
import jax
import jax.numpy as jnp
from jax import lax
from jax.experimental import pallas as pl
from jax.experimental.pallas import tpu as pltpu
from jax.sharding import PartitionSpec as P

MESH_AXES = ('outer', 'middle', 'inner')
ADAM_BETA1 = 0.9
ADAM_BETA2 = 0.98
ADAM_EPS = 1e-9
LEARN_RATE = 0.05
ADAM_STEP = 3
STEP_RATE = LEARN_RATE / (1.0 - ADAM_BETA1 ** ADAM_STEP)

MESH = pl.DeviceIdType.MESH
F32 = jnp.float32
BF16 = jnp.bfloat16

LANES = 128
GROUP = 32
ROWS = 7366656 // LANES
SLICE_ROWS = ROWS // 8
CHUNK_GROUPS = 20
CHUNK = CHUNK_GROUPS * GROUP
HALF = CHUNK // 2
LEAD = (4, 12)
MAIN = 10
LAST = (10,)
SIZES = LEAD + (CHUNK_GROUPS,) * MAIN + LAST
CHUNKS = len(SIZES)
RING = 4
D2D_RING = 6
SKEW = 3
OUT_RING = 5
WINDOW_GROUPS = sum(SIZES)
WINDOW = WINDOW_GROUPS * GROUP
MARGIN = GROUP
BOUNDS = (0, 1024, 1280, 1536, 1792, 1799)
PERMUTED = (1024, 1536)
VEC_ROWS = 208
VEC_AT = (BOUNDS[4] - SLICE_ROWS * 7 // GROUP) * GROUP


def window_start(device):
    return SLICE_ROWS * device // GROUP


def window_start_traced(device):
    return lax.div(device * SLICE_ROWS, GROUP)


def chunk_first(chunk):
    return sum(SIZES[:chunk])


def pieces(first, groups):
    found = []
    for tensor in range(5):
        low, high = max(first, BOUNDS[tensor]), min(first + groups, BOUNDS[tensor + 1])
        if low < high:
            row, off, size = (low - BOUNDS[tensor]) * GROUP, (low - first) * GROUP, (high - low) * GROUP
            if tensor == 4 and row + size > VEC_ROWS:
                found.append((tensor, 0, off + VEC_ROWS - row, row + size - VEC_ROWS))
                size = VEC_ROWS - row
            found.append((tensor, row, off, size))
    return tuple(found)


def split_chunks(groups):
    spans = [window_start(d) + chunk_first(c) for d in range(8) for c in range(CHUNKS) if SIZES[c] == groups]
    return [(first, pieces(first, groups)) for first in spans if len(pieces(first, groups)) > 1 or first >= BOUNDS[4]]


FIRSTS = tuple(SLICE_ROWS * d // GROUP for d in range(8)) + (BOUNDS[-1] - 1,)


def step_kernel(e_ref, a_ref, f1_ref, f2_ref, b_ref, m_ref, v_ref, w_ref,
                m_out, v_out, w_out, wg_ref,
                acc, local, p1x, p1y, p2x, p2y, gflat, wflat, m_in, stage, vec,
                stage_sem, local_sem, d2d_send, d2d_recv, sum_send, p1_recv, p2_recv, in_sem, out_send, ag_recv, relay_recv, fwd_recv):
    o, m, i = lax.axis_index('outer'), lax.axis_index('middle'), lax.axis_index('inner')
    x_dev, y_dev, p_dev = (o, 1 - m, i), (1 - o, m, i), (o, m, 1 - i)
    places = ((o, m), (o, 1 - m), (1 - o, m), (1 - o, 1 - m))
    mine = [(po * 2 + pm) * 2 + i for po, pm in places]
    theirs = [(po * 2 + pm) * 2 + (1 - i) for po, pm in places]
    start = window_start_traced(mine[0])
    shift = mine[0] * SLICE_ROWS - start * GROUP
    tensors = (e_ref, a_ref, f1_ref, f2_ref, b_ref)

    barrier = pltpu.get_barrier_semaphore()
    for device in (x_dev, y_dev, p_dev):
        pl.semaphore_signal(barrier, inc=1, device_id=device, device_id_type=MESH)

    def remote(src, dst, send, recv, device):
        pltpu.make_async_remote_copy(src_ref=src, dst_ref=dst, send_sem=send, recv_sem=recv, device_id=device, device_id_type=MESH).start()

    def drain(ref, sem):
        pltpu.make_async_copy(ref, ref, sem).wait()

    def mod(value, base):
        return value % base if isinstance(value, int) else lax.rem(value, base)

    def load_chunk(device, base, size, copy):
        groups = size // GROUP
        first = window_start_traced(device) + (base // GROUP if isinstance(base, int) else lax.div(base, GROUP))
        for tensor in range(4):
            @pl.when((first >= BOUNDS[tensor]) & (first + groups <= BOUNDS[tensor + 1]))
            def _():
                row = pl.multiple_of((first - BOUNDS[tensor]) * GROUP, GROUP)
                copy(tensors[tensor].at[pl.ds(row, size)], 0, size)
        for known, parts in split_chunks(groups):
            @pl.when(first == known)
            def _():
                for tensor, row, off, count in parts:
                    copy(tensors[tensor].at[pl.ds(row, count)], off, count)

    def load_ours(j, chunk, base, size):
        slot = mod(chunk, 3)
        load_chunk(mine[j], base, size, lambda src, off, count: pltpu.make_async_copy(
            src, local.at[slot, j, pl.ds(off, count)], local_sem.at[slot, int(j != 3)]).start())

    def issue_gradients(chunk, base, size):
        for j in (3, 1, 2, 0):
            load_chunk(theirs[j], base, size, lambda src, off, count: remote(
                src, acc.at[j, pl.ds(pl.multiple_of(base + off, 8), count)], d2d_send, d2d_recv.at[mod(chunk, D2D_RING), int(j != 3)], p_dev))
            load_ours(j, chunk, base, size)

    def add_rows(j, base, count, term):
        @pl.loop(0, count // GROUP)
        def _(r):
            off = pl.multiple_of(r * GROUP, GROUP)
            at = pl.ds(pl.multiple_of(base + off, GROUP), GROUP)
            acc[j, at] = acc[j, at] + term(off)

    def shifted(base, count):
        return base + count if isinstance(base, int) else pl.multiple_of(base + count, GROUP)

    def first_phase(chunk, base, size, cuts):
        slot, ring = mod(chunk, 3), mod(chunk, RING)
        _, x_cut, y_cut, d_cut = cuts

        def ready(j, count):
            arrived = local.at[0, pl.ds(0, count), pl.ds(0, size)]
            drain(arrived, local_sem.at[slot, j])
            drain(arrived, d2d_recv.at[mod(chunk, D2D_RING), j])

        def add(j, first, count):
            add_rows(j, shifted(base, first), count, lambda off: local[slot, j, pl.ds(first + off, GROUP)])

        def send(j, first, count, dst, place, device):
            remote(acc.at[j, pl.ds(shifted(base, first), count)], dst.at[ring, place, pl.ds(0, count)], sum_send, p1_recv.at[ring], device)

        ready(0, 1)
        add(3, 0, size)
        send(3, 0, d_cut, p1x, 1, x_dev)
        send(3, d_cut, size - d_cut, p1y, 1, y_dev)
        ready(1, 3)
        add(1, 0, x_cut)
        send(1, 0, x_cut, p1x, 0, x_dev)
        add(2, y_cut, size - y_cut)
        send(2, y_cut, size - y_cut, p1y, 0, y_dev)
        add(1, x_cut, size - x_cut)
        add(2, 0, y_cut)
        add(0, 0, size)

    def second_phase(chunk, base, size, cuts):
        ring = mod(chunk, RING)
        cut, x_cut, y_cut, _ = cuts
        drain(local.at[0, pl.ds(0, 2), pl.ds(0, size + (y_cut - x_cut) // 2)], p1_recv.at[ring])
        far = shifted(base, x_cut)
        add_rows(2, base, y_cut, lambda off: p1x[ring, 1, pl.ds(off, GROUP)])
        add_rows(1, far, size - x_cut, lambda off: p1y[ring, 1, pl.ds(off, GROUP)])
        remote(acc.at[2, pl.ds(base, y_cut)], p2y.at[ring, pl.ds(0, y_cut)], sum_send, p2_recv.at[ring], y_dev)
        remote(acc.at[1, pl.ds(far, size - x_cut)], p2x.at[ring, pl.ds(0, size - x_cut)], sum_send, p2_recv.at[ring], x_dev)
        add_rows(0, base, cut, lambda off: p1x[ring, 0, pl.ds(off, GROUP)])
        add_rows(0, shifted(base, cut), size - cut, lambda off: p1y[ring, 0, pl.ds(off, GROUP)])

    def is_permuted(group):
        return (group >= PERMUTED[0]) & (group < PERMUTED[1])

    def last_phase(chunk, base, size, cuts):
        ring = mod(chunk, RING)
        cut = cuts[0]
        first = start + (base // GROUP if isinstance(base, int) else lax.div(base, GROUP))
        drain(local.at[0, 0, pl.ds(0, size)], p2_recv.at[ring])
        for arrived, begin, count in ((p2y, 0, cut), (p2x, cut, size - cut)):
            @pl.loop(0, count // GROUP)
            def _(r):
                off = pl.multiple_of(r * GROUP, GROUP)
                row = pl.multiple_of(base + begin + off, GROUP)
                total = acc[0, pl.ds(row, GROUP)] + arrived[ring, pl.ds(off, GROUP)]
                permuted = is_permuted(first + begin // GROUP + r)

                @pl.when(permuted)
                def _():
                    for tile in range(4):
                        gflat[pl.ds(row + tile, 8, stride=4)] = total[8 * tile:8 * tile + 8]

                @pl.when(jnp.logical_not(permuted))
                def _():
                    gflat[pl.ds(row, GROUP)] = total

        if isinstance(chunk, int) and chunk == CHUNKS - 1:
            @pl.when(mine[0] == 7)
            def _():
                vec[...] = gflat[pl.ds(VEC_AT, VEC_ROWS)]
                for tile in range(26):
                    gflat[pl.ds(VEC_AT + tile // 13 * 104 + tile % 13, 8, stride=13)] = vec[8 * tile:8 * tile + 8]

    def start_loads(block, base, size):
        slot = mod(block, 2)
        count = size if not isinstance(base, int) else min(size, SLICE_ROWS - base)
        for q, ref in enumerate((m_ref, v_ref, w_ref)):
            pltpu.make_async_copy(ref.at[pl.ds(base, count)], m_in.at[slot, q, pl.ds(0, count)], in_sem.at[slot]).start()

    def adam_rows(slot, base, off, count):
        at = pl.ds(off, count)
        grad = gflat[pl.ds(base + off + shift, count)] / 8
        m_val = ADAM_BETA1 * m_in[slot, 0, at] + (1.0 - ADAM_BETA1) * grad
        v_val = ADAM_BETA2 * m_in[slot, 1, at] + (1.0 - ADAM_BETA2) * (grad * grad)
        v_hat = v_val / (1.0 - ADAM_BETA2 ** ADAM_STEP)
        w_val = m_in[slot, 2, at] - STEP_RATE * m_val / (jnp.sqrt(v_hat) + ADAM_EPS)
        out = pl.ds(pl.multiple_of(base + off, GROUP), count)
        m_out[out] = m_val
        v_out[out] = v_val
        w_out[out] = w_val
        wflat[pl.ds(pl.multiple_of(MARGIN + base + off, GROUP), count)] = w_val

    def adam(block, base, size):
        slot = mod(block, 2)
        rows = size if not isinstance(base, int) else min(size, SLICE_ROWS - base)
        drain(m_in.at[slot, :, pl.ds(0, rows)], in_sem.at[slot])

        @pl.loop(0, rows // GROUP)
        def _(r):
            adam_rows(slot, base, pl.multiple_of(r * GROUP, GROUP), GROUP)

        if rows % GROUP:
            adam_rows(slot, base, rows // GROUP * GROUP, rows % GROUP)
        first = start + (base // GROUP if isinstance(base, int) else lax.div(base, GROUP))

        @pl.loop(0, size // GROUP)
        def _(r):
            row = pl.multiple_of(base + r * GROUP, GROUP)
            source = MARGIN + row - shift
            permuted = is_permuted(first + r)

            @pl.when(permuted)
            def _():
                tiles = [wflat[pl.ds(source + tile, 8, stride=4)] for tile in range(4)]
                wg_ref[mine[0], pl.ds(row, GROUP)] = jnp.concatenate(tiles, axis=0).astype(BF16)

            @pl.when(jnp.logical_not(permuted))
            def _():
                wg_ref[mine[0], pl.ds(row, GROUP)] = wflat[pl.ds(source, GROUP)].astype(BF16)

        if isinstance(base, int) and base + size > VEC_AT:
            @pl.when(mine[0] == 7)
            def _():
                for pair in range(13):
                    row = VEC_AT + 16 * pair
                    if base <= row < base + size:
                        tiles = [wflat[pl.ds(MARGIN + VEC_AT - shift + tile // 13 * 104 + tile % 13, 8, stride=13)] for tile in (2 * pair, 2 * pair + 1)]
                        wg_ref[7, pl.ds(row, 16)] = jnp.concatenate(tiles, axis=0).astype(BF16)

        ours = wg_ref.at[mine[0], pl.ds(base, size)]
        remote(ours, ours, out_send, ag_recv.at[mod(block, OUT_RING)], x_dev)
        remote(ours, ours, out_send, ag_recv.at[mod(block, OUT_RING)], y_dev)
        remote(ours, ours, out_send, fwd_recv, p_dev)

    def relay(chunk, base, size):
        half, turn = size // 2, mod(chunk, OUT_RING)
        at, head, tail = pl.ds(base, size), pl.ds(base, half), pl.ds(shifted(base, half), half)
        drain(wg_ref.at[pl.ds(0, 2), pl.ds(0, size)], ag_recv.at[turn])
        remote(wg_ref.at[mine[1], head], wg_ref.at[mine[1], head], out_send, relay_recv.at[turn], y_dev)
        remote(wg_ref.at[mine[2], tail], wg_ref.at[mine[2], tail], out_send, relay_recv.at[turn], x_dev)
        remote(wg_ref.at[mine[1], at], wg_ref.at[mine[1], at], out_send, fwd_recv, p_dev)
        remote(wg_ref.at[mine[2], at], wg_ref.at[mine[2], at], out_send, fwd_recv, p_dev)

    def forward(chunk, base, size):
        at = pl.ds(base, size)
        drain(wg_ref.at[0, pl.ds(0, size)], relay_recv.at[mod(chunk, OUT_RING)])
        remote(wg_ref.at[mine[3], at], wg_ref.at[mine[3], at], out_send, fwd_recv, p_dev)

    begin = SIZES[0] * GROUP
    for j in (3, 1, 2, 0):
        load_chunk(theirs[j], 0, begin, lambda src, off, count: pltpu.make_async_copy(
            src, stage.at[j, pl.ds(off, count)], stage_sem.at[int(j != 3)]).start())
        load_ours(j, 0, 0, begin)
    pl.semaphore_wait(barrier, 3)
    for j in (3, 1, 2, 0):
        if j == 3:
            drain(stage.at[3], stage_sem.at[0])
        elif j == 1:
            drain(stage.at[pl.ds(0, 3)], stage_sem.at[1])
        remote(stage.at[j], acc.at[j, pl.ds(0, begin)], d2d_send, d2d_recv.at[0, int(j != 3)], p_dev)
    issue_gradients(1, chunk_first(1) * GROUP, SIZES[1] * GROUP)

    def cut_of(chip, size):
        return size // 2 + SKEW * GROUP * ((chip == 1) - (chip == 2))

    def run(chunk, action, summing):
        lead = len(LEAD)

        def halves(size):
            return ((size // 2,) * 4,) if summing else ()

        @pl.when((chunk >= lead) & (chunk < lead + MAIN))
        def _():
            action(chunk, pl.multiple_of(chunk * CHUNK + (sum(LEAD) - lead * CHUNK_GROUPS) * GROUP, GROUP), CHUNK, *halves(CHUNK))

        for other in [*range(lead), *range(lead + MAIN, CHUNKS)]:
            @pl.when(chunk == other)
            def _():
                size = SIZES[other] * GROUP
                if other < CHUNKS - 1 or not halves(size):
                    action(other, chunk_first(other) * GROUP, size, *halves(size))
                else:
                    for chip in range(4):
                        @pl.when(mine[0] // 2 == chip)
                        def _():
                            action(other, chunk_first(other) * GROUP, size, tuple(cut_of(chip ^ j, size) for j in range(4)))

    stages = ((-2, issue_gradients), (2, start_loads), (0, first_phase), (1, second_phase), (2, last_phase), (3, adam), (5, relay), (7, forward))

    @pl.loop(0, CHUNKS + stages[-1][0])
    def _(t):
        for lag, action in stages:
            run(t - lag, action, action in (first_phase, second_phase, last_phase))

    drain(acc, d2d_send)
    drain(acc.at[pl.ds(0, 3)], sum_send)
    drain(wg_ref.at[pl.ds(0, 7)], out_send)
    drain(wg_ref.at[pl.ds(0, 4)], fwd_recv)

    for d in range(1, 8):
        keep = SLICE_ROWS * d - FIRSTS[d] * GROUP
        row = lax.broadcasted_iota(jnp.int32, (GROUP, LANES), 0)
        if PERMUTED[0] <= FIRSTS[d] < PERMUTED[1]:
            row = 4 * (row % 8) + row // 8
        before = pl.ds((FIRSTS[d] - window_start(d - 1)) * GROUP, GROUP)
        after = pl.ds((FIRSTS[d] - window_start(d)) * GROUP, GROUP)
        wg_ref[d - 1, before] = jnp.where(row < keep, wg_ref[d - 1, before].astype(F32), wg_ref[d, after].astype(F32)).astype(BF16)


def step_call(tensors, state):
    hbm = pl.BlockSpec(memory_space=pl.ANY)
    dma = pltpu.SemaphoreType.DMA
    flat = pltpu.VMEM((SLICE_ROWS, LANES), F32)
    return pl.pallas_call(
        step_kernel,
        name='adam_step',
        out_shape=(flat, flat, flat, pltpu.VMEM((8, WINDOW, LANES), BF16)),
        in_specs=[hbm] * 8,
        out_specs=[pl.BlockSpec(memory_space=pltpu.VMEM)] * 4,
        scratch_shapes=[
            pltpu.VMEM((4, WINDOW, LANES), F32),
            pltpu.VMEM((3, 4, CHUNK, LANES), F32),
            pltpu.VMEM((RING, 2, HALF, LANES), F32),
            pltpu.VMEM((RING, 2, HALF, LANES), F32),
            pltpu.VMEM((RING, HALF, LANES), F32),
            pltpu.VMEM((RING, HALF, LANES), F32),
            pltpu.VMEM((WINDOW + MARGIN, LANES), F32),
            pltpu.VMEM((WINDOW + MARGIN, LANES), F32),
            pltpu.VMEM((2, 3, CHUNK, LANES), F32),
            pltpu.VMEM((4, SIZES[0] * GROUP, LANES), F32),
            pltpu.VMEM((VEC_ROWS, LANES), F32),
            dma((2,)), dma((3, 2)), dma, dma((D2D_RING, 2)), dma, dma((RING,)), dma((RING,)), dma((2,)), dma,
            dma((OUT_RING,)), dma((OUT_RING,)), dma,
        ],
        compiler_params=pltpu.CompilerParams(collective_id=0, has_side_effects=True, vmem_limit_bytes=36 * 1024 * 1024),
    )(*tensors, *state)


LAYERS = 16
PAIR_ROWS = 8192 + 3 * 2048 + 52
PAIR_SIZE = PAIR_ROWS * LANES
PARTS = 4


def place_kernel(mv_ref, vv_ref, wv_ref, wg_ref, m_out, v_out, w_out, e_ref, a_ref, f1_ref, f2_ref, b_ref, pair_ref, flat, wide, state_sem, out_sem, pair_sem):
    pair = lax.axis_index('outer') * 2 + lax.axis_index('middle')

    def put(src, dst, sem):
        pltpu.make_async_copy(src, dst, sem).start()

    for q, (src, dst) in enumerate(((mv_ref, m_out), (vv_ref, v_out), (wv_ref, w_out))):
        put(src, dst, state_sem.at[q])
    for d in range(8):
        low, high = (FIRSTS[d] + 1 if d else 0), FIRSTS[d + 1] + 1
        for q, ref in enumerate((e_ref, a_ref, f1_ref, f2_ref, b_ref)):
            begin, end = max(low, BOUNDS[q]), min(high, BOUNDS[q + 1])
            if begin < end:
                offset = (begin - BOUNDS[q]) * GROUP
                size = min((end - begin) * GROUP, ref.shape[0] - offset)
                put(wg_ref.at[d, pl.ds((begin - window_start(d)) * GROUP, size)], ref.at[pl.ds(offset, size)], out_sem)

    def finish(begin, size):
        put(flat.at[:, pl.ds(begin * LANES, size * LANES)], pair_ref.at[:, pl.ds(begin * LANES, size * LANES)], pair_sem)

    def source(group, low, last, starts):
        late = group > last
        row = (group - jnp.where(late, starts[1], starts[0])) * GROUP
        return low + jnp.where(late, 1, 0), pl.multiple_of(row, GROUP)

    embed_starts = (window_start_traced(pair), window_start_traced(pair + 1))
    for part in range(PARTS):
        @pl.loop(part * 256 // PARTS, (part + 1) * 256 // PARTS, unroll=4)
        def _(g):
            d, row = source(pair * 256 + g, pair, embed_starts[1], embed_starts)
            flat[0:1, pl.ds(pl.multiple_of(g * 4096, 4096), 4096)] = wg_ref[d, pl.ds(row, GROUP)].reshape(1, 4096)

        finish(part * 8192 // PARTS, 8192 // PARTS)

    for q in (2, 0, 1):
        low = 4 + q
        base = 8192 + 2048 * q

        @pl.loop(0, LAYERS, unroll=2)
        def _(layer):
            for g in range(4):
                d, row = source(BOUNDS[1 + q] + layer * 16 + pair * 4 + g, low, FIRSTS[low + 1], (window_start(low), window_start(low + 1)))
                group = wg_ref[d, pl.ds(row, GROUP)]
                if q < 2:
                    turn = lax.rem(layer, 2)
                    group = group.astype(F32)
                    for tile in range(4):
                        wide[turn, g, pl.ds(tile, 8, stride=4)] = group[8 * tile:8 * tile + 8]
                    group = wide[turn, g].astype(BF16)
                flat[0:1, pl.ds(pl.multiple_of((base + layer * 128 + g * GROUP) * LANES, 4096), 4096)] = group.reshape(1, 4096)

        finish(base, 2048)
    lines = []
    for half in range(2):
        tiles = [wg_ref[7, pl.ds(pl.multiple_of(VEC_AT + half * 104 + jnp.minimum(3 * pair + tile, 12) * 8, 8), 8)].astype(F32) for tile in range(5)]
        turned = pltpu.roll(jnp.concatenate(tiles, axis=1), 5 * LANES - 32 * pair, 1)
        lines += [turned[line:line + 1, :416] for line in range(8)]
    flat[0:1, pl.ds(14336 * LANES, 52 * LANES)] = jnp.concatenate(lines, axis=1).astype(BF16)
    finish(14336, 52)
    for q, (src, dst) in enumerate(((mv_ref, m_out), (vv_ref, v_out), (wv_ref, w_out))):
        pltpu.make_async_copy(src, dst, state_sem.at[q]).wait()
    every = wg_ref.at[:, pl.ds(0, SLICE_ROWS)]
    pltpu.make_async_copy(every, every, out_sem).wait()
    pltpu.make_async_copy(flat, pair_ref, pair_sem).wait()


def place_call(m_new, v_new, w_new, gathered):
    hbm = pl.BlockSpec(memory_space=pl.ANY)
    dma = pltpu.SemaphoreType.DMA
    flat = jax.ShapeDtypeStruct((SLICE_ROWS, LANES), F32)
    return pl.pallas_call(
        place_kernel,
        name='place_weights',
        out_shape=(flat, flat, flat) + tuple(jax.ShapeDtypeStruct((size, LANES), BF16) for size in (32768, 8192, 8192, 8192, 208))
        + (jax.ShapeDtypeStruct((1, PAIR_SIZE), BF16),),
        in_specs=[pl.BlockSpec(memory_space=pltpu.VMEM)] * 4,
        out_specs=[hbm] * 9,
        scratch_shapes=[
            pltpu.VMEM((1, PAIR_SIZE), BF16),
            pltpu.VMEM((2, 4, GROUP, LANES), F32),
            dma((3,)), dma, dma,
        ],
        compiler_params=pltpu.CompilerParams(vmem_limit_bytes=12 * 1024 * 1024),
    )(*(pltpu.with_memory_space_constraint(x, pltpu.VMEM) for x in (m_new, v_new, w_new, gathered)))


def to_tiles(tensor):
    return tensor.reshape(256, 8, 4, LANES).transpose(0, 2, 1, 3).reshape(8192, LANES)


def from_tiles(rows):
    return rows.reshape(256, 4, 8, LANES).transpose(0, 2, 1, 3).reshape(16, 128, 512)


def solution(mesh):
    def local_step(g_embed, g_attn, g_ffn_in, g_ffn_out, g_vec, m_shard, v_shard, w_shard):
        vec_rows = g_vec.reshape(2, 8, 13, LANES).transpose(0, 2, 1, 3).reshape(VEC_ROWS, LANES)
        tensors = (g_embed.reshape(32768, LANES), to_tiles(g_attn), to_tiles(g_ffn_in), g_ffn_out.reshape(8192, LANES), vec_rows)
        state = [shard.reshape(SLICE_ROWS, LANES) for shard in (m_shard, v_shard, w_shard)]
        m_new, v_new, w_new, gathered = step_call(tensors, state)
        m_new, v_new, w_new, embed, attn, ffn_in, ffn_out, vec, w_pair = place_call(m_new, v_new, w_new, gathered)
        wb_vec = vec.reshape(2, 13, 8, LANES).transpose(0, 2, 1, 3).reshape(16, 1664)
        return (m_new.reshape(-1), v_new.reshape(-1), w_new.reshape(-1), embed, from_tiles(attn), from_tiles(ffn_in),
                ffn_out.reshape(16, 512, 128), wb_vec, w_pair)

    return jax.shard_map(local_step, mesh=mesh, in_specs=(P(MESH_AXES),) * 8, out_specs=(P(MESH_AXES),) * 3 + (P(),) * 5 + (P(MESH_AXES),), check_vma=False)
```

```python
import functools
import math
import jax
import jax.numpy as jnp
from jax import lax
from jax.experimental import pallas as pl
from jax.experimental.pallas import tpu as pltpu
from jax.sharding import PartitionSpec as P

MESH_AXES = ('outer', 'middle', 'inner')
ADAM_BETA1 = 0.9
ADAM_BETA2 = 0.98
ADAM_EPS = 1e-9
LEARN_RATE = 0.05
ADAM_STEP = 3
STEP_RATE = LEARN_RATE / (1.0 - ADAM_BETA1 ** ADAM_STEP)

MESH = pl.DeviceIdType.MESH
F32 = jnp.float32
BF16 = jnp.bfloat16

LANES = 128
GROUP = 32
ROWS = 7366656 // LANES
SLICE_ROWS = ROWS // 8
CHUNK_GROUPS = 24
CHUNK = CHUNK_GROUPS * GROUP
HALF = CHUNK // 2
LEAD = (4, 16)
MAIN = 8
LAST = (14,)
SIZES = LEAD + (CHUNK_GROUPS,) * MAIN + LAST
CHUNKS = len(SIZES)
RING = 4
D2D_RING = 6
SKEW = 3
OUT_RING = 5
WINDOW_GROUPS = sum(SIZES)
WINDOW = WINDOW_GROUPS * GROUP
MARGIN = GROUP
BOUNDS = (0, 1024, 1280, 1536, 1792, 1799)
PERMUTED = (1024, 1536)
VEC_ROWS = 208
VEC_AT = (BOUNDS[4] - SLICE_ROWS * 7 // GROUP) * GROUP


def window_start(device):
    return SLICE_ROWS * device // GROUP


def window_start_traced(device):
    return lax.div(device * SLICE_ROWS, GROUP)


def chunk_first(chunk):
    return sum(SIZES[:chunk])


def pieces(first, groups):
    found = []
    for tensor in range(5):
        low, high = max(first, BOUNDS[tensor]), min(first + groups, BOUNDS[tensor + 1])
        if low < high:
            row, off, size = (low - BOUNDS[tensor]) * GROUP, (low - first) * GROUP, (high - low) * GROUP
            if tensor == 4 and row + size > VEC_ROWS:
                found.append((tensor, 0, off + VEC_ROWS - row, row + size - VEC_ROWS))
                size = VEC_ROWS - row
            found.append((tensor, row, off, size))
    return tuple(found)


def split_chunks(groups):
    spans = [window_start(d) + chunk_first(c) for d in range(8) for c in range(CHUNKS) if SIZES[c] == groups]
    return [(first, pieces(first, groups)) for first in spans if len(pieces(first, groups)) > 1 or first >= BOUNDS[4]]


FIRSTS = tuple(SLICE_ROWS * d // GROUP for d in range(8)) + (BOUNDS[-1] - 1,)


def step_kernel(e_ref, a_ref, f1_ref, f2_ref, b_ref, m_ref, v_ref, w_ref,
                m_out, v_out, w_out, wg_ref,
                acc, local, p1x, p1y, p2x, p2y, gflat, wflat, m_in, stage, vec,
                stage_sem, local_sem, d2d_send, d2d_recv, sum_send, p1_recv, p2_recv, in_sem, out_send, ag_recv, relay_recv, fwd_recv):
    o, m, i = lax.axis_index('outer'), lax.axis_index('middle'), lax.axis_index('inner')
    x_dev, y_dev, p_dev = (o, 1 - m, i), (1 - o, m, i), (o, m, 1 - i)
    places = ((o, m), (o, 1 - m), (1 - o, m), (1 - o, 1 - m))
    mine = [(po * 2 + pm) * 2 + i for po, pm in places]
    theirs = [(po * 2 + pm) * 2 + (1 - i) for po, pm in places]
    start = window_start_traced(mine[0])
    shift = mine[0] * SLICE_ROWS - start * GROUP
    tensors = (e_ref, a_ref, f1_ref, f2_ref, b_ref)

    barrier = pltpu.get_barrier_semaphore()
    for device in (x_dev, y_dev, p_dev):
        pl.semaphore_signal(barrier, inc=1, device_id=device, device_id_type=MESH)

    def remote(src, dst, send, recv, device):
        pltpu.make_async_remote_copy(src_ref=src, dst_ref=dst, send_sem=send, recv_sem=recv, device_id=device, device_id_type=MESH).start()

    def drain(ref, sem):
        pltpu.make_async_copy(ref, ref, sem).wait()

    def mod(value, base):
        return value % base if isinstance(value, int) else lax.rem(value, base)

    def load_chunk(device, base, size, copy):
        groups = size // GROUP
        first = window_start_traced(device) + (base // GROUP if isinstance(base, int) else lax.div(base, GROUP))
        for tensor in range(4):
            @pl.when((first >= BOUNDS[tensor]) & (first + groups <= BOUNDS[tensor + 1]))
            def _():
                row = pl.multiple_of((first - BOUNDS[tensor]) * GROUP, GROUP)
                copy(tensors[tensor].at[pl.ds(row, size)], 0, size)
        for known, parts in split_chunks(groups):
            @pl.when(first == known)
            def _():
                for tensor, row, off, count in parts:
                    copy(tensors[tensor].at[pl.ds(row, count)], off, count)

    def load_ours(j, chunk, base, size):
        slot = mod(chunk, 3)
        load_chunk(mine[j], base, size, lambda src, off, count: pltpu.make_async_copy(
            src, local.at[slot, j, pl.ds(off, count)], local_sem.at[slot, int(j != 3)]).start())

    def issue_gradients(chunk, base, size):
        for j in (3, 1, 2, 0):
            load_chunk(theirs[j], base, size, lambda src, off, count: remote(
                src, acc.at[j, pl.ds(pl.multiple_of(base + off, 8), count)], d2d_send, d2d_recv.at[mod(chunk, D2D_RING), int(j != 3)], p_dev))
            load_ours(j, chunk, base, size)

    def add_rows(j, base, count, term):
        @pl.loop(0, count // GROUP)
        def _(r):
            off = pl.multiple_of(r * GROUP, GROUP)
            at = pl.ds(pl.multiple_of(base + off, GROUP), GROUP)
            acc[j, at] = acc[j, at] + term(off)

    def shifted(base, count):
        return base + count if isinstance(base, int) else pl.multiple_of(base + count, GROUP)

    def first_phase(chunk, base, size, cuts):
        slot, ring = mod(chunk, 3), mod(chunk, RING)
        _, x_cut, y_cut, d_cut = cuts

        def ready(j, count):
            arrived = local.at[0, pl.ds(0, count), pl.ds(0, size)]
            drain(arrived, local_sem.at[slot, j])
            drain(arrived, d2d_recv.at[mod(chunk, D2D_RING), j])

        def add(j, first, count):
            add_rows(j, shifted(base, first), count, lambda off: local[slot, j, pl.ds(first + off, GROUP)])

        def send(j, first, count, dst, place, device):
            remote(acc.at[j, pl.ds(shifted(base, first), count)], dst.at[ring, place, pl.ds(0, count)], sum_send, p1_recv.at[ring], device)

        ready(0, 1)
        add(3, 0, size)
        send(3, 0, d_cut, p1x, 1, x_dev)
        send(3, d_cut, size - d_cut, p1y, 1, y_dev)
        ready(1, 3)
        add(1, 0, x_cut)
        send(1, 0, x_cut, p1x, 0, x_dev)
        add(2, y_cut, size - y_cut)
        send(2, y_cut, size - y_cut, p1y, 0, y_dev)
        add(1, x_cut, size - x_cut)
        add(2, 0, y_cut)
        add(0, 0, size)

    def second_phase(chunk, base, size, cuts):
        ring = mod(chunk, RING)
        cut, x_cut, y_cut, _ = cuts
        drain(local.at[0, pl.ds(0, 2), pl.ds(0, size + (y_cut - x_cut) // 2)], p1_recv.at[ring])
        far = shifted(base, x_cut)
        add_rows(2, base, y_cut, lambda off: p1x[ring, 1, pl.ds(off, GROUP)])
        add_rows(1, far, size - x_cut, lambda off: p1y[ring, 1, pl.ds(off, GROUP)])
        remote(acc.at[2, pl.ds(base, y_cut)], p2y.at[ring, pl.ds(0, y_cut)], sum_send, p2_recv.at[ring], y_dev)
        remote(acc.at[1, pl.ds(far, size - x_cut)], p2x.at[ring, pl.ds(0, size - x_cut)], sum_send, p2_recv.at[ring], x_dev)
        add_rows(0, base, cut, lambda off: p1x[ring, 0, pl.ds(off, GROUP)])
        add_rows(0, shifted(base, cut), size - cut, lambda off: p1y[ring, 0, pl.ds(off, GROUP)])

    def is_permuted(group):
        return (group >= PERMUTED[0]) & (group < PERMUTED[1])

    def last_phase(chunk, base, size, cuts):
        ring = mod(chunk, RING)
        cut = cuts[0]
        first = start + (base // GROUP if isinstance(base, int) else lax.div(base, GROUP))
        drain(local.at[0, 0, pl.ds(0, size)], p2_recv.at[ring])
        for arrived, begin, count in ((p2y, 0, cut), (p2x, cut, size - cut)):
            @pl.loop(0, count // GROUP)
            def _(r):
                off = pl.multiple_of(r * GROUP, GROUP)
                row = pl.multiple_of(base + begin + off, GROUP)
                total = acc[0, pl.ds(row, GROUP)] + arrived[ring, pl.ds(off, GROUP)]
                permuted = is_permuted(first + begin // GROUP + r)

                @pl.when(permuted)
                def _():
                    for tile in range(4):
                        gflat[pl.ds(row + tile, 8, stride=4)] = total[8 * tile:8 * tile + 8]

                @pl.when(jnp.logical_not(permuted))
                def _():
                    gflat[pl.ds(row, GROUP)] = total

        if isinstance(chunk, int) and chunk == CHUNKS - 1:
            @pl.when(mine[0] == 7)
            def _():
                vec[...] = gflat[pl.ds(VEC_AT, VEC_ROWS)]
                for tile in range(26):
                    gflat[pl.ds(VEC_AT + tile // 13 * 104 + tile % 13, 8, stride=13)] = vec[8 * tile:8 * tile + 8]

    def start_loads(block, base, size):
        slot = mod(block, 2)
        count = size if not isinstance(base, int) else min(size, SLICE_ROWS - base)
        for q, ref in enumerate((m_ref, v_ref, w_ref)):
            pltpu.make_async_copy(ref.at[pl.ds(base, count)], m_in.at[slot, q, pl.ds(0, count)], in_sem.at[slot]).start()

    def adam_rows(slot, base, off, count):
        at = pl.ds(off, count)
        grad = gflat[pl.ds(base + off + shift, count)] / 8
        m_val = ADAM_BETA1 * m_in[slot, 0, at] + (1.0 - ADAM_BETA1) * grad
        v_val = ADAM_BETA2 * m_in[slot, 1, at] + (1.0 - ADAM_BETA2) * (grad * grad)
        v_hat = v_val / (1.0 - ADAM_BETA2 ** ADAM_STEP)
        w_val = m_in[slot, 2, at] - STEP_RATE * m_val / (jnp.sqrt(v_hat) + ADAM_EPS)
        out = pl.ds(pl.multiple_of(base + off, GROUP), count)
        m_out[out] = m_val
        v_out[out] = v_val
        w_out[out] = w_val
        wflat[pl.ds(pl.multiple_of(MARGIN + base + off, GROUP), count)] = w_val

    def adam(block, base, size):
        slot = mod(block, 2)
        rows = size if not isinstance(base, int) else min(size, SLICE_ROWS - base)
        drain(m_in.at[slot, :, pl.ds(0, rows)], in_sem.at[slot])

        @pl.loop(0, rows // GROUP)
        def _(r):
            adam_rows(slot, base, pl.multiple_of(r * GROUP, GROUP), GROUP)

        if rows % GROUP:
            adam_rows(slot, base, rows // GROUP * GROUP, rows % GROUP)
        first = start + (base // GROUP if isinstance(base, int) else lax.div(base, GROUP))

        @pl.loop(0, size // GROUP)
        def _(r):
            row = pl.multiple_of(base + r * GROUP, GROUP)
            source = MARGIN + row - shift
            permuted = is_permuted(first + r)

            @pl.when(permuted)
            def _():
                tiles = [wflat[pl.ds(source + tile, 8, stride=4)] for tile in range(4)]
                wg_ref[mine[0], pl.ds(row, GROUP)] = jnp.concatenate(tiles, axis=0).astype(BF16)

            @pl.when(jnp.logical_not(permuted))
            def _():
                wg_ref[mine[0], pl.ds(row, GROUP)] = wflat[pl.ds(source, GROUP)].astype(BF16)

        if isinstance(base, int) and base + size > VEC_AT:
            @pl.when(mine[0] == 7)
            def _():
                for pair in range(13):
                    row = VEC_AT + 16 * pair
                    if base <= row < base + size:
                        tiles = [wflat[pl.ds(MARGIN + VEC_AT - shift + tile // 13 * 104 + tile % 13, 8, stride=13)] for tile in (2 * pair, 2 * pair + 1)]
                        wg_ref[7, pl.ds(row, 16)] = jnp.concatenate(tiles, axis=0).astype(BF16)

        ours = wg_ref.at[mine[0], pl.ds(base, size)]
        remote(ours, ours, out_send, ag_recv.at[mod(block, OUT_RING)], x_dev)
        remote(ours, ours, out_send, ag_recv.at[mod(block, OUT_RING)], y_dev)
        remote(ours, ours, out_send, fwd_recv, p_dev)

    def relay(chunk, base, size):
        half, turn = size // 2, mod(chunk, OUT_RING)
        at, head, tail = pl.ds(base, size), pl.ds(base, half), pl.ds(shifted(base, half), half)
        drain(wg_ref.at[pl.ds(0, 2), pl.ds(0, size)], ag_recv.at[turn])
        remote(wg_ref.at[mine[1], head], wg_ref.at[mine[1], head], out_send, relay_recv.at[turn], y_dev)
        remote(wg_ref.at[mine[2], tail], wg_ref.at[mine[2], tail], out_send, relay_recv.at[turn], x_dev)
        remote(wg_ref.at[mine[1], at], wg_ref.at[mine[1], at], out_send, fwd_recv, p_dev)
        remote(wg_ref.at[mine[2], at], wg_ref.at[mine[2], at], out_send, fwd_recv, p_dev)

    def forward(chunk, base, size):
        at = pl.ds(base, size)
        drain(wg_ref.at[0, pl.ds(0, size)], relay_recv.at[mod(chunk, OUT_RING)])
        remote(wg_ref.at[mine[3], at], wg_ref.at[mine[3], at], out_send, fwd_recv, p_dev)

    begin = SIZES[0] * GROUP
    for j in (3, 1, 2, 0):
        load_chunk(theirs[j], 0, begin, lambda src, off, count: pltpu.make_async_copy(
            src, stage.at[j, pl.ds(off, count)], stage_sem.at[int(j != 3)]).start())
        load_ours(j, 0, 0, begin)
    pl.semaphore_wait(barrier, 3)
    for j in (3, 1, 2, 0):
        if j == 3:
            drain(stage.at[3], stage_sem.at[0])
        elif j == 1:
            drain(stage.at[pl.ds(0, 3)], stage_sem.at[1])
        remote(stage.at[j], acc.at[j, pl.ds(0, begin)], d2d_send, d2d_recv.at[0, int(j != 3)], p_dev)
    issue_gradients(1, chunk_first(1) * GROUP, SIZES[1] * GROUP)

    def cut_of(chip, size):
        return size // 2 + SKEW * GROUP * ((chip == 1) - (chip == 2))

    def run(chunk, action, summing):
        lead = len(LEAD)

        def halves(size):
            return ((size // 2,) * 4,) if summing else ()

        @pl.when((chunk >= lead) & (chunk < lead + MAIN))
        def _():
            action(chunk, pl.multiple_of(chunk * CHUNK + (sum(LEAD) - lead * CHUNK_GROUPS) * GROUP, GROUP), CHUNK, *halves(CHUNK))

        for other in [*range(lead), *range(lead + MAIN, CHUNKS)]:
            @pl.when(chunk == other)
            def _():
                size = SIZES[other] * GROUP
                if other < CHUNKS - 1 or not halves(size):
                    action(other, chunk_first(other) * GROUP, size, *halves(size))
                else:
                    for chip in range(4):
                        @pl.when(mine[0] // 2 == chip)
                        def _():
                            action(other, chunk_first(other) * GROUP, size, tuple(cut_of(chip ^ j, size) for j in range(4)))

    stages = ((-2, issue_gradients), (2, start_loads), (0, first_phase), (1, second_phase), (2, last_phase), (3, adam), (5, relay), (7, forward))

    @pl.loop(0, CHUNKS + stages[-1][0])
    def _(t):
        for lag, action in stages:
            run(t - lag, action, action in (first_phase, second_phase, last_phase))

    drain(acc, d2d_send)
    drain(acc.at[pl.ds(0, 3)], sum_send)
    drain(wg_ref.at[pl.ds(0, 7)], out_send)
    drain(wg_ref.at[pl.ds(0, 4)], fwd_recv)

    for d in range(1, 8):
        keep = SLICE_ROWS * d - FIRSTS[d] * GROUP
        row = lax.broadcasted_iota(jnp.int32, (GROUP, LANES), 0)
        if PERMUTED[0] <= FIRSTS[d] < PERMUTED[1]:
            row = 4 * (row % 8) + row // 8
        before = pl.ds((FIRSTS[d] - window_start(d - 1)) * GROUP, GROUP)
        after = pl.ds((FIRSTS[d] - window_start(d)) * GROUP, GROUP)
        wg_ref[d - 1, before] = jnp.where(row < keep, wg_ref[d - 1, before].astype(F32), wg_ref[d, after].astype(F32)).astype(BF16)


def step_call(tensors, state):
    hbm = pl.BlockSpec(memory_space=pl.ANY)
    dma = pltpu.SemaphoreType.DMA
    flat = pltpu.VMEM((SLICE_ROWS, LANES), F32)
    return pl.pallas_call(
        step_kernel,
        name='adam_step',
        out_shape=(flat, flat, flat, pltpu.VMEM((8, WINDOW, LANES), BF16)),
        in_specs=[hbm] * 8,
        out_specs=[pl.BlockSpec(memory_space=pltpu.VMEM)] * 4,
        scratch_shapes=[
            pltpu.VMEM((4, WINDOW, LANES), F32),
            pltpu.VMEM((3, 4, CHUNK, LANES), F32),
            pltpu.VMEM((RING, 2, HALF, LANES), F32),
            pltpu.VMEM((RING, 2, HALF, LANES), F32),
            pltpu.VMEM((RING, HALF, LANES), F32),
            pltpu.VMEM((RING, HALF, LANES), F32),
            pltpu.VMEM((WINDOW + MARGIN, LANES), F32),
            pltpu.VMEM((WINDOW + MARGIN, LANES), F32),
            pltpu.VMEM((2, 3, CHUNK, LANES), F32),
            pltpu.VMEM((4, SIZES[0] * GROUP, LANES), F32),
            pltpu.VMEM((VEC_ROWS, LANES), F32),
            dma((2,)), dma((3, 2)), dma, dma((D2D_RING, 2)), dma, dma((RING,)), dma((RING,)), dma((2,)), dma,
            dma((OUT_RING,)), dma((OUT_RING,)), dma,
        ],
        compiler_params=pltpu.CompilerParams(collective_id=0, has_side_effects=True, vmem_limit_bytes=36 * 1024 * 1024),
    )(*tensors, *state)


LAYERS = 16
PAIR_ROWS = 8192 + 3 * 2048 + 52
PAIR_SIZE = PAIR_ROWS * LANES
PARTS = 4


def place_kernel(mv_ref, vv_ref, wv_ref, wg_ref, m_out, v_out, w_out, e_ref, a_ref, f1_ref, f2_ref, b_ref, pair_ref, flat, wide, state_sem, out_sem, pair_sem):
    pair = lax.axis_index('outer') * 2 + lax.axis_index('middle')

    def put(src, dst, sem):
        pltpu.make_async_copy(src, dst, sem).start()

    for q, (src, dst) in enumerate(((mv_ref, m_out), (vv_ref, v_out), (wv_ref, w_out))):
        put(src, dst, state_sem.at[q])
    for d in range(8):
        low, high = (FIRSTS[d] + 1 if d else 0), FIRSTS[d + 1] + 1
        for q, ref in enumerate((e_ref, a_ref, f1_ref, f2_ref, b_ref)):
            begin, end = max(low, BOUNDS[q]), min(high, BOUNDS[q + 1])
            if begin < end:
                offset = (begin - BOUNDS[q]) * GROUP
                size = min((end - begin) * GROUP, ref.shape[0] - offset)
                put(wg_ref.at[d, pl.ds((begin - window_start(d)) * GROUP, size)], ref.at[pl.ds(offset, size)], out_sem)

    def finish(begin, size):
        put(flat.at[:, pl.ds(begin * LANES, size * LANES)], pair_ref.at[:, pl.ds(begin * LANES, size * LANES)], pair_sem)

    def source(group, low, last, starts):
        late = group > last
        row = (group - jnp.where(late, starts[1], starts[0])) * GROUP
        return low + jnp.where(late, 1, 0), pl.multiple_of(row, GROUP)

    embed_starts = (window_start_traced(pair), window_start_traced(pair + 1))
    for part in range(PARTS):
        @pl.loop(part * 256 // PARTS, (part + 1) * 256 // PARTS, unroll=4)
        def _(g):
            d, row = source(pair * 256 + g, pair, embed_starts[1], embed_starts)
            flat[0:1, pl.ds(pl.multiple_of(g * 4096, 4096), 4096)] = wg_ref[d, pl.ds(row, GROUP)].reshape(1, 4096)

        finish(part * 8192 // PARTS, 8192 // PARTS)

    for q in (2, 0, 1):
        low = 4 + q
        base = 8192 + 2048 * q

        @pl.loop(0, LAYERS, unroll=2)
        def _(layer):
            for g in range(4):
                d, row = source(BOUNDS[1 + q] + layer * 16 + pair * 4 + g, low, FIRSTS[low + 1], (window_start(low), window_start(low + 1)))
                group = wg_ref[d, pl.ds(row, GROUP)]
                if q < 2:
                    turn = lax.rem(layer, 2)
                    group = group.astype(F32)
                    for tile in range(4):
                        wide[turn, g, pl.ds(tile, 8, stride=4)] = group[8 * tile:8 * tile + 8]
                    group = wide[turn, g].astype(BF16)
                flat[0:1, pl.ds(pl.multiple_of((base + layer * 128 + g * GROUP) * LANES, 4096), 4096)] = group.reshape(1, 4096)

        finish(base, 2048)
    lines = []
    for half in range(2):
        tiles = [wg_ref[7, pl.ds(pl.multiple_of(VEC_AT + half * 104 + jnp.minimum(3 * pair + tile, 12) * 8, 8), 8)].astype(F32) for tile in range(5)]
        turned = pltpu.roll(jnp.concatenate(tiles, axis=1), 5 * LANES - 32 * pair, 1)
        lines += [turned[line:line + 1, :416] for line in range(8)]
    flat[0:1, pl.ds(14336 * LANES, 52 * LANES)] = jnp.concatenate(lines, axis=1).astype(BF16)
    finish(14336, 52)
    for q, (src, dst) in enumerate(((mv_ref, m_out), (vv_ref, v_out), (wv_ref, w_out))):
        pltpu.make_async_copy(src, dst, state_sem.at[q]).wait()
    every = wg_ref.at[:, pl.ds(0, SLICE_ROWS)]
    pltpu.make_async_copy(every, every, out_sem).wait()
    pltpu.make_async_copy(flat, pair_ref, pair_sem).wait()


def place_call(m_new, v_new, w_new, gathered):
    hbm = pl.BlockSpec(memory_space=pl.ANY)
    dma = pltpu.SemaphoreType.DMA
    flat = jax.ShapeDtypeStruct((SLICE_ROWS, LANES), F32)
    return pl.pallas_call(
        place_kernel,
        name='place_weights',
        out_shape=(flat, flat, flat) + tuple(jax.ShapeDtypeStruct((size, LANES), BF16) for size in (32768, 8192, 8192, 8192, 208))
        + (jax.ShapeDtypeStruct((1, PAIR_SIZE), BF16),),
        in_specs=[pl.BlockSpec(memory_space=pltpu.VMEM)] * 4,
        out_specs=[hbm] * 9,
        scratch_shapes=[
            pltpu.VMEM((1, PAIR_SIZE), BF16),
            pltpu.VMEM((2, 4, GROUP, LANES), F32),
            dma((3,)), dma, dma,
        ],
        compiler_params=pltpu.CompilerParams(vmem_limit_bytes=12 * 1024 * 1024),
    )(*(pltpu.with_memory_space_constraint(x, pltpu.VMEM) for x in (m_new, v_new, w_new, gathered)))


def to_tiles(tensor):
    return tensor.reshape(256, 8, 4, LANES).transpose(0, 2, 1, 3).reshape(8192, LANES)


def from_tiles(rows):
    return rows.reshape(256, 4, 8, LANES).transpose(0, 2, 1, 3).reshape(16, 128, 512)


def solution(mesh):
    def local_step(g_embed, g_attn, g_ffn_in, g_ffn_out, g_vec, m_shard, v_shard, w_shard):
        vec_rows = g_vec.reshape(2, 8, 13, LANES).transpose(0, 2, 1, 3).reshape(VEC_ROWS, LANES)
        tensors = (g_embed.reshape(32768, LANES), to_tiles(g_attn), to_tiles(g_ffn_in), g_ffn_out.reshape(8192, LANES), vec_rows)
        state = [shard.reshape(SLICE_ROWS, LANES) for shard in (m_shard, v_shard, w_shard)]
        m_new, v_new, w_new, gathered = step_call(tensors, state)
        m_new, v_new, w_new, embed, attn, ffn_in, ffn_out, vec, w_pair = place_call(m_new, v_new, w_new, gathered)
        wb_vec = vec.reshape(2, 13, 8, LANES).transpose(0, 2, 1, 3).reshape(16, 1664)
        return (m_new.reshape(-1), v_new.reshape(-1), w_new.reshape(-1), embed, from_tiles(attn), from_tiles(ffn_in),
                ffn_out.reshape(16, 512, 128), wb_vec, w_pair)

    return jax.shard_map(local_step, mesh=mesh, in_specs=(P(MESH_AXES),) * 8, out_specs=(P(MESH_AXES),) * 3 + (P(),) * 5 + (P(MESH_AXES),), check_vma=False)
```
